128 devices in a mesh: dp: 8 (over x, core), tensor: 16 (over z, y).
Axes of the slice: x: 4, y: 4, z: 4, core: 2. Of those that a mesh axis runs over, the one named last changes fastest.
Arguments:
- tokens: bfloat16 [192, 8, 4096], P('dp'), may hold values from -6 to 6
- norm_gain: float32 [4096], replicated, may hold values from 0.1 to 1.9
- in_weight: bfloat16 [4096, 2, 8192], P(None, None, 'tensor'), may hold values from -0.09375 to 0.09375
- group_weight: bfloat16 [4096, 2048], P(None, 'tensor'), may hold values from -0.09375 to 0.09375
- step_weight: bfloat16 [4096, 128], P(None, 'tensor'), may hold values from -0.09375 to 0.09375
- value_kernel: bfloat16 [4, 8192], P(None, 'tensor'), may hold values from -3 to 3
- value_offset: bfloat16 [8192], P('tensor'), may hold values from -3 to 3
- group_kernel: bfloat16 [4, 2048], P(None, 'tensor'), may hold values from -3 to 3
- group_offset: bfloat16 [2048], P('tensor'), may hold values from -3 to 3
- step_bias: float32 [128], P('tensor'), may hold values from -4 to 1
- decay_rate: float32 [128], P('tensor'), may hold values from 0.05 to 2
- skip_gain: float32 [128], P('tensor'), may hold values from 0.5 to 2
- out_gain: float32 [8192], P('tensor'), may hold values from 0.1 to 1.9
- out_weight: bfloat16 [8192, 4096], P('tensor'), may hold values from -0.0625 to 0.0625
- scan_state: bfloat16 [192, 128, 64, 128], P('dp', 'tensor'), may hold values from -6 to 6
- value_cache: bfloat16 [192, 3, 8192], P('dp', None, 'tensor'), may hold values from -6 to 6
- group_cache: bfloat16 [192, 3, 2048], P('dp', None, 'tensor'), may hold values from -6 to 6
- accepted: int32 [192], P('dp'), may hold values from 0 to 8, as said below
- draft_lengths: int32 [192], P('dp'), may hold values from 1 to 8, as said below
- live_flags: int32 [192], P('dp'), may hold values 0 or 1
Outputs:
- layer_out: bfloat16 [192, 8, 4096], P('dp')
- kept_state: bfloat16 [192, 128, 64, 128], P('dp', 'tensor')
- value_kept: bfloat16 [192, 3, 8192], P('dp', None, 'tensor')
- group_kept: bfloat16 [192, 3, 2048], P('dp', None, 'tensor')
- accepted_total: int32 [1], replicated
The draws below stay inside these ranges and needn't reach their ends.
Inputs may be any that keep to these rules, and one draw needn't show every extreme that they name: `draft_lengths`: positions at or after a request's draft length are padding. `accepted`: never more than the same request's draft length.
All inputs are finite; a program needn't handle non-finite values.
Results may differ from the reference program's by a relative error of at most 0.012.
Values may be sent and summed in bfloat16 or wider, within the bound.
A program may use at most 128 MiB of HBM per device.

```python
import math
import jax
import jax.numpy as jnp
from jax import lax

D = 4096
STATE = 128
HEADDIM = 64
CONV = 4
DRAFT = 8
REQ_DEV = 24
HEADS = 128
NGROUPS = 8
INNER = 8192
GCOLS = 2048
REQUESTS = 192


def draft_pair(key):
    block_count = REQUESTS // REQ_DEV
    full_row = jax.random.randint(jax.random.fold_in(key, 10), (), 0, REQUESTS)
    short_row = (full_row + 1) % REQUESTS
    block_caps = jax.random.randint(jax.random.fold_in(key, 11), (block_count,), 1, DRAFT + 1)
    block_caps = jnp.where(jnp.arange(block_count) == full_row // REQ_DEV, DRAFT, block_caps)
    per_request = jnp.repeat(block_caps, REQ_DEV, total_repeat_length=REQUESTS)
    lengths = jax.random.randint(jax.random.fold_in(key, 12), (REQUESTS,), 1, per_request + 1)
    row_ids = jnp.arange(REQUESTS)
    lengths = jnp.where(row_ids == full_row, DRAFT, lengths)
    lengths = jnp.where(row_ids == short_row, 1, lengths)
    accepted_counts = jax.random.randint(jax.random.fold_in(key, 13), (REQUESTS,), 0, lengths + 1)
    accepted_counts = jnp.where(row_ids == full_row, DRAFT, accepted_counts)
    accepted_counts = jnp.where(row_ids == short_row, 0, accepted_counts)
    return (lengths.astype(jnp.int32), accepted_counts.astype(jnp.int32))


def draw_draft_lengths(key, part):
    return draft_pair(key)[0]


def draw_accepted(key, part):
    return draft_pair(key)[1]


def plant(array, own_key, smallest, largest):
    extent = array.shape
    index_at = [jax.random.randint(jax.random.fold_in(own_key, axis), (), 0, extent[axis]) for axis in range(len(extent))]
    array = array.at[tuple(index_at)].set(smallest)
    longest = extent.index(max(extent))
    index_at[longest] = (index_at[longest] + 1) % extent[longest]
    return array.at[tuple(index_at)].set(largest)


def block_levels(own_key, dims, cuts, smallest, top_value):
    factor_of, own = 1.0, jax.random.fold_in(own_key, 6)
    for dim, blocks in cuts:
        draws = jnp.exp(jax.random.uniform(jax.random.fold_in(own, dim), (blocks,), jnp.float32, smallest / len(cuts), top_value / len(cuts)))
        factor_of = factor_of * jnp.repeat(draws, dims[dim] // blocks).reshape([-1 if axis == dim else 1 for axis in range(len(dims))])
    return factor_of


def noise(own_key, dims, deviation, most, cuts=(), kind=jnp.bfloat16):
    factor_of = block_levels(own_key, dims, cuts, -0.22, 0.18) if cuts else 1.0
    result = jax.random.normal(own_key, dims, jnp.float32) * deviation * factor_of
    return jnp.minimum(jnp.maximum(result, -most), most).astype(kind)


def setup_inputs(seed: int = 0) -> dict:
    arg_keys = jax.random.split(jax.random.key(seed), 21)
    tokens = noise(arg_keys[0], (REQUESTS, DRAFT, D), 1.0, 6.0, ((0, 8),))
    norm_gain = jnp.clip(1.0 + 0.18 * jax.random.normal(arg_keys[1], (D,), jnp.float32), 0.1, 1.9)
    in_weight = noise(arg_keys[2], (D, 2, INNER), D ** -0.5, 0.09375, ((2, 16),))
    group_weight = noise(arg_keys[3], (D, GCOLS), D ** -0.5, 0.09375, ((1, 16),))
    step_weight = noise(arg_keys[4], (D, HEADS), D ** -0.5, 0.09375, ((1, 16),))
    value_kernel = noise(arg_keys[5], (CONV, INNER), CONV ** -0.5, 3.0, ((1, 16),))
    value_offset = noise(arg_keys[6], (INNER,), 0.5, 3.0, ((0, 16),))
    group_kernel = noise(arg_keys[7], (CONV, GCOLS), CONV ** -0.5, 3.0, ((1, 16),))
    group_offset = noise(arg_keys[8], (GCOLS,), 0.5, 3.0, ((0, 16),))
    step_bias = jnp.clip(-4.0 + 5.0 * jax.random.uniform(arg_keys[9], (HEADS,), jnp.float32) ** block_levels(arg_keys[9], (HEADS,), ((0, 16),), -0.2, 0.2), -4.0, 1.0)
    decay_rate = jnp.clip(jnp.exp(math.log(2.0) - 3.6888794 * jax.random.uniform(arg_keys[10], (HEADS,), jnp.float32) ** block_levels(arg_keys[10], (HEADS,), ((0, 16),), -0.2, 0.2)), 0.05, 2.0)
    skip_gain = jnp.clip(0.5 + 1.5 * jax.random.uniform(arg_keys[11], (HEADS,), jnp.float32) ** block_levels(arg_keys[11], (HEADS,), ((0, 16),), -0.2, 0.2), 0.5, 2.0)
    out_gain = jnp.clip(1.0 + 0.18 * jax.random.normal(arg_keys[12], (INNER,), jnp.float32), 0.1, 1.9)
    out_weight = noise(arg_keys[13], (INNER, D), INNER ** -0.5, 0.0625, ((0, 16),))
    scan_state = noise(arg_keys[14], (REQUESTS, HEADS, HEADDIM, STATE), 1.0, 6.0, ((0, 8), (1, 16)))
    value_cache = noise(arg_keys[15], (REQUESTS, CONV - 1, INNER), 1.0, 6.0, ((0, 8), (2, 16)))
    group_cache = noise(arg_keys[16], (REQUESTS, CONV - 1, GCOLS), 1.0, 6.0, ((0, 8), (2, 16)))
    accepted = draw_accepted(jax.random.fold_in(arg_keys[20], 71), 0)
    draft_lengths = draw_draft_lengths(jax.random.fold_in(arg_keys[20], 71), 0)
    live_flags = plant((jax.random.randint(arg_keys[19], (REQUESTS,), 0, 8) < 7).astype(jnp.int32), jax.random.fold_in(arg_keys[19], 1), 0, 1)
    return {"tokens": tokens, "norm_gain": norm_gain, "in_weight": in_weight, "group_weight": group_weight, "step_weight": step_weight, "value_kernel": value_kernel, "value_offset": value_offset, "group_kernel": group_kernel, "group_offset": group_offset, "step_bias": step_bias, "decay_rate": decay_rate, "skip_gain": skip_gain, "out_gain": out_gain, "out_weight": out_weight, "scan_state": scan_state, "value_cache": value_cache, "group_cache": group_cache, "accepted": accepted, "draft_lengths": draft_lengths, "live_flags": live_flags}


EPSILON = 1e-05

def convolve(window, fresh_rows, kernel, offset):
    sequence = jnp.concatenate([window, fresh_rows], axis=1)
    length = fresh_rows.shape[1]
    summed = jnp.zeros(fresh_rows.shape, jnp.float32) + offset.astype(jnp.float32)
    for tap_index in range(kernel.shape[0]):
        summed = summed + kernel[tap_index].astype(jnp.float32) * sequence[:, tap_index:tap_index + length].astype(jnp.float32)
    return (jax.nn.silu(summed), sequence)

def keep_window(sequence, kept_count, width_rows):
    return jax.vmap(lambda single, start_row: lax.dynamic_slice_in_dim(single, start_row, width_rows, 0))(sequence, kept_count)

def reference(tokens, norm_gain, in_weight, group_weight, step_weight, value_kernel, value_offset, group_kernel, group_offset, step_bias, decay_rate, skip_gain, out_gain, out_weight, scan_state, value_cache, group_cache, accepted, draft_lengths, live_flags):
    flat_rows = tokens.reshape(REQUESTS * DRAFT, D).astype(jnp.float32)
    normed = (flat_rows * lax.rsqrt(lax.optimization_barrier(jnp.mean(flat_rows * flat_rows, axis=1, keepdims=True)) + EPSILON) * norm_gain).astype(jnp.bfloat16)
    inner_proj = jnp.dot(normed, in_weight.reshape(D, 2 * INNER), preferred_element_type=jnp.float32).astype(jnp.bfloat16).reshape(REQUESTS, DRAFT, 2, INNER)
    gate_part = inner_proj[:, :, 0]
    value_part = inner_proj[:, :, 1]
    group_proj = jnp.dot(normed, group_weight, preferred_element_type=jnp.float32).astype(jnp.bfloat16).reshape(REQUESTS, DRAFT, GCOLS)
    step_raw = jnp.dot(normed, step_weight, preferred_element_type=jnp.float32).reshape(REQUESTS, DRAFT, HEADS)
    value_conv, value_seq = convolve(value_cache, value_part, value_kernel, value_offset)
    group_conv, group_seq = convolve(group_cache, group_proj, group_kernel, group_offset)
    group_maps = group_conv.reshape(REQUESTS, DRAFT, NGROUPS, 2, STATE)
    input_maps = group_maps[:, :, :, 0]
    output_maps = group_maps[:, :, :, 1]
    step_size = jax.nn.softplus(step_raw + step_bias)
    decay_step = jnp.exp(-step_size * decay_rate)
    kept_count = accepted * live_flags
    per_group = HEADS // NGROUPS

    def head_scan(head_index):
        values = lax.dynamic_slice_in_dim(value_conv, head_index * HEADDIM, HEADDIM, 2)
        group_index = head_index // per_group
        input_map = lax.dynamic_index_in_dim(input_maps, group_index, 2, keepdims=False)
        output_map = lax.dynamic_index_in_dim(output_maps, group_index, 2, keepdims=False)
        head_decay = lax.dynamic_index_in_dim(decay_step, head_index, 2, keepdims=False)
        head_step = lax.dynamic_index_in_dim(step_size, head_index, 2, keepdims=False)
        initial = lax.dynamic_index_in_dim(scan_state, head_index, 1, keepdims=False).astype(jnp.float32)
        head_skip = lax.dynamic_index_in_dim(skip_gain, head_index, 0, keepdims=False)

        def advance(carry_pair, position):
            current, kept_now = carry_pair
            scaled = (head_step[:, position][:, None] * values[:, position])[:, :, None]
            current = head_decay[:, position][:, None, None] * current + scaled * input_map[:, position][:, None, :]
            produced = lax.optimization_barrier(jnp.sum(current * output_map[:, position][:, None, :], axis=2)) + head_skip * values[:, position]
            kept_now = jnp.where((position < kept_count)[:, None, None], current, kept_now)
            return ((current, kept_now), produced)
        (final_state, kept_now), produced = lax.scan(advance, (initial, initial), jnp.arange(DRAFT, dtype=jnp.int32))
        return (produced, kept_now.astype(jnp.bfloat16))
    produced, kept_heads = lax.map(head_scan, jnp.arange(HEADS, dtype=jnp.int32))
    head_out = jnp.transpose(produced, (2, 1, 0, 3)).reshape(REQUESTS, DRAFT, INNER)
    kept_state = jnp.transpose(kept_heads, (1, 0, 2, 3))
    gated = head_out * jax.nn.silu(gate_part.astype(jnp.float32))
    grouped = gated.reshape(REQUESTS, DRAFT, NGROUPS, INNER // NGROUPS)
    scale_rows = lax.rsqrt(lax.optimization_barrier(jnp.mean(grouped * grouped, axis=3, keepdims=True)) + EPSILON)
    valid_rows = (jnp.arange(DRAFT)[None, :] < draft_lengths[:, None]) & (live_flags[:, None] == 1)
    normalized = jnp.where(valid_rows[:, :, None], (grouped * scale_rows).reshape(REQUESTS, DRAFT, INNER) * out_gain, 0.0).astype(jnp.bfloat16)
    layer_out = jnp.dot(normalized.reshape(REQUESTS * DRAFT, INNER), out_weight, preferred_element_type=jnp.float32).astype(jnp.bfloat16).reshape(REQUESTS, DRAFT, D)
    value_kept = keep_window(value_seq, kept_count, CONV - 1)
    group_kept = keep_window(group_seq, kept_count, CONV - 1)
    accepted_total = jnp.sum(kept_count).astype(jnp.int32).reshape(1)
    return (layer_out, kept_state, value_kept, group_kept, accepted_total)
```

```python
import jax
import jax.numpy as jnp
from jax import lax
from jax.experimental import pallas as pl
from jax.experimental.pallas import tpu as pltpu
from jax.sharding import PartitionSpec as P

DP = "dp"


EPSILON = 1e-05


def swapped(value, axis, distance):
    mask = 2**distance
    pairs = [(source, source ^ mask) for source in range(lax.axis_size(axis))]
    return lax.ppermute(value, axis, pairs)


MESH = pl.DeviceIdType.MESH
TOP, BOTTOM = pl.ds(0, 48), pl.ds(48, 48)


def ring_places():
    tensor = lax.axis_index("tensor")
    z, y = tensor // 4, tensor % 4
    along_y = [{"tensor": z * 4 + (y + d) % 4} for d in range(4)]
    along_z = [{"tensor": ((z + d) % 4) * 4 + y} for d in range(4)]
    return (z, y, along_z, along_y)


def remote(src, dst, sems, place):
    send, recv, index = sems
    return pltpu.make_async_remote_copy(
        src_ref=src,
        dst_ref=dst,
        send_sem=send.at[index],
        recv_sem=recv.at[index],
        device_id=place,
        device_id_type=MESH,
    )


def widened_sum(*refs):
    total = refs[0][...].astype(jnp.float32)
    for ref in refs[1:]:
        total = total + ref[...].astype(jnp.float32)
    return total.astype(jnp.bfloat16)


def exchange_kernel(
    rows_ref,
    weight_ref,
    counts_ref,
    out_ref,
    total_ref,
    partial,
    first_recv,
    first_mix,
    first_sum,
    second_recv,
    second_mix,
    count_buf,
    send_sems,
    recv_sems,
    count_send,
    count_recv,
):
    z, y, along_z, along_y = ring_places()
    dp = lax.axis_index("dp")
    barrier = pltpu.get_barrier_semaphore()
    dp_peers = [{"dp": (dp + d) % 8} for d in range(1, 8)]
    ring_peers = [along_z[1], along_z[3], along_y[1], along_y[3]]
    for place in ring_peers + dp_peers:
        pl.semaphore_signal(barrier, inc=1, device_id=place, device_id_type=MESH)
    kept = jnp.sum(counts_ref[...].astype(jnp.float32), axis=1, keepdims=True)
    count_buf[0] = jnp.broadcast_to(kept, (8, 128))
    firsts = [along_y, along_z]
    seconds = [along_z, along_y]
    first_at = [y, z]
    second_at = [z, y]
    copies = []

    def launch(src, dst, stage, route, slot, place):
        copy = remote(src, dst, (send_sems, recv_sems, (stage, route, slot)), place)
        copy.start()
        copies.append(copy)
        return copy

    def project(route, step):
        base = ((first_at[route] + step) % 4) * 1024

        def one(j, carry):
            columns = pl.ds(pl.multiple_of(base + j * 256, 256), 256)
            partial[route, step, :, pl.ds(pl.multiple_of(j * 256, 256), 256)] = jnp.dot(
                rows_ref[pl.ds(route * 96, 96), :],
                weight_ref[:, columns],
                preferred_element_type=jnp.float32,
            ).astype(jnp.bfloat16)
            return carry

        lax.fori_loop(0, 4, one, 0)

    project(0, 2)
    pl.semaphore_wait(barrier, 11)
    count_copies = []
    for d in range(1, 8):
        copy = remote(count_buf.at[0], count_buf.at[d], (count_send, count_recv, d), dp_peers[d - 1])
        copy.start()
        count_copies.append(copy)

    def first_step(route):
        unit = partial.at[route]
        plus, minus = (firsts[route][1], firsts[route][3])
        a = launch(unit.at[2, TOP], first_recv.at[route, 0], 0, route, 0, plus)
        b = launch(unit.at[2, BOTTOM], first_recv.at[route, 1], 0, route, 1, minus)
        return [a, b]

    held = [first_step(0)]
    project(1, 2)
    held.append(first_step(1))
    for route in range(2):
        project(route, 1)
        held[route].append(
            launch(
                partial.at[route, 1, BOTTOM], first_recv.at[route, 3], 0, route, 3, firsts[route][1]
            )
        )
    for route in range(2):
        project(route, 3)
        held[route].append(
            launch(
                partial.at[route, 3, TOP], first_recv.at[route, 4], 0, route, 4, firsts[route][3]
            )
        )
    for route in range(2):
        held[route][0].wait_recv()
        first_mix[route, 0] = widened_sum(first_recv.at[route, 0], partial.at[route, 1, TOP])
        held[route].append(
            launch(first_mix.at[route, 0], first_recv.at[route, 2], 0, route, 2, firsts[route][1])
        )
        held[route][1].wait_recv()
        first_mix[route, 1] = widened_sum(first_recv.at[route, 1], partial.at[route, 3, BOTTOM])
        held[route].append(
            launch(first_mix.at[route, 1], first_recv.at[route, 5], 0, route, 5, firsts[route][3])
        )
    for route in range(2):
        project(route, 0)
    for half in range(2):
        for route in range(2):
            rows = (TOP, BOTTOM)[half]
            waits = ((3, 4), (2, 5))[half]
            for index in waits:
                held[route][index].wait_recv()
            plus_ref = first_recv.at[route, 2 + half]
            minus_ref = first_recv.at[route, 4 + half]
            for j in range(4):
                columns = pl.ds(j * 256, 256)
                first_sum[route, j, rows] = widened_sum(
                    partial.at[route, 0, rows, columns],
                    plus_ref.at[:, columns],
                    minus_ref.at[:, columns],
                )
    late = []
    for route in range(2):
        at = second_at[route]
        plus, minus = (seconds[route][1], seconds[route][3])
        unit = [first_sum.at[route, (at + k) % 4] for k in range(4)]
        landing = second_recv.at[route]
        late.append(
            [
                launch(unit[2].at[TOP], landing.at[0], 1, route, 0, plus),
                launch(unit[2].at[BOTTOM], landing.at[1], 1, route, 1, minus),
                launch(unit[1].at[BOTTOM], landing.at[3], 1, route, 3, plus),
                launch(unit[3].at[TOP], landing.at[4], 1, route, 4, minus),
            ]
        )
    for route in range(2):
        at = second_at[route]
        plus, minus = (seconds[route][1], seconds[route][3])
        landing = second_recv.at[route]
        late[route][0].wait_recv()
        second_mix[route, 0] = widened_sum(landing.at[0], first_sum.at[route, (at + 1) % 4, TOP])
        late[route].append(
            launch(second_mix.at[route, 0], landing.at[2], 1, route, 2, plus)
        )
        late[route][1].wait_recv()
        second_mix[route, 1] = widened_sum(landing.at[1], first_sum.at[route, (at + 3) % 4, BOTTOM])
        late[route].append(
            launch(second_mix.at[route, 1], landing.at[5], 1, route, 5, minus)
        )

    def spot(route, half, first, second, width):
        column = pl.multiple_of(first * 1024 + second * 256, 256)
        return out_ref.at[pl.ds(route * 96 + half * 48, 48), pl.ds(column, width)]

    for half in range(2):
        for route in range(2):
            rows = (TOP, BOTTOM)[half]
            waits = ((3, 4), (2, 5))[half]
            for index in waits:
                late[route][index].wait_recv()
            own = spot(route, half, first_at[route], second_at[route], 256)
            own[...] = widened_sum(
                first_sum.at[route, second_at[route], rows],
                second_recv.at[route, 2 + half],
                second_recv.at[route, 4 + half],
            )

    def spread(stage, places, piece):
        started = []
        for route in range(2):
            plus, minus = (places[route][1], places[route][3])
            started.append(
                [
                    launch(piece(route, 0, 0), piece(route, 0, 0), stage, route, 0, plus),
                    launch(piece(route, 1, 0), piece(route, 1, 0), stage, route, 1, minus),
                    launch(piece(route, 1, 0), piece(route, 1, 0), stage, route, 2, plus),
                    launch(piece(route, 0, 0), piece(route, 0, 0), stage, route, 3, minus),
                ]
            )
        for route in range(2):
            plus, minus = (places[route][1], places[route][3])
            started[route][0].wait_recv()
            started[route].append(
                launch(piece(route, 0, 3), piece(route, 0, 3), stage, route, 4, plus)
            )
            started[route][1].wait_recv()
            started[route].append(
                launch(piece(route, 1, 1), piece(route, 1, 1), stage, route, 5, minus)
            )
        for route in range(2):
            for index in range(2, 6):
                started[route][index].wait_recv()

    def near(route, half, k):
        return spot(route, half, first_at[route], (second_at[route] + k) % 4, 256)

    def far(route, half, k):
        return spot(route, half, (first_at[route] + k) % 4, 0, 1024)

    spread(2, seconds, near)
    spread(3, firsts, far)
    for copy in count_copies:
        copy.wait_recv()
    everyone = count_buf[0]
    for d in range(1, 8):
        everyone = everyone + count_buf[d]
    total_ref[...] = everyone.astype(jnp.int32)
    for copy in copies + count_copies:
        copy.wait_send()


def exchange(rows, weight, counts):
    half = pltpu.VMEM((2, 6, 48, 1024), jnp.bfloat16)
    return pl.pallas_call(
        exchange_kernel,
        out_shape=(
            jax.ShapeDtypeStruct((192, 4096), jnp.bfloat16),
            jax.ShapeDtypeStruct((8, 128), jnp.int32),
        ),
        in_specs=[pl.BlockSpec(memory_space=pltpu.VMEM)] * 3,
        out_specs=(pl.BlockSpec(memory_space=pltpu.VMEM),) * 2,
        scratch_shapes=[
            pltpu.VMEM((2, 4, 96, 1024), jnp.bfloat16),
            half,
            pltpu.VMEM((2, 2, 48, 1024), jnp.bfloat16),
            pltpu.VMEM((2, 4, 96, 256), jnp.bfloat16),
            pltpu.VMEM((2, 6, 48, 256), jnp.bfloat16),
            pltpu.VMEM((2, 2, 48, 256), jnp.bfloat16),
            pltpu.VMEM((8, 8, 128), jnp.float32),
            pltpu.SemaphoreType.DMA((4, 2, 6)),
            pltpu.SemaphoreType.DMA((4, 2, 6)),
            pltpu.SemaphoreType.DMA((8,)),
            pltpu.SemaphoreType.DMA((8,)),
        ],
        compiler_params=pltpu.CompilerParams(
            collective_id=0, has_side_effects=True, vmem_limit_bytes=40 * 1024 * 1024
        ),
    )(rows, weight, counts)


def convolve(window, fresh_rows, kernel, offset):
    sequence = jnp.concatenate([window, fresh_rows], axis=1)
    length = fresh_rows.shape[1]
    summed = jnp.zeros(fresh_rows.shape, jnp.float32) + offset.astype(jnp.float32)
    for tap_index in range(kernel.shape[0]):
        summed = summed + kernel[tap_index].astype(jnp.float32) * sequence[
            :, tap_index : tap_index + length
        ].astype(jnp.float32)
    return (jax.nn.silu(summed), sequence)


def keep_window(sequence, kept_count, width_rows):
    return jax.vmap(
        lambda single, start_row: lax.dynamic_slice_in_dim(single, start_row, width_rows, 0)
    )(sequence, kept_count)


def local(
    tokens,
    norm_gain,
    in_weight,
    group_weight,
    step_weight,
    value_kernel,
    value_offset,
    group_kernel,
    group_offset,
    step_bias,
    decay_rate,
    skip_gain,
    out_gain,
    out_weight,
    scan_state,
    value_cache,
    group_cache,
    accepted,
    draft_lengths,
    live_flags,
):
    requests, positions, model_width = tokens.shape
    row_total = requests * positions
    head_count = step_bias.shape[0]
    inner_dev = value_offset.shape[0]
    head_dim = inner_dev // head_count
    tap_count = value_kernel.shape[0]
    kept_count = accepted * live_flags
    flat_rows = tokens.reshape(row_total, model_width).astype(jnp.float32)
    normed = (
        flat_rows
        * lax.rsqrt(jnp.mean(flat_rows * flat_rows, axis=1, keepdims=True) + EPSILON)
        * norm_gain
    ).astype(jnp.bfloat16)
    parity = lax.axis_index("tensor") % 2
    in_flat = in_weight.reshape(in_weight.shape[0], 2 * inner_dev)
    inner_sum = jnp.dot(normed, in_flat, preferred_element_type=jnp.float32)
    group_sum = jnp.dot(normed, group_weight, preferred_element_type=jnp.float32)
    step_raw = jnp.dot(normed, step_weight, preferred_element_type=jnp.float32)
    inner_proj = inner_sum.astype(jnp.bfloat16).reshape(requests, positions, 2 * inner_dev)
    gate_part = inner_proj[:, :, :inner_dev]
    value_part = inner_proj[:, :, inner_dev:]
    group_proj = group_sum.astype(jnp.bfloat16).reshape(requests, positions, group_weight.shape[1])
    value_conv, value_seq = convolve(value_cache, value_part, value_kernel, value_offset)
    own_conv, group_seq = convolve(group_cache, group_proj, group_kernel, group_offset)
    other_conv = swapped(own_conv, "tensor", 0)
    input_map = jnp.where(parity == 0, own_conv, other_conv)
    output_map = jnp.where(parity == 0, other_conv, own_conv)
    values = value_conv.reshape(requests, positions, head_count, head_dim)
    step_size = jax.nn.softplus(step_raw.reshape(requests, positions, head_count) + step_bias)
    log_decay = -step_size * decay_rate
    prefix = jnp.concatenate(
        [jnp.zeros((requests, 1, head_count), jnp.float32), jnp.cumsum(log_decay, axis=1)], axis=1
    )
    after_step = prefix[:, 1:]
    alignment = jnp.einsum("rsn,rjn->rsj", output_map, input_map)
    causal = (jnp.arange(positions)[:, None] >= jnp.arange(positions)[None, :])[None, :, :, None]
    spread = after_step[:, :, None, :] - after_step[:, None, :, :]
    weights_mix = (
        jnp.where(causal, jnp.exp(jnp.where(causal, spread, 0.0)), 0.0)
        * step_size[:, None, :, :]
        * alignment[:, :, :, None]
    )
    within = jnp.einsum("rsjh,rjhp->rshp", weights_mix, values)
    initial = scan_state.astype(jnp.float32)
    carried = jnp.einsum("rhpn,rsn->rshp", initial, output_map) * jnp.exp(after_step)[:, :, :, None]
    head_out = within + carried + skip_gain[:, None] * values
    one_hot = (jnp.arange(positions + 1)[None, :] == kept_count[:, None]).astype(jnp.float32)
    prefix_kept = jnp.sum(one_hot[:, :, None] * prefix, axis=1)
    before_kept = (jnp.arange(positions)[None, :] < kept_count[:, None])[:, :, None]
    keep_weight = (
        jnp.where(
            before_kept,
            jnp.exp(jnp.where(before_kept, prefix_kept[:, None, :] - after_step, 0.0)),
            0.0,
        )
        * step_size
    )
    weighted = keep_weight[:, :, :, None] * values
    kept_state = (
        jnp.exp(prefix_kept)[:, :, None, None] * initial
        + jnp.einsum("rjhp,rjn->rhpn", weighted, input_map)
    ).astype(jnp.bfloat16)
    gated = head_out.reshape(row_total, inner_dev) * jax.nn.silu(
        gate_part.reshape(row_total, inner_dev).astype(jnp.float32)
    )
    own_squares = jnp.sum(gated * gated, axis=1)
    other_squares = swapped(own_squares, "tensor", 0)
    scale_rows = lax.rsqrt((own_squares + other_squares) / (2 * inner_dev) + EPSILON)
    valid_rows = (jnp.arange(positions)[None, :] < draft_lengths[:, None]) & (
        live_flags[:, None] == 1
    )
    normalized = jnp.where(
        valid_rows.reshape(row_total, 1), gated * scale_rows[:, None] * out_gain, 0.0
    ).astype(jnp.bfloat16)
    layer_rows, totals = exchange(normalized, out_weight, kept_count.reshape(1, requests))
    accepted_total = totals[0, :1]
    value_kept = keep_window(value_seq, kept_count, tap_count - 1)
    group_kept = keep_window(group_seq, kept_count, tap_count - 1)
    return (
        layer_rows.reshape(requests, positions, model_width),
        kept_state,
        value_kept,
        group_kept,
        accepted_total,
    )


def solution(mesh):
    in_specs = (
        P(DP, None, None),
        P(),
        P(None, None, "tensor"),
        P(None, "tensor"),
        P(None, "tensor"),
        P(None, "tensor"),
        P("tensor"),
        P(None, "tensor"),
        P("tensor"),
        P("tensor"),
        P("tensor"),
        P("tensor"),
        P("tensor"),
        P("tensor", None),
        P(DP, "tensor", None, None),
        P(DP, None, "tensor"),
        P(DP, None, "tensor"),
        P(DP),
        P(DP),
        P(DP),
    )
    out_specs = (
        P(DP, None, None),
        P(DP, "tensor", None, None),
        P(DP, None, "tensor"),
        P(DP, None, "tensor"),
        P(),
    )
    return jax.shard_map(local, mesh=mesh, in_specs=in_specs, out_specs=out_specs, check_vma=False)
```

```python
import jax
import jax.numpy as jnp
from jax import lax
from jax.experimental import pallas as pl
from jax.experimental.pallas import tpu as pltpu
from jax.sharding import PartitionSpec as P

DP = "dp"


EPSILON = 1e-05


def swapped(value, axis, distance):
    mask = 2**distance
    pairs = [(source, source ^ mask) for source in range(lax.axis_size(axis))]
    return lax.ppermute(value, axis, pairs)


MESH = pl.DeviceIdType.MESH
TOP, BOTTOM = pl.ds(0, 48), pl.ds(48, 48)


def ring_places():
    tensor = lax.axis_index("tensor")
    z, y = tensor // 4, tensor % 4
    along_y = [{"tensor": z * 4 + (y + d) % 4} for d in range(4)]
    along_z = [{"tensor": ((z + d) % 4) * 4 + y} for d in range(4)]
    return (z, y, along_z, along_y)


def remote(src, dst, sems, place):
    send, recv, index = sems
    return pltpu.make_async_remote_copy(
        src_ref=src,
        dst_ref=dst,
        send_sem=send.at[index],
        recv_sem=recv.at[index],
        device_id=place,
        device_id_type=MESH,
    )


def widened_sum(*refs):
    total = refs[0][...].astype(jnp.float32)
    for ref in refs[1:]:
        total = total + ref[...].astype(jnp.float32)
    return total.astype(jnp.bfloat16)


def layer_kernel(
    tokens_in,
    gain_in,
    in_weight_in,
    group_weight_in,
    step_weight_in,
    value_kernel_in,
    value_offset_in,
    group_kernel_in,
    group_offset_in,
    step_bias_in,
    decay_rate_in,
    skip_gain_in,
    out_gain_in,
    out_weight_in,
    state_in,
    value_cache_in,
    group_cache_in,
    accepted_in,
    lengths_in,
    live_in,
    out_ref,
    kept_ref,
    value_kept,
    group_kept,
    total_ref,
    tokens,
    gain,
    in_weight,
    group_weight,
    step_weight,
    value_kernel,
    value_offset,
    group_kernel,
    group_offset,
    step_bias,
    decay_rate,
    skip_gain,
    out_gain,
    out_weight,
    state,
    value_cache,
    group_cache,
    accepted,
    lengths,
    live,
    normed,
    spread_a,
    spread_b,
    inner,
    group_rows,
    step_rows,
    maps,
    map_rows,
    carried,
    small,
    mixing,
    decay_kept,
    weighted,
    turned,
    input_rows,
    gated_rows,
    rows_ref,
    squares,
    square_own,
    square_other,
    scale_rows,
    partial,
    first_recv,
    first_mix,
    first_sum,
    second_recv,
    second_mix,
    count_buf,
    send_sems,
    recv_sems,
    count_send,
    count_recv,
    swap_sems,
    load_sems,
    chunk_sems,
):
    z, y, along_z, along_y = ring_places()
    dp = lax.axis_index("dp")
    parity = y % 2
    mate = {"tensor": z * 4 + (y + 1 - 2 * parity)}
    barrier = pltpu.get_barrier_semaphore()
    dp_peers = [{"dp": (dp + d) % 8} for d in range(1, 8)]
    ring_peers = [along_z[1], along_z[3], along_y[1], along_y[3]]
    for place in ring_peers + dp_peers:
        pl.semaphore_signal(barrier, inc=1, device_id=place, device_id_type=MESH)
    loads = {}

    def load(name, src, dst, index):
        loads[name] = pltpu.make_async_copy(src, dst, load_sems.at[index])
        loads[name].start()

    load("tokens", tokens_in, tokens, 0)
    load("gain", gain_in, gain, 1)
    load("group_weight", group_weight_in, group_weight, 3)
    load("accepted", accepted_in, accepted, 17)
    load("lengths", lengths_in, lengths, 18)
    load("live", live_in, live, 19)
    load("group_cache", group_cache_in, group_cache, 16)
    load("group_kernel", group_kernel_in, group_kernel, 7)
    load("group_offset", group_offset_in, group_offset, 8)
    load("step_weight", step_weight_in, step_weight, 4)
    load("step_bias", step_bias_in, step_bias, 9)
    load("decay_rate", decay_rate_in, decay_rate, 10)
    load("skip_gain", skip_gain_in, skip_gain, 11)
    chunks = []
    for index in range(4):
        rows = pl.ds(index * 8192, 8192)
        copy = pltpu.make_async_copy(in_weight_in.at[rows], in_weight.at[rows], chunk_sems.at[index])
        copy.start()
        chunks.append(copy)
    load("value_cache", value_cache_in, value_cache, 15)
    load("value_kernel", value_kernel_in, value_kernel, 5)
    load("value_offset", value_offset_in, value_offset, 6)
    load("out_gain", out_gain_in, out_gain, 12)
    load("state", state_in, state, 14)
    load("out_weight", out_weight_in, out_weight, 13)
    def column(ref):
        square = lax.broadcasted_iota(jnp.int32, (24, 24), 0) == lax.broadcasted_iota(
            jnp.int32, (24, 24), 1
        )
        values = jnp.broadcast_to(ref[...].astype(jnp.float32), (24, 24))
        return jnp.sum(jnp.where(square, values, 0.0), axis=1, keepdims=True)

    loads["gain"].wait()
    loads["tokens"].wait()

    def normalize(block, carry):
        rows = pl.ds(pl.multiple_of(block * 16, 16), 16)
        total = jnp.zeros((16, 256), jnp.float32)
        for part in range(16):
            piece = tokens[rows, part * 256 : (part + 1) * 256].astype(jnp.float32)
            total = total + piece * piece
        mean = jnp.sum(total, axis=1, keepdims=True) / 4096.0
        scale = jnp.broadcast_to(lax.rsqrt(mean + EPSILON), (16, 256))
        for part in range(16):
            columns = slice(part * 256, (part + 1) * 256)
            piece = tokens[rows, columns].astype(jnp.float32)
            normed[rows, columns] = (piece * scale * gain[:, columns]).astype(jnp.bfloat16)
        return carry

    lax.fori_loop(0, 12, normalize, 0)
    loads["group_weight"].wait()
    group_rows[...] = jnp.dot(
        normed[...], group_weight[...], preferred_element_type=jnp.float32
    )
    for name in ("accepted", "lengths", "live", "group_cache", "group_kernel", "group_offset"):
        loads[name].wait()
    kept = column(accepted) * column(live)
    alive = column(live) == 1.0
    length_column = column(lengths)

    def sequence_of(cache, rows):
        early = [cache[t].astype(jnp.float32) for t in range(3)]
        return early + [rounded(piece) for piece in rows]

    def rounded(piece):
        return piece.astype(jnp.bfloat16).astype(jnp.float32)

    def convolved(sequence, taps, offset):
        out = []
        for s in range(8):
            total = offset
            for k in range(4):
                total = total + taps[k] * sequence[s + k]
            out.append(total / (1.0 + jnp.exp(-total)))
        return out

    def kept_rows(sequence, counts, t):
        chosen = sequence[t]
        for k in range(1, 9):
            chosen = jnp.where(counts == float(k), sequence[k + t], chosen)
        return chosen.astype(jnp.bfloat16)

    group_taps = [group_kernel[k : k + 1, :].astype(jnp.float32) for k in range(4)]
    group_sequence = sequence_of(
        group_cache, [group_rows[pl.ds(s, 24, stride=8), :] for s in range(8)]
    )
    own_maps = convolved(
        group_sequence, group_taps, group_offset[...].astype(jnp.float32).reshape(1, 128)
    )
    for s in range(8):
        maps[parity, s] = own_maps[s]
    pl.semaphore_wait(barrier, 11)
    swap = pltpu.make_async_remote_copy(
        src_ref=maps.at[parity],
        dst_ref=maps.at[parity],
        send_sem=swap_sems.at[0],
        recv_sem=swap_sems.at[1],
        device_id=mate,
        device_id_type=MESH,
    )
    swap.start()
    count_buf[0] = jnp.broadcast_to(jnp.sum(kept, axis=0, keepdims=True), (8, 128))
    count_copies = []
    for d in range(1, 8):
        copy = remote(count_buf.at[0], count_buf.at[d], (count_send, count_recv, d), dp_peers[d - 1])
        copy.start()
        count_copies.append(copy)
    for t in range(3):
        group_kept[t] = kept_rows(group_sequence, kept, t)

    for name in ("step_weight", "step_bias", "decay_rate", "skip_gain"):
        loads[name].wait()
    step_rows[:, 0:8] = lax.dot_general(
        normed[...],
        step_weight[...],
        (((1,), (1,)), ((), ())),
        preferred_element_type=jnp.float32,
    )

    inner[...] = jnp.zeros_like(inner)

    def widen(start, spread):
        spread[...] = in_weight[pl.ds(pl.multiple_of(start * 2048, 2048), 2048), :].astype(
            jnp.float32
        )

    def multiply(start, spread):
        left = normed[:, pl.ds(pl.multiple_of(start * 256, 256), 256)]
        for part in range(2):
            for j in range(0, 4, 2):
                right = jnp.concatenate(
                    [
                        spread[pl.ds((j + i) * 2 + part, 256, stride=8), :].astype(jnp.bfloat16)
                        for i in range(2)
                    ],
                    axis=1,
                )
                product = jnp.dot(left, right, preferred_element_type=jnp.float32)
                for i in range(2):
                    inner[part * 4 + j + i] += product[:, i * 128 : (i + 1) * 128]

    def pair(index, carry):
        widen(2 * index, spread_a)
        multiply(2 * index, spread_a)
        widen(2 * index + 1, spread_b)
        multiply(2 * index + 1, spread_b)
        return carry

    for index in range(4):
        chunks[index].wait()
        lax.fori_loop(2 * index, 2 * index + 2, pair, 0)

    steps, after = [], []
    running = None
    for s in range(8):
        raw = step_rows[pl.ds(s, 24, stride=8), 0:8] + step_bias[...]
        size = jnp.maximum(raw, 0.0) + jnp.log1p(jnp.exp(-jnp.abs(raw)))
        change = -size * decay_rate[...]
        running = change if running is None else running + change
        steps.append(size)
        after.append(running)
    prefix_kept = jnp.zeros_like(running)
    for s in range(8):
        prefix_kept = jnp.where(kept == float(s + 1), after[s], prefix_kept)
    for s in range(8):
        small[pl.ds((36 + s) * 24, 24), 0:8] = jnp.exp(after[s])
        small[pl.ds((44 + s) * 24, 24), 0:8] = (
            jnp.where(kept > float(s), jnp.exp(prefix_kept - after[s]), 0.0) * steps[s]
        )
    head_decay = jnp.exp(prefix_kept)
    for h in range(8):
        decay_kept[h] = jnp.broadcast_to(head_decay[:, h : h + 1], (24, 128))
    swap.wait_recv()
    for s in range(8):
        map_rows[pl.ds(s, 24, stride=8), :] = maps[1, s]
        input_rows[pl.ds(s * 24, 24), :] = maps[0, s]
        for j in range(s + 1):
            match = jnp.sum(maps[1, s] * maps[0, j], axis=1, keepdims=True)
            small[pl.ds((s * (s + 1) // 2 + j) * 24, 24), 0:8] = (
                jnp.exp(after[s] - after[j]) * steps[j] * match
            )
    hot = (
        lax.broadcasted_iota(jnp.int32, (8, 512), 1) // 64
        == lax.broadcasted_iota(jnp.int32, (8, 512), 0)
    ).astype(jnp.bfloat16)

    def expand(index, carry):
        rows = pl.ds(pl.multiple_of(index * 208, 16), 208)
        mixing[rows, :] = jnp.dot(
            small[rows, 0:8].astype(jnp.bfloat16), hot, preferred_element_type=jnp.float32
        )
        return carry

    lax.fori_loop(0, 6, expand, 0)
    loads["state"].wait()

    def carry_over(index, carry):
        for i in range(6):
            request = index * 6 + i
            rows = pl.ds(pl.multiple_of(request * 8, 8), 8)
            product = lax.dot_general(
                map_rows[rows, :].astype(jnp.bfloat16),
                state[request],
                (((1,), (1,)), ((), ())),
                preferred_element_type=jnp.float32,
            )
            for block in range(4):
                carried[block, rows, :] = product[:, block * 128 : (block + 1) * 128]
        return carry

    lax.fori_loop(0, 4, carry_over, 0)
    for name in ("value_cache", "value_kernel", "value_offset", "out_gain"):
        loads[name].wait()

    offset_row = value_offset[...].astype(jnp.float32).reshape(1, 512)
    for block in range(4):
        columns = slice(block * 128, (block + 1) * 128)
        lane = lax.broadcasted_iota(jnp.int32, (8, 128), 1)
        skip = jnp.where(
            lane < 64,
            jnp.broadcast_to(skip_gain[:, 2 * block : 2 * block + 1], (8, 128)),
            jnp.broadcast_to(skip_gain[:, 2 * block + 1 : 2 * block + 2], (8, 128)),
        )
        taps = [value_kernel[k : k + 1, columns].astype(jnp.float32) for k in range(4)]
        offset = offset_row[:, columns]
        for tile in range(3):
            eight = pl.ds(tile * 8, 8)
            counts = kept[tile * 8 : tile * 8 + 8]
            sequence = [value_cache[t, eight, columns].astype(jnp.float32) for t in range(3)] + [
                rounded(inner[4 + block, pl.ds(tile * 64 + s, 8, stride=8), :])
                for s in range(8)
            ]
            for t in range(3):
                value_kept[t, eight, columns] = kept_rows(sequence, counts, t)
            values = convolved(sequence, taps, offset)
            for s in range(8):
                weighted[pl.ds(s * 24 + tile * 8, 8), columns] = (
                    mixing[pl.ds((44 + s) * 24 + tile * 8, 8), columns] * values[s]
                )
                total = (
                    mixing[pl.ds((36 + s) * 24 + tile * 8, 8), columns]
                    * carried[block, pl.ds(tile * 64 + s, 8, stride=8), :]
                    + skip * values[s]
                )
                for j in range(s + 1):
                    q = s * (s + 1) // 2 + j
                    total = total + mixing[pl.ds(q * 24 + tile * 8, 8), columns] * values[j]
                gate = rounded(inner[block, pl.ds(tile * 64 + s, 8, stride=8), :])
                gated = total * (gate / (1.0 + jnp.exp(-gate)))
                square = gated * gated
                if block:
                    square = square + squares[s, eight]
                squares[s, eight] = square
                valid = jnp.logical_and(
                    alive[tile * 8 : tile * 8 + 8],
                    length_column[tile * 8 : tile * 8 + 8] > float(s),
                )
                gated_rows[block, pl.ds(tile * 64 + s, 8, stride=8), :] = jnp.where(
                    valid, gated * out_gain[:, columns], 0.0
                )
    lanes = lax.broadcasted_iota(jnp.int32, (24, 128), 1)
    own = jnp.zeros((24, 128), jnp.float32)
    for s in range(8):
        own = jnp.where(lanes == s, jnp.sum(squares[s], axis=1, keepdims=True), own)
    square_own[...] = own
    square_swap = pltpu.make_async_remote_copy(
        src_ref=square_own,
        dst_ref=square_other,
        send_sem=swap_sems.at[2],
        recv_sem=swap_sems.at[3],
        device_id=mate,
        device_id_type=MESH,
    )
    square_swap.start()
    for block in range(4):
        rows_ref[:, block * 128 : (block + 1) * 128] = gated_rows[block].astype(jnp.bfloat16)
    loads["out_weight"].wait()
    weight_ref = out_weight
    turned[...] = jnp.transpose(weighted[...]).astype(jnp.bfloat16)
    square_swap.wait_recv()
    scales = lax.rsqrt((square_own[...] + square_other[...]) / 1024.0 + EPSILON)
    for s in range(8):
        scale_rows[pl.ds(s, 24, stride=8), :] = jnp.broadcast_to(scales[:, s : s + 1], (24, 128))

    def keep_states():
        owner = lax.rem(lax.broadcasted_iota(jnp.int32, (192, 128), 0), 24)

        def keep(index, carry):
            inputs = input_rows[...]
            right = jnp.concatenate(
                [
                    jnp.where(owner == 2 * index + i, inputs, 0.0).astype(jnp.bfloat16)
                    for i in range(2)
                ],
                axis=1,
            )
            for h in range(8):
                update = jnp.dot(
                    turned[h * 64 : (h + 1) * 64, :], right, preferred_element_type=jnp.float32
                )
                for i in range(2):
                    request = 2 * index + i
                    decay = decay_kept[h, pl.ds(request, 1), :]
                    before = state[request, h * 64 : (h + 1) * 64, :].astype(jnp.float32)
                    kept_ref[request, h * 64 : (h + 1) * 64, :] = (
                        decay * before + update[:, i * 128 : (i + 1) * 128]
                    ).astype(jnp.bfloat16)
            return carry

        lax.fori_loop(0, 12, keep, 0)

    firsts = [along_y, along_z]
    seconds = [along_z, along_y]
    first_at = [y, z]
    second_at = [z, y]
    copies = []

    def launch(src, dst, stage, route, slot, place):
        copy = remote(src, dst, (send_sems, recv_sems, (stage, route, slot)), place)
        copy.start()
        copies.append(copy)
        return copy

    def project(route, step):
        base = ((first_at[route] + step) % 4) * 1024

        def one(j, carry):
            columns = pl.ds(pl.multiple_of(base + j * 256, 256), 256)
            product = jnp.dot(
                rows_ref[pl.ds(route * 96, 96), :],
                weight_ref[:, columns],
                preferred_element_type=jnp.float32,
            )
            scale = scale_rows[pl.ds(route * 96, 96), :]
            partial[route, step, :, pl.ds(pl.multiple_of(j * 256, 256), 256)] = (
                product * jnp.concatenate([scale, scale], axis=1)
            ).astype(jnp.bfloat16)
            return carry

        lax.fori_loop(0, 4, one, 0)

    project(0, 2)

    def first_step(route):
        unit = partial.at[route]
        plus, minus = (firsts[route][1], firsts[route][3])
        a = launch(unit.at[2, TOP], first_recv.at[route, 0], 0, route, 0, plus)
        b = launch(unit.at[2, BOTTOM], first_recv.at[route, 1], 0, route, 1, minus)
        return [a, b]

    held = [first_step(0)]
    project(1, 2)
    held.append(first_step(1))
    for route in range(2):
        project(route, 1)
        held[route].append(
            launch(
                partial.at[route, 1, BOTTOM], first_recv.at[route, 3], 0, route, 3, firsts[route][1]
            )
        )
    for route in range(2):
        project(route, 3)
        held[route].append(
            launch(
                partial.at[route, 3, TOP], first_recv.at[route, 4], 0, route, 4, firsts[route][3]
            )
        )
    for route in range(2):
        held[route][0].wait_recv()
        first_mix[route, 0] = widened_sum(first_recv.at[route, 0], partial.at[route, 1, TOP])
        held[route].append(
            launch(first_mix.at[route, 0], first_recv.at[route, 2], 0, route, 2, firsts[route][1])
        )
        held[route][1].wait_recv()
        first_mix[route, 1] = widened_sum(first_recv.at[route, 1], partial.at[route, 3, BOTTOM])
        held[route].append(
            launch(first_mix.at[route, 1], first_recv.at[route, 5], 0, route, 5, firsts[route][3])
        )
    for route in range(2):
        project(route, 0)
    keep_states()
    for half in range(2):
        for route in range(2):
            rows = (TOP, BOTTOM)[half]
            waits = ((3, 4), (2, 5))[half]
            for index in waits:
                held[route][index].wait_recv()
            plus_ref = first_recv.at[route, 2 + half]
            minus_ref = first_recv.at[route, 4 + half]
            for j in range(4):
                columns = pl.ds(j * 256, 256)
                first_sum[route, j, rows] = widened_sum(
                    partial.at[route, 0, rows, columns],
                    plus_ref.at[:, columns],
                    minus_ref.at[:, columns],
                )
    late = []
    for route in range(2):
        at = second_at[route]
        plus, minus = (seconds[route][1], seconds[route][3])
        unit = [first_sum.at[route, (at + k) % 4] for k in range(4)]
        landing = second_recv.at[route]
        late.append(
            [
                launch(unit[2].at[TOP], landing.at[0], 1, route, 0, plus),
                launch(unit[2].at[BOTTOM], landing.at[1], 1, route, 1, minus),
                launch(unit[1].at[BOTTOM], landing.at[3], 1, route, 3, plus),
                launch(unit[3].at[TOP], landing.at[4], 1, route, 4, minus),
            ]
        )
    for route in range(2):
        at = second_at[route]
        plus, minus = (seconds[route][1], seconds[route][3])
        landing = second_recv.at[route]
        late[route][0].wait_recv()
        second_mix[route, 0] = widened_sum(landing.at[0], first_sum.at[route, (at + 1) % 4, TOP])
        late[route].append(
            launch(second_mix.at[route, 0], landing.at[2], 1, route, 2, plus)
        )
        late[route][1].wait_recv()
        second_mix[route, 1] = widened_sum(landing.at[1], first_sum.at[route, (at + 3) % 4, BOTTOM])
        late[route].append(
            launch(second_mix.at[route, 1], landing.at[5], 1, route, 5, minus)
        )

    def spot(route, half, first, second, width):
        column = pl.multiple_of(first * 1024 + second * 256, 256)
        return out_ref.at[pl.ds(route * 96 + half * 48, 48), pl.ds(column, width)]

    for half in range(2):
        for route in range(2):
            rows = (TOP, BOTTOM)[half]
            waits = ((3, 4), (2, 5))[half]
            for index in waits:
                late[route][index].wait_recv()
            own = spot(route, half, first_at[route], second_at[route], 256)
            own[...] = widened_sum(
                first_sum.at[route, second_at[route], rows],
                second_recv.at[route, 2 + half],
                second_recv.at[route, 4 + half],
            )

    def spread(stage, places, piece):
        started = []
        for route in range(2):
            plus, minus = (places[route][1], places[route][3])
            started.append(
                [
                    launch(piece(route, 0, 0), piece(route, 0, 0), stage, route, 0, plus),
                    launch(piece(route, 1, 0), piece(route, 1, 0), stage, route, 1, minus),
                    launch(piece(route, 1, 0), piece(route, 1, 0), stage, route, 2, plus),
                    launch(piece(route, 0, 0), piece(route, 0, 0), stage, route, 3, minus),
                ]
            )
        for route in range(2):
            plus, minus = (places[route][1], places[route][3])
            started[route][0].wait_recv()
            started[route].append(
                launch(piece(route, 0, 3), piece(route, 0, 3), stage, route, 4, plus)
            )
            started[route][1].wait_recv()
            started[route].append(
                launch(piece(route, 1, 1), piece(route, 1, 1), stage, route, 5, minus)
            )
        for route in range(2):
            for index in range(2, 6):
                started[route][index].wait_recv()

    def near(route, half, k):
        return spot(route, half, first_at[route], (second_at[route] + k) % 4, 256)

    def far(route, half, k):
        return spot(route, half, (first_at[route] + k) % 4, 0, 1024)

    spread(2, seconds, near)
    spread(3, firsts, far)
    for copy in count_copies:
        copy.wait_recv()
    everyone = count_buf[0]
    for d in range(1, 8):
        everyone = everyone + count_buf[d]
    total_ref[0] = jnp.sum(everyone[0:1, 0:1]).astype(jnp.int32)
    for copy in copies + count_copies + [swap, square_swap]:
        copy.wait_send()


def layer(*operands):
    return pl.pallas_call(
        layer_kernel,
        out_shape=(
            jax.ShapeDtypeStruct((192, 4096), jnp.bfloat16),
            jax.ShapeDtypeStruct((24, 512, 128), jnp.bfloat16),
            jax.ShapeDtypeStruct((3, 24, 512), jnp.bfloat16),
            jax.ShapeDtypeStruct((3, 24, 128), jnp.bfloat16),
            jax.ShapeDtypeStruct((1,), jnp.int32),
        ),
        in_specs=[pl.BlockSpec(memory_space=pltpu.HBM)] * 20,
        out_specs=(pl.BlockSpec(memory_space=pltpu.VMEM),) * 4
        + (pl.BlockSpec(memory_space=pltpu.SMEM),),
        scratch_shapes=[
            pltpu.VMEM((192, 4096), jnp.bfloat16),
            pltpu.VMEM((1, 4096), jnp.float32),
            pltpu.VMEM((32768, 128), jnp.bfloat16),
            pltpu.VMEM((4096, 128), jnp.bfloat16),
            pltpu.VMEM((8, 4096), jnp.bfloat16),
            pltpu.VMEM((4, 512), jnp.bfloat16),
            pltpu.VMEM((512,), jnp.bfloat16),
            pltpu.VMEM((4, 128), jnp.bfloat16),
            pltpu.VMEM((128,), jnp.bfloat16),
            pltpu.VMEM((1, 8), jnp.float32),
            pltpu.VMEM((1, 8), jnp.float32),
            pltpu.VMEM((1, 8), jnp.float32),
            pltpu.VMEM((1, 512), jnp.float32),
            pltpu.VMEM((512, 4096), jnp.bfloat16),
            pltpu.VMEM((24, 512, 128), jnp.bfloat16),
            pltpu.VMEM((3, 24, 512), jnp.bfloat16),
            pltpu.VMEM((3, 24, 128), jnp.bfloat16),
            pltpu.VMEM((1, 24), jnp.int32),
            pltpu.VMEM((1, 24), jnp.int32),
            pltpu.VMEM((1, 24), jnp.int32),
            pltpu.VMEM((192, 4096), jnp.bfloat16),
            pltpu.VMEM((2048, 128), jnp.float32),
            pltpu.VMEM((2048, 128), jnp.float32),
            pltpu.VMEM((8, 192, 128), jnp.float32),
            pltpu.VMEM((192, 128), jnp.float32),
            pltpu.VMEM((192, 128), jnp.float32),
            pltpu.VMEM((2, 8, 24, 128), jnp.float32),
            pltpu.VMEM((192, 128), jnp.float32),
            pltpu.VMEM((4, 192, 128), jnp.float32),
            pltpu.VMEM((1248, 128), jnp.float32),
            pltpu.VMEM((1248, 512), jnp.float32),
            pltpu.VMEM((8, 24, 128), jnp.float32),
            pltpu.VMEM((192, 512), jnp.float32),
            pltpu.VMEM((512, 192), jnp.bfloat16),
            pltpu.VMEM((192, 128), jnp.float32),
            pltpu.VMEM((4, 192, 128), jnp.float32),
            pltpu.VMEM((192, 512), jnp.bfloat16),
            pltpu.VMEM((8, 24, 128), jnp.float32),
            pltpu.VMEM((24, 128), jnp.float32),
            pltpu.VMEM((24, 128), jnp.float32),
            pltpu.VMEM((192, 128), jnp.float32),
            pltpu.VMEM((2, 4, 96, 1024), jnp.bfloat16),
            pltpu.VMEM((2, 6, 48, 1024), jnp.bfloat16),
            pltpu.VMEM((2, 2, 48, 1024), jnp.bfloat16),
            pltpu.VMEM((2, 4, 96, 256), jnp.bfloat16),
            pltpu.VMEM((2, 6, 48, 256), jnp.bfloat16),
            pltpu.VMEM((2, 2, 48, 256), jnp.bfloat16),
            pltpu.VMEM((8, 8, 128), jnp.float32),
            pltpu.SemaphoreType.DMA((4, 2, 6)),
            pltpu.SemaphoreType.DMA((4, 2, 6)),
            pltpu.SemaphoreType.DMA((8,)),
            pltpu.SemaphoreType.DMA((8,)),
            pltpu.SemaphoreType.DMA((4,)),
            pltpu.SemaphoreType.DMA((20,)),
            pltpu.SemaphoreType.DMA((4,)),
        ],
        compiler_params=pltpu.CompilerParams(
            collective_id=0, has_side_effects=True, vmem_limit_bytes=38 * 1024 * 1024
        ),
    )(*(pltpu.with_memory_space_constraint(operand, pltpu.HBM) for operand in operands))


def place_kernel(*refs):
    sources, targets, sems = refs[:4], refs[4:8], refs[8]
    copies = [
        pltpu.make_async_copy(source, target, sems.at[index])
        for index, (source, target) in enumerate(zip(sources, targets))
    ]
    for copy in copies:
        copy.start()
    for copy in copies:
        copy.wait()


def place(*arrays):
    return pl.pallas_call(
        place_kernel,
        out_shape=tuple(jax.ShapeDtypeStruct(a.shape, a.dtype) for a in arrays),
        in_specs=[pl.BlockSpec(memory_space=pltpu.VMEM)] * 4,
        out_specs=(pl.BlockSpec(memory_space=pltpu.HBM),) * 4,
        scratch_shapes=[pltpu.SemaphoreType.DMA((4,))],
        compiler_params=pltpu.CompilerParams(vmem_limit_bytes=16 * 1024 * 1024),
    )(*arrays)


def local(
    tokens,
    norm_gain,
    in_weight,
    group_weight,
    step_weight,
    value_kernel,
    value_offset,
    group_kernel,
    group_offset,
    step_bias,
    decay_rate,
    skip_gain,
    out_gain,
    out_weight,
    scan_state,
    value_cache,
    group_cache,
    accepted,
    draft_lengths,
    live_flags,
):
    woven = in_weight.reshape(4096, 2, 4, 128).transpose(0, 2, 1, 3).reshape(32768, 128)
    rows, kept_state, value_kept, group_kept, total = layer(
        tokens.reshape(192, 4096),
        norm_gain.reshape(1, 4096),
        woven,
        group_weight,
        step_weight.T,
        value_kernel,
        value_offset,
        group_kernel,
        group_offset,
        step_bias.reshape(1, 8),
        decay_rate.reshape(1, 8),
        skip_gain.reshape(1, 8),
        out_gain.reshape(1, 512),
        out_weight,
        scan_state.reshape(24, 512, 128),
        value_cache.transpose(1, 0, 2),
        group_cache.transpose(1, 0, 2),
        accepted.reshape(1, 24),
        draft_lengths.reshape(1, 24),
        live_flags.reshape(1, 24),
    )
    rows, kept_state, value_kept, group_kept = place(rows, kept_state, value_kept, group_kept)
    return (
        rows.reshape(24, 8, 4096),
        kept_state.reshape(24, 8, 64, 128),
        value_kept.transpose(1, 0, 2),
        group_kept.transpose(1, 0, 2),
        total,
    )


def solution(mesh):
    in_specs = (
        P(DP, None, None),
        P(),
        P(None, None, "tensor"),
        P(None, "tensor"),
        P(None, "tensor"),
        P(None, "tensor"),
        P("tensor"),
        P(None, "tensor"),
        P("tensor"),
        P("tensor"),
        P("tensor"),
        P("tensor"),
        P("tensor"),
        P("tensor", None),
        P(DP, "tensor", None, None),
        P(DP, None, "tensor"),
        P(DP, None, "tensor"),
        P(DP),
        P(DP),
        P(DP),
    )
    out_specs = (
        P(DP, None, None),
        P(DP, "tensor", None, None),
        P(DP, None, "tensor"),
        P(DP, None, "tensor"),
        P(),
    )
    return jax.shard_map(local, mesh=mesh, in_specs=in_specs, out_specs=out_specs, check_vma=False)
```

```python
import jax
import jax.numpy as jnp
from jax import lax
from jax.experimental import pallas as pl
from jax.experimental.pallas import tpu as pltpu
from jax.sharding import PartitionSpec as P

DP = "dp"


EPSILON = 1e-05


def swapped(value, axis, distance):
    mask = 2**distance
    pairs = [(source, source ^ mask) for source in range(lax.axis_size(axis))]
    return lax.ppermute(value, axis, pairs)


MESH = pl.DeviceIdType.MESH
TOP, BOTTOM = pl.ds(0, 48), pl.ds(48, 48)


def ring_places():
    tensor = lax.axis_index("tensor")
    z, y = tensor // 4, tensor % 4
    along_y = [{"tensor": z * 4 + (y + d) % 4} for d in range(4)]
    along_z = [{"tensor": ((z + d) % 4) * 4 + y} for d in range(4)]
    return (z, y, along_z, along_y)


def remote(src, dst, sems, place):
    send, recv, index = sems
    return pltpu.make_async_remote_copy(
        src_ref=src,
        dst_ref=dst,
        send_sem=send.at[index],
        recv_sem=recv.at[index],
        device_id=place,
        device_id_type=MESH,
    )


def widened_sum(*refs):
    total = refs[0][...].astype(jnp.float32)
    for ref in refs[1:]:
        total = total + ref[...].astype(jnp.float32)
    return total.astype(jnp.bfloat16)


def layer_kernel(
    tokens_in,
    gain_in,
    in_weight_in,
    group_weight_in,
    step_weight_in,
    value_kernel_in,
    value_offset_in,
    group_kernel_in,
    group_offset_in,
    step_bias_in,
    decay_rate_in,
    skip_gain_in,
    out_gain_in,
    out_weight_in,
    state_in,
    value_cache_in,
    group_cache_in,
    accepted_in,
    lengths_in,
    live_in,
    out_ref,
    kept_ref,
    value_kept,
    group_kept,
    total_ref,
    tokens,
    gain,
    in_weight,
    group_weight,
    step_weight,
    value_kernel,
    value_offset,
    group_kernel,
    group_offset,
    step_bias,
    decay_rate,
    skip_gain,
    out_gain,
    out_weight,
    state,
    value_cache,
    group_cache,
    accepted,
    lengths,
    live,
    normed,
    spread_a,
    spread_b,
    inner,
    group_rows,
    step_rows,
    maps,
    map_rows,
    carried,
    small,
    mixing,
    decay_kept,
    weighted,
    turned,
    input_rows,
    gated_rows,
    rows_ref,
    squares,
    square_own,
    square_other,
    scale_rows,
    first_products,
    partial,
    first_recv,
    first_mix,
    gathered,
    count_buf,
    send_sems,
    recv_sems,
    count_send,
    count_recv,
    swap_sems,
    load_sems,
    token_sems,
    chunk_sems,
):
    z, y, along_z, along_y = ring_places()
    dp = lax.axis_index("dp")
    parity = y % 2
    mate = {"tensor": z * 4 + (y + 1 - 2 * parity)}
    barrier = pltpu.get_barrier_semaphore()
    dp_peers = [{"dp": (dp + d) % 8} for d in range(1, 8)]
    ring_peers = [along_z[1], along_z[3], along_y[1], along_y[3]]
    for place in ring_peers + dp_peers:
        pl.semaphore_signal(barrier, inc=1, device_id=place, device_id_type=MESH)
    loads = {}

    def load(name, src, dst, index):
        loads[name] = pltpu.make_async_copy(src, dst, load_sems.at[index])
        loads[name].start()

    token_copies = []
    for index in range(4):
        rows = pl.ds(index * 48, 48)
        copy = pltpu.make_async_copy(tokens_in.at[rows], tokens.at[rows], token_sems.at[index])
        copy.start()
        token_copies.append(copy)
    load("gain", gain_in, gain, 1)
    load("step_weight", step_weight_in, step_weight, 4)
    load("group_weight", group_weight_in, group_weight.at[:, 0:128], 3)
    load("accepted", accepted_in, accepted, 17)
    load("lengths", lengths_in, lengths, 18)
    load("live", live_in, live, 19)
    load("group_cache", group_cache_in, group_cache, 16)
    load("group_kernel", group_kernel_in, group_kernel, 7)
    load("group_offset", group_offset_in, group_offset, 8)
    load("step_bias", step_bias_in, step_bias, 9)
    load("decay_rate", decay_rate_in, decay_rate, 10)
    load("skip_gain", skip_gain_in, skip_gain, 11)
    for index in range(4):
        rows = pl.ds(index * 8192, 8192)
        copy = pltpu.make_async_copy(in_weight_in.at[rows], in_weight.at[rows], chunk_sems.at[index])
        copy.start()
    load("value_cache", value_cache_in, value_cache, 15)
    load("value_kernel", value_kernel_in, value_kernel, 5)
    load("value_offset", value_offset_in, value_offset, 6)
    load("out_gain", out_gain_in, out_gain, 12)
    load("state", state_in, state, 14)
    load("out_weight", out_weight_in, out_weight, 13)
    def column(ref):
        square = lax.broadcasted_iota(jnp.int32, (24, 24), 0) == lax.broadcasted_iota(
            jnp.int32, (24, 24), 1
        )
        values = jnp.broadcast_to(ref[...].astype(jnp.float32), (24, 24))
        return jnp.sum(jnp.where(square, values, 0.0), axis=1, keepdims=True)

    loads["step_weight"].wait()
    for block in range(32):
        rows = slice(block * 128, (block + 1) * 128)
        group_weight[rows, 128:136] = jnp.transpose(
            step_weight[:, rows].astype(jnp.float32)
        ).astype(jnp.bfloat16)
    loads["gain"].wait()

    def normalize(block):
        rows = slice(block * 16, block * 16 + 16)
        total = jnp.zeros((16, 256), jnp.float32)
        for part in range(16):
            piece = tokens[rows, part * 256 : (part + 1) * 256].astype(jnp.float32)
            total = total + piece * piece
        mean = jnp.sum(total, axis=1, keepdims=True) / 4096.0
        scale = jnp.broadcast_to(lax.rsqrt(mean + EPSILON), (16, 256))
        for part in range(16):
            columns = slice(part * 256, (part + 1) * 256)
            piece = tokens[rows, columns].astype(jnp.float32)
            normed[rows, columns] = (piece * scale * gain[:, columns]).astype(jnp.bfloat16)

    for index in range(4):
        token_copies[index].wait()
        for block in range(3):
            normalize(index * 3 + block)
    loads["group_weight"].wait()
    product = jnp.dot(normed[...], group_weight[...], preferred_element_type=jnp.float32)
    group_rows[...] = product[:, 0:128]
    step_rows[...] = product[:, 128:256]
    for name in ("accepted", "lengths", "live", "group_cache", "group_kernel", "group_offset"):
        loads[name].wait()
    kept = column(accepted) * column(live)
    alive = column(live) == 1.0
    length_column = column(lengths)

    def sequence_of(cache, rows):
        early = [cache[t].astype(jnp.float32) for t in range(3)]
        return early + [rounded(piece) for piece in rows]

    def rounded(piece):
        return piece.astype(jnp.bfloat16).astype(jnp.float32)

    def convolved(sequence, taps, offset):
        out = []
        for s in range(8):
            total = offset
            for k in range(4):
                total = total + taps[k] * sequence[s + k]
            out.append(total / (1.0 + jnp.exp(-total)))
        return out

    def kept_rows(sequence, counts, t):
        chosen = sequence[t]
        for k in range(1, 9):
            chosen = jnp.where(counts == float(k), sequence[k + t], chosen)
        return chosen.astype(jnp.bfloat16)

    group_taps = [group_kernel[k : k + 1, :].astype(jnp.float32) for k in range(4)]
    group_sequence = sequence_of(
        group_cache, [group_rows[pl.ds(s, 24, stride=8), :] for s in range(8)]
    )
    own_maps = convolved(
        group_sequence, group_taps, group_offset[...].astype(jnp.float32).reshape(1, 128)
    )
    for s in range(8):
        maps[parity, s] = own_maps[s]
    pl.semaphore_wait(barrier, 11)
    swap = pltpu.make_async_remote_copy(
        src_ref=maps.at[parity],
        dst_ref=maps.at[parity],
        send_sem=swap_sems.at[0],
        recv_sem=swap_sems.at[1],
        device_id=mate,
        device_id_type=MESH,
    )
    swap.start()
    count_buf[0] = jnp.broadcast_to(jnp.sum(kept, axis=0, keepdims=True), (8, 128))
    count_copies = []
    for d in range(1, 8):
        copy = remote(count_buf.at[0], count_buf.at[d], (count_send, count_recv, d), dp_peers[d - 1])
        copy.start()
        count_copies.append(copy)
    for t in range(3):
        group_kept[t] = kept_rows(group_sequence, kept, t)

    for name in ("step_bias", "decay_rate", "skip_gain"):
        loads[name].wait()

    inner[...] = jnp.zeros_like(inner)

    def widen(start, spread):
        spread[...] = in_weight[pl.ds(pl.multiple_of(start * 4096, 4096), 4096), :].astype(
            jnp.float32
        )

    def multiply(start, spread):
        left = normed[:, pl.ds(pl.multiple_of(start * 512, 512), 512)]
        for part in range(2):
            for j in range(0, 4, 2):
                right = jnp.concatenate(
                    [
                        spread[pl.ds((j + i) * 2 + part, 512, stride=8), :].astype(jnp.bfloat16)
                        for i in range(2)
                    ],
                    axis=1,
                )
                product = jnp.dot(left, right, preferred_element_type=jnp.float32)
                for i in range(2):
                    inner[part * 4 + j + i] += product[:, i * 128 : (i + 1) * 128]

    def pair(index, carry):
        rows = pl.ds(pl.multiple_of(index * 8192, 8192), 8192)
        pltpu.make_async_copy(
            in_weight_in.at[rows], in_weight.at[rows], chunk_sems.at[index]
        ).wait()
        widen(2 * index, spread_a)
        multiply(2 * index, spread_a)
        widen(2 * index + 1, spread_b)
        multiply(2 * index + 1, spread_b)
        return carry

    lax.fori_loop(0, 4, pair, 0)

    steps, after = [], []
    running = None
    for s in range(8):
        raw = step_rows[pl.ds(s, 24, stride=8), 0:8] + step_bias[...]
        size = jnp.maximum(raw, 0.0) + jnp.log1p(jnp.exp(-jnp.abs(raw)))
        change = -size * decay_rate[...]
        running = change if running is None else running + change
        steps.append(size)
        after.append(running)
    prefix_kept = jnp.zeros_like(running)
    for s in range(8):
        prefix_kept = jnp.where(kept == float(s + 1), after[s], prefix_kept)
    for s in range(8):
        small[pl.ds((36 + s) * 24, 24), 0:8] = jnp.exp(after[s])
        small[pl.ds((44 + s) * 24, 24), 0:8] = (
            jnp.where(kept > float(s), jnp.exp(prefix_kept - after[s]), 0.0) * steps[s]
        )
    head_decay = jnp.exp(prefix_kept)
    for h in range(8):
        decay_kept[h] = jnp.broadcast_to(head_decay[:, h : h + 1], (24, 128))
    swap.wait_recv()
    for s in range(8):
        map_rows[pl.ds(s, 24, stride=8), :] = maps[1, s]
        input_rows[pl.ds(s * 24, 24), :] = maps[0, s]
        for j in range(s + 1):
            match = jnp.sum(maps[1, s] * maps[0, j], axis=1, keepdims=True)
            small[pl.ds((s * (s + 1) // 2 + j) * 24, 24), 0:8] = (
                jnp.exp(after[s] - after[j]) * steps[j] * match
            )
    hot = (
        lax.broadcasted_iota(jnp.int32, (8, 512), 1) // 64
        == lax.broadcasted_iota(jnp.int32, (8, 512), 0)
    ).astype(jnp.bfloat16)

    def expand(index, carry):
        rows = pl.ds(index * 416, 416)
        mixing[rows, :] = jnp.dot(
            small[rows, 0:8].astype(jnp.bfloat16), hot, preferred_element_type=jnp.float32
        )
        return carry

    for index in range(3):
        expand(index, 0)
    loads["state"].wait()

    def carry_over(index, carry):
        for i in range(12):
            request = index * 12 + i
            rows = pl.ds(pl.multiple_of(request * 8, 8), 8)
            product = lax.dot_general(
                map_rows[rows, :].astype(jnp.bfloat16),
                state[request],
                (((1,), (1,)), ((), ())),
                preferred_element_type=jnp.float32,
            )
            for block in range(4):
                carried[block, rows, :] = product[:, block * 128 : (block + 1) * 128]
        return carry

    lax.fori_loop(0, 2, carry_over, 0)
    for name in ("value_cache", "value_kernel", "value_offset", "out_gain"):
        loads[name].wait()

    offset_row = value_offset[...].astype(jnp.float32).reshape(1, 512)
    for block in range(4):
        columns = slice(block * 128, (block + 1) * 128)
        lane = lax.broadcasted_iota(jnp.int32, (8, 128), 1)
        skip = jnp.where(
            lane < 64,
            jnp.broadcast_to(skip_gain[:, 2 * block : 2 * block + 1], (8, 128)),
            jnp.broadcast_to(skip_gain[:, 2 * block + 1 : 2 * block + 2], (8, 128)),
        )
        taps = [value_kernel[k : k + 1, columns].astype(jnp.float32) for k in range(4)]
        offset = offset_row[:, columns]
        for tile in range(3):
            eight = pl.ds(tile * 8, 8)
            counts = kept[tile * 8 : tile * 8 + 8]
            sequence = [value_cache[t, eight, columns].astype(jnp.float32) for t in range(3)] + [
                rounded(inner[4 + block, pl.ds(tile * 64 + s, 8, stride=8), :])
                for s in range(8)
            ]
            for t in range(3):
                value_kept[t, eight, columns] = kept_rows(sequence, counts, t)
            values = convolved(sequence, taps, offset)
            for s in range(8):
                weighted[pl.ds(s * 24 + tile * 8, 8), columns] = (
                    mixing[pl.ds((44 + s) * 24 + tile * 8, 8), columns] * values[s]
                )
                total = (
                    mixing[pl.ds((36 + s) * 24 + tile * 8, 8), columns]
                    * carried[block, pl.ds(tile * 64 + s, 8, stride=8), :]
                    + skip * values[s]
                )
                for j in range(s + 1):
                    q = s * (s + 1) // 2 + j
                    total = total + mixing[pl.ds(q * 24 + tile * 8, 8), columns] * values[j]
                gate = rounded(inner[block, pl.ds(tile * 64 + s, 8, stride=8), :])
                gated = total * (gate / (1.0 + jnp.exp(-gate)))
                square = gated * gated
                if block:
                    square = square + squares[s, eight]
                squares[s, eight] = square
                valid = jnp.logical_and(
                    alive[tile * 8 : tile * 8 + 8],
                    length_column[tile * 8 : tile * 8 + 8] > float(s),
                )
                gated_rows[block, pl.ds(tile * 64 + s, 8, stride=8), :] = jnp.where(
                    valid, gated * out_gain[:, columns], 0.0
                )
    lanes = lax.broadcasted_iota(jnp.int32, (24, 128), 1)
    own = jnp.zeros((24, 128), jnp.float32)
    for s in range(8):
        own = jnp.where(lanes == s, jnp.sum(squares[s], axis=1, keepdims=True), own)
    square_own[...] = own
    square_swap = pltpu.make_async_remote_copy(
        src_ref=square_own,
        dst_ref=square_other,
        send_sem=swap_sems.at[2],
        recv_sem=swap_sems.at[3],
        device_id=mate,
        device_id_type=MESH,
    )
    square_swap.start()
    for block in range(4):
        rows_ref[:, block * 128 : (block + 1) * 128] = gated_rows[block].astype(jnp.bfloat16)
    loads["out_weight"].wait()
    firsts = [along_y, along_z]
    seconds = [along_z, along_y]
    first_at = [y, z]
    second_at = [z, y]
    copies = []

    def launch(src, dst, stage, route, chunk, slot, place):
        copy = remote(src, dst, (send_sems, recv_sems, (stage, route, chunk, slot)), place)
        copy.start()
        copies.append(copy)
        return copy

    def product_of(route, step, chunk):
        base = ((first_at[route] + step) % 4) * 1024 + chunk * 512
        return jnp.dot(
            rows_ref[pl.ds(route * 96, 96), :],
            out_weight[:, pl.ds(pl.multiple_of(base, 512), 512)],
            preferred_element_type=jnp.float32,
        )

    def settle(route, step, chunk, product):
        scale = scale_rows[pl.ds(route * 96, 96), :]
        partial[route, step, chunk] = (
            product * jnp.concatenate([scale] * 4, axis=1)
        ).astype(jnp.bfloat16)

    for step in (2, 1, 3):
        for route in range(2):
            first_products[route, step - 1] = product_of(route, step, 0)
    turned[...] = jnp.transpose(weighted[...]).astype(jnp.bfloat16)
    square_swap.wait_recv()
    scales = lax.rsqrt((square_own[...] + square_other[...]) / 1024.0 + EPSILON)
    for s in range(8):
        scale_rows[pl.ds(s, 24, stride=8), :] = jnp.broadcast_to(scales[:, s : s + 1], (24, 128))

    def keep_states(first, last):
        owner = lax.rem(lax.broadcasted_iota(jnp.int32, (192, 128), 0), 24)

        def keep(index, carry):
            inputs = input_rows[...]
            right = jnp.concatenate(
                [
                    jnp.where(owner == 2 * index + i, inputs, 0.0).astype(jnp.bfloat16)
                    for i in range(2)
                ],
                axis=1,
            )
            for h in range(8):
                update = jnp.dot(
                    turned[h * 64 : (h + 1) * 64, :], right, preferred_element_type=jnp.float32
                )
                for i in range(2):
                    request = 2 * index + i
                    decay = decay_kept[h, pl.ds(request, 1), :]
                    before = state[request, h * 64 : (h + 1) * 64, :].astype(jnp.float32)
                    kept_ref[request, h * 64 : (h + 1) * 64, :] = (
                        decay * before + update[:, i * 128 : (i + 1) * 128]
                    ).astype(jnp.bfloat16)
            return carry

        lax.fori_loop(first, last, keep, 0)

    held = {}
    for chunk in range(2):
        for step in (2, 1, 3):
            for route in range(2):
                product = first_products[route, step - 1] if chunk == 0 else product_of(route, step, 1)
                settle(route, step, chunk, product)
                unit = partial.at[route, step, chunk]
                landing = first_recv.at[route, chunk]
                plus, minus = (firsts[route][1], firsts[route][3])
                sends = {
                    2: ((TOP, 0, plus), (BOTTOM, 1, minus)),
                    1: ((BOTTOM, 3, plus),),
                    3: ((TOP, 4, minus),),
                }[step]
                for rows, slot, place in sends:
                    held[route, chunk, slot] = launch(
                        unit.at[rows], landing.at[slot], 0, route, chunk, slot, place
                    )
    for chunk in range(2):
        for route in range(2):
            settle(route, 0, chunk, product_of(route, 0, chunk))
    for chunk in range(2):
        for half in range(2):
            for route in range(2):
                rows = (TOP, BOTTOM)[half]
                landing = first_recv.at[route, chunk]
                held[route, chunk, half].wait_recv()
                mix = first_mix.at[route, chunk, half]
                mix[...] = widened_sum(
                    landing.at[half], partial.at[route, (1, 3)[half], chunk, rows]
                )
                slot = (2, 5)[half]
                held[route, chunk, slot] = launch(
                    mix, landing.at[slot], 0, route, chunk, slot, firsts[route][(1, 3)[half]]
                )

    def spread_start(stage, places, piece, chunk):
        started = []
        for route in range(2):
            plus, minus = (places[route][1], places[route][3])
            started.append([])
            for half, slot, place in ((0, 0, plus), (1, 1, minus), (1, 2, plus), (0, 3, minus)):
                own = piece(route, chunk, half, 0)
                started[route].append(launch(own, own, stage, route, chunk, slot, place))
        return started

    def spread_forward(started, stage, places, piece, chunk):
        for half in range(2):
            for route in range(2):
                started[route][half].wait_recv()
                passed = piece(route, chunk, half, (3, 1)[half])
                started[route].append(
                    launch(
                        passed, passed, stage, route, chunk, 4 + half, places[route][(1, 3)[half]]
                    )
                )

    def spread_finish(started):
        for route in range(2):
            for index in range(2, 6):
                started[route][index].wait_recv()

    def middle(route, chunk, half, k):
        return gathered.at[route, chunk, (second_at[route] + k) % 4, (TOP, BOTTOM)[half]]

    def spot(route, chunk, half, k):
        column = ((first_at[route] + k) % 4) * 1024 + chunk * 512
        return out_ref.at[
            pl.ds(route * 96 + half * 48, 48), pl.ds(pl.multiple_of(column, 512), 512)
        ]

    inner_spread = []
    for chunk in range(2):
        for half in range(2):
            for route in range(2):
                rows = (TOP, BOTTOM)[half]
                for slot in ((4, 2), (3, 5))[half]:
                    held[route, chunk, slot].wait_recv()
                own = middle(route, chunk, half, 0)
                own[...] = widened_sum(
                    partial.at[route, 0, chunk, rows],
                    first_recv.at[route, chunk, 2 + half],
                    first_recv.at[route, chunk, 4 + half],
                )
        inner_spread.append(spread_start(1, seconds, middle, chunk))
    keep_states(0, 6)
    for chunk in range(2):
        spread_forward(inner_spread[chunk], 1, seconds, middle, chunk)
    outer_spread = []
    for chunk in range(2):
        spread_finish(inner_spread[chunk])
        for half in range(2):
            for route in range(2):
                rows = (TOP, BOTTOM)[half]
                own = spot(route, chunk, half, 0)
                own[...] = widened_sum(*(gathered.at[route, chunk, b, rows] for b in range(4)))
        outer_spread.append(spread_start(2, firsts, spot, chunk))
    keep_states(6, 12)
    for chunk in range(2):
        spread_forward(outer_spread[chunk], 2, firsts, spot, chunk)
    for chunk in range(2):
        spread_finish(outer_spread[chunk])
    for copy in count_copies:
        copy.wait_recv()
    everyone = count_buf[0]
    for d in range(1, 8):
        everyone = everyone + count_buf[d]
    total_ref[0] = jnp.sum(everyone[0:1, 0:1]).astype(jnp.int32)
    for copy in copies + count_copies + [swap, square_swap]:
        copy.wait_send()


def layer(*operands):
    return pl.pallas_call(
        layer_kernel,
        out_shape=(
            jax.ShapeDtypeStruct((192, 4096), jnp.bfloat16),
            jax.ShapeDtypeStruct((24, 512, 128), jnp.bfloat16),
            jax.ShapeDtypeStruct((3, 24, 512), jnp.bfloat16),
            jax.ShapeDtypeStruct((3, 24, 128), jnp.bfloat16),
            jax.ShapeDtypeStruct((1,), jnp.int32),
        ),
        in_specs=[pl.BlockSpec(memory_space=pltpu.HBM)] * 20,
        out_specs=(pl.BlockSpec(memory_space=pltpu.VMEM),) * 4
        + (pl.BlockSpec(memory_space=pltpu.SMEM),),
        scratch_shapes=[
            pltpu.VMEM((192, 4096), jnp.bfloat16),
            pltpu.VMEM((1, 4096), jnp.float32),
            pltpu.VMEM((32768, 128), jnp.bfloat16),
            pltpu.VMEM((4096, 256), jnp.bfloat16),
            pltpu.VMEM((8, 4096), jnp.bfloat16),
            pltpu.VMEM((4, 512), jnp.bfloat16),
            pltpu.VMEM((512,), jnp.bfloat16),
            pltpu.VMEM((4, 128), jnp.bfloat16),
            pltpu.VMEM((128,), jnp.bfloat16),
            pltpu.VMEM((1, 8), jnp.float32),
            pltpu.VMEM((1, 8), jnp.float32),
            pltpu.VMEM((1, 8), jnp.float32),
            pltpu.VMEM((1, 512), jnp.float32),
            pltpu.VMEM((512, 4096), jnp.bfloat16),
            pltpu.VMEM((24, 512, 128), jnp.bfloat16),
            pltpu.VMEM((3, 24, 512), jnp.bfloat16),
            pltpu.VMEM((3, 24, 128), jnp.bfloat16),
            pltpu.VMEM((1, 24), jnp.int32),
            pltpu.VMEM((1, 24), jnp.int32),
            pltpu.VMEM((1, 24), jnp.int32),
            pltpu.VMEM((192, 4096), jnp.bfloat16),
            pltpu.VMEM((4096, 128), jnp.float32),
            pltpu.VMEM((4096, 128), jnp.float32),
            pltpu.VMEM((8, 192, 128), jnp.float32),
            pltpu.VMEM((192, 128), jnp.float32),
            pltpu.VMEM((192, 128), jnp.float32),
            pltpu.VMEM((2, 8, 24, 128), jnp.float32),
            pltpu.VMEM((192, 128), jnp.float32),
            pltpu.VMEM((4, 192, 128), jnp.float32),
            pltpu.VMEM((1248, 128), jnp.float32),
            pltpu.VMEM((1248, 512), jnp.float32),
            pltpu.VMEM((8, 24, 128), jnp.float32),
            pltpu.VMEM((192, 512), jnp.float32),
            pltpu.VMEM((512, 192), jnp.bfloat16),
            pltpu.VMEM((192, 128), jnp.float32),
            pltpu.VMEM((4, 192, 128), jnp.float32),
            pltpu.VMEM((192, 512), jnp.bfloat16),
            pltpu.VMEM((8, 24, 128), jnp.float32),
            pltpu.VMEM((24, 128), jnp.float32),
            pltpu.VMEM((24, 128), jnp.float32),
            pltpu.VMEM((192, 128), jnp.float32),
            pltpu.VMEM((2, 3, 96, 512), jnp.float32),
            pltpu.VMEM((2, 4, 2, 96, 512), jnp.bfloat16),
            pltpu.VMEM((2, 2, 6, 48, 512), jnp.bfloat16),
            pltpu.VMEM((2, 2, 2, 48, 512), jnp.bfloat16),
            pltpu.VMEM((2, 2, 4, 96, 512), jnp.bfloat16),
            pltpu.VMEM((8, 8, 128), jnp.float32),
            pltpu.SemaphoreType.DMA((3, 2, 2, 6)),
            pltpu.SemaphoreType.DMA((3, 2, 2, 6)),
            pltpu.SemaphoreType.DMA((8,)),
            pltpu.SemaphoreType.DMA((8,)),
            pltpu.SemaphoreType.DMA((4,)),
            pltpu.SemaphoreType.DMA((20,)),
            pltpu.SemaphoreType.DMA((4,)),
            pltpu.SemaphoreType.DMA((4,)),
        ],
        compiler_params=pltpu.CompilerParams(
            collective_id=0, has_side_effects=True, vmem_limit_bytes=44 * 1024 * 1024
        ),
    )(*(pltpu.with_memory_space_constraint(operand, pltpu.HBM) for operand in operands))


def place_kernel(*refs):
    sources, targets, sems = refs[:4], refs[4:8], refs[8]
    copies = [
        pltpu.make_async_copy(source, target, sems.at[index])
        for index, (source, target) in enumerate(zip(sources, targets))
    ]
    for copy in copies:
        copy.start()
    for copy in copies:
        copy.wait()


def place(*arrays):
    return pl.pallas_call(
        place_kernel,
        out_shape=tuple(jax.ShapeDtypeStruct(a.shape, a.dtype) for a in arrays),
        in_specs=[pl.BlockSpec(memory_space=pltpu.VMEM)] * 4,
        out_specs=(pl.BlockSpec(memory_space=pltpu.HBM),) * 4,
        scratch_shapes=[pltpu.SemaphoreType.DMA((4,))],
        compiler_params=pltpu.CompilerParams(vmem_limit_bytes=16 * 1024 * 1024),
    )(*arrays)


def local(
    tokens,
    norm_gain,
    in_weight,
    group_weight,
    step_weight,
    value_kernel,
    value_offset,
    group_kernel,
    group_offset,
    step_bias,
    decay_rate,
    skip_gain,
    out_gain,
    out_weight,
    scan_state,
    value_cache,
    group_cache,
    accepted,
    draft_lengths,
    live_flags,
):
    woven = in_weight.reshape(4096, 2, 4, 128).transpose(0, 2, 1, 3).reshape(32768, 128)
    rows, kept_state, value_kept, group_kept, total = layer(
        tokens.reshape(192, 4096),
        norm_gain.reshape(1, 4096),
        woven,
        group_weight,
        step_weight.T,
        value_kernel,
        value_offset,
        group_kernel,
        group_offset,
        step_bias.reshape(1, 8),
        decay_rate.reshape(1, 8),
        skip_gain.reshape(1, 8),
        out_gain.reshape(1, 512),
        out_weight,
        scan_state.reshape(24, 512, 128),
        value_cache.transpose(1, 0, 2),
        group_cache.transpose(1, 0, 2),
        accepted.reshape(1, 24),
        draft_lengths.reshape(1, 24),
        live_flags.reshape(1, 24),
    )
    rows, kept_state, value_kept, group_kept = place(rows, kept_state, value_kept, group_kept)
    return (
        rows.reshape(24, 8, 4096),
        kept_state.reshape(24, 8, 64, 128),
        value_kept.transpose(1, 0, 2),
        group_kept.transpose(1, 0, 2),
        total,
    )


def solution(mesh):
    in_specs = (
        P(DP, None, None),
        P(),
        P(None, None, "tensor"),
        P(None, "tensor"),
        P(None, "tensor"),
        P(None, "tensor"),
        P("tensor"),
        P(None, "tensor"),
        P("tensor"),
        P("tensor"),
        P("tensor"),
        P("tensor"),
        P("tensor"),
        P("tensor", None),
        P(DP, "tensor", None, None),
        P(DP, None, "tensor"),
        P(DP, None, "tensor"),
        P(DP),
        P(DP),
        P(DP),
    )
    out_specs = (
        P(DP, None, None),
        P(DP, "tensor", None, None),
        P(DP, None, "tensor"),
        P(DP, None, "tensor"),
        P(),
    )
    return jax.shard_map(local, mesh=mesh, in_specs=in_specs, out_specs=out_specs, check_vma=False)
```

```python
import jax
import jax.numpy as jnp
from jax import lax
from jax.experimental import pallas as pl
from jax.experimental.pallas import tpu as pltpu
from jax.sharding import PartitionSpec as P

DP = "dp"


EPSILON = 1e-05


def swapped(value, axis, distance):
    mask = 2**distance
    pairs = [(source, source ^ mask) for source in range(lax.axis_size(axis))]
    return lax.ppermute(value, axis, pairs)


MESH = pl.DeviceIdType.MESH
HALVES = (pl.ds(0, 512), pl.ds(512, 512))


def ring_places():
    tensor = lax.axis_index("tensor")
    z, y = tensor // 4, tensor % 4
    along_y = [{"tensor": z * 4 + (y + d) % 4} for d in range(4)]
    along_z = [{"tensor": ((z + d) % 4) * 4 + y} for d in range(4)]
    return (z, y, along_z, along_y)


def remote(src, dst, send, recv, place):
    return pltpu.make_async_remote_copy(
        src_ref=src,
        dst_ref=dst,
        send_sem=send,
        recv_sem=recv,
        device_id=place,
        device_id_type=MESH,
    )


def widened_sum(*refs):
    total = refs[0][...].astype(jnp.float32)
    for ref in refs[1:]:
        total = total + ref[...].astype(jnp.float32)
    return total.astype(jnp.bfloat16)


def layer_kernel(
    tokens_in,
    gain_in,
    in_weight_in,
    group_weight_in,
    step_weight_in,
    value_kernel_in,
    value_offset_in,
    group_kernel_in,
    group_offset_in,
    step_bias_in,
    decay_rate_in,
    skip_gain_in,
    out_gain_in,
    out_weight_in,
    state_in,
    value_cache_in,
    group_cache_in,
    accepted_in,
    lengths_in,
    live_in,
    out_ref,
    kept_ref,
    value_kept,
    group_kept,
    total_ref,
    tokens,
    gain,
    in_weight,
    group_weight,
    step_weight,
    value_kernel,
    value_offset,
    group_kernel,
    group_offset,
    step_bias,
    decay_rate,
    skip_gain,
    out_gain,
    out_weight,
    state,
    value_cache,
    group_cache,
    accepted,
    lengths,
    live,
    normed,
    spread_a,
    spread_b,
    inner,
    group_rows,
    step_rows,
    maps,
    map_rows,
    carried,
    small,
    mixing,
    decay_kept,
    weighted,
    turned,
    input_rows,
    gated_rows,
    rows_ref,
    squares,
    square_own,
    square_other,
    scale_rows,
    first_products,
    partial,
    first_recv,
    first_mix,
    gathered,
    count_buf,
    total_own,
    send_sems,
    recv_sems,
    count_sems,
    swap_sems,
    load_sems,
    token_sems,
    chunk_sems,
):
    z, y, along_z, along_y = ring_places()
    dp = lax.axis_index("dp")
    parity = y % 2
    mate = {"tensor": z * 4 + (y + 1 - 2 * parity)}
    barrier = pltpu.get_barrier_semaphore()
    dp_peers = [{"dp": (dp + d) % 8} for d in range(1, 8)]
    ring_peers = [along_z[1], along_z[3], along_y[1], along_y[3]]
    for place in ring_peers + dp_peers:
        pl.semaphore_signal(barrier, inc=1, device_id=place, device_id_type=MESH)
    loads = {}

    def load(name, src, dst, index):
        loads[name] = pltpu.make_async_copy(src, dst, load_sems.at[index])
        loads[name].start()

    token_copies = []
    for index in range(4):
        rows = pl.ds(index * 48, 48)
        copy = pltpu.make_async_copy(tokens_in.at[rows], tokens.at[rows], token_sems.at[index])
        copy.start()
        token_copies.append(copy)
    load("gain", gain_in, gain, 1)
    load("step_weight", step_weight_in, step_weight, 4)
    load("group_weight", group_weight_in, group_weight.at[:, 0:128], 3)
    load("accepted", accepted_in, accepted, 17)
    load("lengths", lengths_in, lengths, 18)
    load("live", live_in, live, 19)
    load("group_cache", group_cache_in, group_cache, 16)
    load("group_kernel", group_kernel_in, group_kernel, 7)
    load("group_offset", group_offset_in, group_offset, 8)
    load("step_bias", step_bias_in, step_bias, 9)
    load("decay_rate", decay_rate_in, decay_rate, 10)
    load("skip_gain", skip_gain_in, skip_gain, 11)
    def load_chunk(index):
        rows = pl.ds(index * 8192, 8192)
        pltpu.make_async_copy(in_weight_in.at[rows], in_weight.at[rows], chunk_sems.at[index]).start()

    def column(ref):
        square = lax.broadcasted_iota(jnp.int32, (24, 24), 0) == lax.broadcasted_iota(
            jnp.int32, (24, 24), 1
        )
        values = jnp.broadcast_to(ref[...].astype(jnp.float32), (24, 24))
        return jnp.sum(jnp.where(square, values, 0.0), axis=1, keepdims=True)

    loads["step_weight"].wait()
    for block in range(32):
        rows = slice(block * 128, (block + 1) * 128)
        group_weight[rows, 128:136] = jnp.transpose(
            step_weight[:, rows].astype(jnp.float32)
        ).astype(jnp.bfloat16)
    loads["gain"].wait()

    def normalize(block):
        rows = slice(block * 16, block * 16 + 16)
        total = jnp.zeros((16, 256), jnp.float32)
        for part in range(16):
            piece = tokens[rows, part * 256 : (part + 1) * 256].astype(jnp.float32)
            total = total + piece * piece
        mean = jnp.sum(total, axis=1, keepdims=True) / 4096.0
        scale = jnp.broadcast_to(lax.rsqrt(mean + EPSILON), (16, 256))
        for part in range(16):
            columns = slice(part * 256, (part + 1) * 256)
            piece = tokens[rows, columns].astype(jnp.float32)
            normed[rows, columns] = (piece * scale * gain[:, columns]).astype(jnp.bfloat16)

    for index in range(4):
        token_copies[index].wait()
        if index in (1, 3):
            load_chunk(index - 1)
            load_chunk(index)
        for block in range(3):
            normalize(index * 3 + block)
    load("value_cache", value_cache_in, value_cache, 15)
    load("value_kernel", value_kernel_in, value_kernel, 5)
    load("value_offset", value_offset_in, value_offset, 6)
    load("out_gain", out_gain_in, out_gain, 12)
    load("state", state_in, state, 14)
    load("out_weight", out_weight_in, out_weight, 13)
    loads["group_weight"].wait()
    product = jnp.dot(normed[...], group_weight[...], preferred_element_type=jnp.float32)
    group_rows[...] = product[:, 0:128]
    step_rows[...] = product[:, 128:256]
    for name in ("accepted", "lengths", "live", "group_cache", "group_kernel", "group_offset"):
        loads[name].wait()
    kept = column(accepted) * column(live)
    alive = column(live) == 1.0
    length_column = column(lengths)

    def sequence_of(cache, rows):
        early = [cache[t].astype(jnp.float32) for t in range(3)]
        return early + [rounded(piece) for piece in rows]

    def rounded(piece):
        return piece.astype(jnp.bfloat16).astype(jnp.float32)

    def convolved(sequence, taps, offset):
        out = []
        for s in range(8):
            total = offset
            for k in range(4):
                total = total + taps[k] * sequence[s + k]
            out.append(total / (1.0 + jnp.exp(-total)))
        return out

    def kept_rows(sequence, counts, t):
        chosen = sequence[t]
        for k in range(1, 9):
            chosen = jnp.where(counts == float(k), sequence[k + t], chosen)
        return chosen.astype(jnp.bfloat16)

    group_taps = [group_kernel[k : k + 1, :].astype(jnp.float32) for k in range(4)]
    group_sequence = sequence_of(
        group_cache, [group_rows[pl.ds(s, 24, stride=8), :] for s in range(8)]
    )
    own_maps = convolved(
        group_sequence, group_taps, group_offset[...].astype(jnp.float32).reshape(1, 128)
    )
    for s in range(8):
        maps[parity, s] = own_maps[s]
    pl.semaphore_wait(barrier, 11)
    swap = pltpu.make_async_remote_copy(
        src_ref=maps.at[parity],
        dst_ref=maps.at[parity],
        send_sem=swap_sems.at[0],
        recv_sem=swap_sems.at[1],
        device_id=mate,
        device_id_type=MESH,
    )
    swap.start()
    count_buf[0] = jnp.broadcast_to(jnp.sum(kept, axis=0, keepdims=True), (8, 128))
    for d in range(1, 8):
        remote(
            count_buf.at[0], count_buf.at[d], count_sems.at[0], count_sems.at[1], dp_peers[d - 1]
        ).start()
    for t in range(3):
        group_kept[t] = kept_rows(group_sequence, kept, t)

    for name in ("step_bias", "decay_rate", "skip_gain"):
        loads[name].wait()

    inner[...] = jnp.zeros_like(inner)

    def widen(start, spread):
        spread[...] = in_weight[pl.ds(pl.multiple_of(start * 4096, 4096), 4096), :].astype(
            jnp.float32
        )

    def multiply(start, spread):
        left = normed[:, pl.ds(pl.multiple_of(start * 512, 512), 512)]
        for part in range(2):
            for j in range(0, 4, 2):
                right = jnp.concatenate(
                    [
                        spread[pl.ds((j + i) * 2 + part, 512, stride=8), :].astype(jnp.bfloat16)
                        for i in range(2)
                    ],
                    axis=1,
                )
                product = jnp.dot(left, right, preferred_element_type=jnp.float32)
                for i in range(2):
                    inner[part * 4 + j + i] += product[:, i * 128 : (i + 1) * 128]

    def await_chunk(index):
        rows = pl.ds(pl.multiple_of(index * 8192, 8192), 8192)
        pltpu.make_async_copy(
            in_weight_in.at[rows], in_weight.at[rows], chunk_sems.at[index]
        ).wait()

    def pair(index, carry):
        await_chunk(index + 1)
        multiply(2 * index, spread_a)
        widen(2 * index + 1, spread_b)
        multiply(2 * index + 1, spread_b)
        widen(2 * index + 2, spread_a)
        return carry

    await_chunk(0)
    widen(0, spread_a)
    lax.fori_loop(0, 3, pair, 0)
    multiply(6, spread_a)
    widen(7, spread_b)
    multiply(7, spread_b)

    steps, after = [], []
    running = None
    for s in range(8):
        raw = step_rows[pl.ds(s, 24, stride=8), 0:8] + step_bias[...]
        size = jnp.maximum(raw, 0.0) + jnp.log1p(jnp.exp(-jnp.abs(raw)))
        change = -size * decay_rate[...]
        running = change if running is None else running + change
        steps.append(size)
        after.append(running)
    prefix_kept = jnp.zeros_like(running)
    for s in range(8):
        prefix_kept = jnp.where(kept == float(s + 1), after[s], prefix_kept)
    for s in range(8):
        small[pl.ds((36 + s) * 24, 24), 0:8] = jnp.exp(after[s])
        small[pl.ds((44 + s) * 24, 24), 0:8] = (
            jnp.where(kept > float(s), jnp.exp(prefix_kept - after[s]), 0.0) * steps[s]
        )
    head_decay = jnp.exp(prefix_kept)
    for h in range(8):
        decay_kept[h] = jnp.broadcast_to(head_decay[:, h : h + 1], (24, 128))
    swap.wait_recv()
    for s in range(8):
        map_rows[pl.ds(s, 24, stride=8), :] = maps[1, s]
        input_rows[pl.ds(s * 24, 24), :] = maps[0, s]
        for j in range(s + 1):
            match = jnp.sum(maps[1, s] * maps[0, j], axis=1, keepdims=True)
            small[pl.ds((s * (s + 1) // 2 + j) * 24, 24), 0:8] = (
                jnp.exp(after[s] - after[j]) * steps[j] * match
            )
    hot = (
        lax.broadcasted_iota(jnp.int32, (8, 512), 1) // 64
        == lax.broadcasted_iota(jnp.int32, (8, 512), 0)
    ).astype(jnp.bfloat16)

    def expand(index, carry):
        rows = pl.ds(index * 416, 416)
        mixing[rows, :] = jnp.dot(
            small[rows, 0:8].astype(jnp.bfloat16), hot, preferred_element_type=jnp.float32
        )
        return carry

    for index in range(3):
        expand(index, 0)
    loads["state"].wait()

    for name in ("value_cache", "value_kernel", "value_offset", "out_gain"):
        loads[name].wait()
    offset_row = value_offset[...].astype(jnp.float32).reshape(1, 512)
    lane = lax.broadcasted_iota(jnp.int32, (8, 128), 1)
    square_copies = []
    for tile in range(3):
        eight = pl.ds(tile * 8, 8)
        for request in range(tile * 8, tile * 8 + 8):
            rows = pl.ds(request * 8, 8)
            product = lax.dot_general(
                map_rows[rows, :].astype(jnp.bfloat16),
                state[request],
                (((1,), (1,)), ((), ())),
                preferred_element_type=jnp.float32,
            )
            for block in range(4):
                carried[block, rows, :] = product[:, block * 128 : (block + 1) * 128]
        for block in range(4):
            columns = slice(block * 128, (block + 1) * 128)
            skip = jnp.where(
                lane < 64,
                jnp.broadcast_to(skip_gain[:, 2 * block : 2 * block + 1], (8, 128)),
                jnp.broadcast_to(skip_gain[:, 2 * block + 1 : 2 * block + 2], (8, 128)),
            )
            taps = [value_kernel[k : k + 1, columns].astype(jnp.float32) for k in range(4)]
            offset = offset_row[:, columns]
            counts = kept[tile * 8 : tile * 8 + 8]
            sequence = [value_cache[t, eight, columns].astype(jnp.float32) for t in range(3)] + [
                rounded(inner[4 + block, pl.ds(tile * 64 + s, 8, stride=8), :])
                for s in range(8)
            ]
            for t in range(3):
                value_kept[t, eight, columns] = kept_rows(sequence, counts, t)
            values = convolved(sequence, taps, offset)
            for s in range(8):
                weighted[pl.ds(s * 24 + tile * 8, 8), columns] = (
                    mixing[pl.ds((44 + s) * 24 + tile * 8, 8), columns] * values[s]
                )
                total = (
                    mixing[pl.ds((36 + s) * 24 + tile * 8, 8), columns]
                    * carried[block, pl.ds(tile * 64 + s, 8, stride=8), :]
                    + skip * values[s]
                )
                for j in range(s + 1):
                    q = s * (s + 1) // 2 + j
                    total = total + mixing[pl.ds(q * 24 + tile * 8, 8), columns] * values[j]
                gate = rounded(inner[block, pl.ds(tile * 64 + s, 8, stride=8), :])
                gated = total * (gate / (1.0 + jnp.exp(-gate)))
                square = gated * gated
                if block:
                    square = square + squares[s, eight]
                squares[s, eight] = square
                valid = jnp.logical_and(
                    alive[tile * 8 : tile * 8 + 8],
                    length_column[tile * 8 : tile * 8 + 8] > float(s),
                )
                gated_rows[block, pl.ds(tile * 64 + s, 8, stride=8), :] = jnp.where(
                    valid, gated * out_gain[:, columns], 0.0
                )
            rows_ref[tile * 64 : tile * 64 + 64, columns] = gated_rows[
                block, tile * 64 : tile * 64 + 64, :
            ].astype(jnp.bfloat16)
        own = jnp.zeros((8, 128), jnp.float32)
        for s in range(8):
            own = jnp.where(lane == s, jnp.sum(squares[s, eight], axis=1, keepdims=True), own)
        square_own[tile] = own
        copy = remote(
            square_own.at[tile],
            square_other.at[tile],
            swap_sems.at[2 + tile],
            swap_sems.at[5 + tile],
            mate,
        )
        copy.start()
        square_copies.append(copy)
    loads["out_weight"].wait()
    firsts = [along_y, along_z]
    seconds = [along_z, along_y]
    first_at = [y, z]
    second_at = [z, y]

    def launch(src, dst, stage, route, chunk, slot, place):
        copy = remote(src, dst, send_sems.at[0], recv_sems.at[stage, route, chunk, slot], place)
        copy.start()
        return copy

    def product_of(route, step, chunk):
        base = ((first_at[route] + step) % 4) * 1024
        return jnp.dot(
            rows_ref[pl.ds(chunk * 64 + route * 32, 32), :],
            out_weight[:, pl.ds(pl.multiple_of(base, 1024), 1024)],
            preferred_element_type=jnp.float32,
        )

    def settle(route, step, chunk, product):
        scale = scale_rows[pl.ds(chunk * 64 + route * 32, 32), :]
        partial[route, step, chunk] = (
            product * jnp.concatenate([scale] * 8, axis=1)
        ).astype(jnp.bfloat16)

    for step in (2, 1, 3):
        for route in range(2):
            first_products[route, step - 1] = product_of(route, step, 0)
    turned[...] = jnp.transpose(weighted[...]).astype(jnp.bfloat16)

    def keep_states(first, last):
        owner = lax.rem(lax.broadcasted_iota(jnp.int32, (192, 128), 0), 24)

        def keep(index, carry):
            inputs = input_rows[...]
            right = jnp.concatenate(
                [
                    jnp.where(owner == 2 * index + i, inputs, 0.0).astype(jnp.bfloat16)
                    for i in range(2)
                ],
                axis=1,
            )
            for h in range(8):
                update = jnp.dot(
                    turned[h * 64 : (h + 1) * 64, :], right, preferred_element_type=jnp.float32
                )
                for i in range(2):
                    request = 2 * index + i
                    decay = decay_kept[h, pl.ds(request, 1), :]
                    before = state[request, h * 64 : (h + 1) * 64, :].astype(jnp.float32)
                    kept_ref[request, h * 64 : (h + 1) * 64, :] = (
                        decay * before + update[:, i * 128 : (i + 1) * 128]
                    ).astype(jnp.bfloat16)
            return carry

        lax.fori_loop(first, last, keep, 0)

    held = {}
    for chunk in range(3):
        square_copies[chunk].wait_recv()
        scales = lax.rsqrt((square_own[chunk] + square_other[chunk]) / 1024.0 + EPSILON)
        for s in range(8):
            scale_rows[pl.ds(chunk * 64 + s, 8, stride=8), :] = jnp.broadcast_to(
                scales[:, s : s + 1], (8, 128)
            )
        for step in (2, 1, 3):
            for route in range(2):
                product = first_products[route, step - 1] if chunk == 0 else product_of(route, step, chunk)
                settle(route, step, chunk, product)
                unit = partial.at[route, step, chunk]
                landing = first_recv.at[route, chunk]
                plus, minus = (firsts[route][1], firsts[route][3])
                sends = {
                    2: ((0, 0, plus), (1, 1, minus)),
                    1: ((1, 3, plus),),
                    3: ((0, 4, minus),),
                }[step]
                for half, slot, place in sends:
                    held[route, chunk, slot] = launch(
                        unit.at[:, HALVES[half]], landing.at[slot], 0, route, chunk, slot, place
                    )
    for chunk in range(3):
        for route in range(2):
            settle(route, 0, chunk, product_of(route, 0, chunk))
    for chunk in range(3):
        for half in range(2):
            for route in range(2):
                landing = first_recv.at[route, chunk]
                held[route, chunk, half].wait_recv()
                mix = first_mix.at[route, chunk, half]
                mix[...] = widened_sum(
                    landing.at[half], partial.at[route, (1, 3)[half], chunk, :, HALVES[half]]
                )
                slot = (2, 5)[half]
                held[route, chunk, slot] = launch(
                    mix, landing.at[slot], 0, route, chunk, slot, firsts[route][(1, 3)[half]]
                )

    def spread_start(stage, places, piece, chunk):
        started = []
        for route in range(2):
            plus, minus = (places[route][1], places[route][3])
            started.append([])
            for half, slot, place in ((0, 0, plus), (1, 1, minus), (1, 2, plus), (0, 3, minus)):
                own = piece(route, chunk, half, 0)
                started[route].append(launch(own, own, stage, route, chunk, slot, place))
        return started

    def spread_forward(started, stage, places, piece, chunk):
        for half in range(2):
            for route in range(2):
                started[route][half].wait_recv()
                passed = piece(route, chunk, half, (3, 1)[half])
                started[route].append(
                    launch(
                        passed, passed, stage, route, chunk, 4 + half, places[route][(1, 3)[half]]
                    )
                )

    def spread_finish(started):
        for route in range(2):
            for index in range(2, 6):
                started[route][index].wait_recv()

    def middle(route, chunk, half, k):
        return gathered.at[route, chunk, (second_at[route] + k) % 4, :, HALVES[half]]

    def spot(route, chunk, half, k):
        column = ((first_at[route] + k) % 4) * 1024 + half * 512
        return out_ref.at[
            pl.ds(chunk * 64 + route * 32, 32), pl.ds(pl.multiple_of(column, 512), 512)
        ]

    inner_spread = []
    for chunk in range(3):
        for half in range(2):
            for route in range(2):
                for slot in ((4, 2), (3, 5))[half]:
                    held[route, chunk, slot].wait_recv()
                own = middle(route, chunk, half, 0)
                own[...] = widened_sum(
                    partial.at[route, 0, chunk, :, HALVES[half]],
                    first_recv.at[route, chunk, 2 + half],
                    first_recv.at[route, chunk, 4 + half],
                )
        inner_spread.append(spread_start(1, seconds, middle, chunk))
    pltpu.make_async_copy(
        count_buf.at[pl.ds(1, 7)], count_buf.at[pl.ds(1, 7)], count_sems.at[1]
    ).wait()
    everyone = count_buf[0]
    for d in range(1, 8):
        everyone = everyone + count_buf[d]
    total_own[0] = jnp.sum(everyone[0:1, 0:1]).astype(jnp.int32)
    total_copy = pltpu.make_async_copy(total_own, total_ref, swap_sems.at[8])
    total_copy.start()
    keep_states(0, 4)
    for chunk in range(3):
        spread_forward(inner_spread[chunk], 1, seconds, middle, chunk)
    outer_spread = []
    for chunk in range(3):
        spread_finish(inner_spread[chunk])
        for half in range(2):
            for route in range(2):
                own = spot(route, chunk, half, 0)
                own[...] = widened_sum(*(gathered.at[route, chunk, b, :, HALVES[half]] for b in range(4)))
        outer_spread.append(spread_start(2, firsts, spot, chunk))
    for chunk in range(3):
        spread_forward(outer_spread[chunk], 2, firsts, spot, chunk)
    keep_states(4, 12)
    for chunk in range(3):
        spread_finish(outer_spread[chunk])
    total_copy.wait()
    pltpu.make_async_copy(
        count_buf.at[pl.ds(1, 7)], count_buf.at[pl.ds(1, 7)], count_sems.at[0]
    ).wait()
    for copy in square_copies + [swap]:
        copy.wait_send()
    sent = in_weight.at[pl.ds(0, 13824)]
    pltpu.make_async_copy(sent, sent, send_sems.at[0]).wait()


def layer(*operands):
    return pl.pallas_call(
        layer_kernel,
        out_shape=(
            jax.ShapeDtypeStruct((192, 4096), jnp.bfloat16),
            jax.ShapeDtypeStruct((24, 512, 128), jnp.bfloat16),
            jax.ShapeDtypeStruct((3, 24, 512), jnp.bfloat16),
            jax.ShapeDtypeStruct((3, 24, 128), jnp.bfloat16),
            jax.ShapeDtypeStruct((1,), jnp.int32),
        ),
        in_specs=[pl.BlockSpec(memory_space=pltpu.HBM)] * 20,
        out_specs=(pl.BlockSpec(memory_space=pltpu.VMEM),) * 4
        + (pl.BlockSpec(memory_space=pltpu.HBM),),
        scratch_shapes=[
            pltpu.VMEM((192, 4096), jnp.bfloat16),
            pltpu.VMEM((1, 4096), jnp.float32),
            pltpu.VMEM((32768, 128), jnp.bfloat16),
            pltpu.VMEM((4096, 256), jnp.bfloat16),
            pltpu.VMEM((8, 4096), jnp.bfloat16),
            pltpu.VMEM((4, 512), jnp.bfloat16),
            pltpu.VMEM((512,), jnp.bfloat16),
            pltpu.VMEM((4, 128), jnp.bfloat16),
            pltpu.VMEM((128,), jnp.bfloat16),
            pltpu.VMEM((1, 8), jnp.float32),
            pltpu.VMEM((1, 8), jnp.float32),
            pltpu.VMEM((1, 8), jnp.float32),
            pltpu.VMEM((1, 512), jnp.float32),
            pltpu.VMEM((512, 4096), jnp.bfloat16),
            pltpu.VMEM((24, 512, 128), jnp.bfloat16),
            pltpu.VMEM((3, 24, 512), jnp.bfloat16),
            pltpu.VMEM((3, 24, 128), jnp.bfloat16),
            pltpu.VMEM((1, 24), jnp.int32),
            pltpu.VMEM((1, 24), jnp.int32),
            pltpu.VMEM((1, 24), jnp.int32),
            pltpu.VMEM((192, 4096), jnp.bfloat16),
            pltpu.VMEM((4096, 128), jnp.float32),
            pltpu.VMEM((4096, 128), jnp.float32),
            pltpu.VMEM((8, 192, 128), jnp.float32),
            pltpu.VMEM((192, 128), jnp.float32),
            pltpu.VMEM((192, 128), jnp.float32),
            pltpu.VMEM((2, 8, 24, 128), jnp.float32),
            pltpu.VMEM((192, 128), jnp.float32),
            pltpu.VMEM((4, 192, 128), jnp.float32),
            pltpu.VMEM((1248, 128), jnp.float32),
            pltpu.VMEM((1248, 512), jnp.float32),
            pltpu.VMEM((8, 24, 128), jnp.float32),
            pltpu.VMEM((192, 512), jnp.float32),
            pltpu.VMEM((512, 192), jnp.bfloat16),
            pltpu.VMEM((192, 128), jnp.float32),
            pltpu.VMEM((4, 192, 128), jnp.float32),
            pltpu.VMEM((192, 512), jnp.bfloat16),
            pltpu.VMEM((8, 24, 128), jnp.float32),
            pltpu.VMEM((3, 8, 128), jnp.float32),
            pltpu.VMEM((3, 8, 128), jnp.float32),
            pltpu.VMEM((192, 128), jnp.float32),
            pltpu.VMEM((2, 3, 32, 1024), jnp.float32),
            pltpu.VMEM((2, 4, 3, 32, 1024), jnp.bfloat16),
            pltpu.VMEM((2, 3, 6, 32, 512), jnp.bfloat16),
            pltpu.VMEM((2, 3, 2, 32, 512), jnp.bfloat16),
            pltpu.VMEM((2, 3, 4, 32, 1024), jnp.bfloat16),
            pltpu.VMEM((8, 8, 128), jnp.float32),
            pltpu.SMEM((1,), jnp.int32),
            pltpu.SemaphoreType.DMA((1,)),
            pltpu.SemaphoreType.DMA((3, 2, 3, 6)),
            pltpu.SemaphoreType.DMA((2,)),
            pltpu.SemaphoreType.DMA((9,)),
            pltpu.SemaphoreType.DMA((20,)),
            pltpu.SemaphoreType.DMA((4,)),
            pltpu.SemaphoreType.DMA((4,)),
        ],
        compiler_params=pltpu.CompilerParams(
            collective_id=0, has_side_effects=True, vmem_limit_bytes=44 * 1024 * 1024
        ),
    )(*(pltpu.with_memory_space_constraint(operand, pltpu.HBM) for operand in operands))


def place_kernel(*refs):
    sources, targets, sems = refs[:4], refs[4:8], refs[8]
    copies = [
        pltpu.make_async_copy(source, target, sems.at[index])
        for index, (source, target) in enumerate(zip(sources, targets))
    ]
    for copy in copies:
        copy.start()
    for copy in copies:
        copy.wait()


def place(*arrays):
    return pl.pallas_call(
        place_kernel,
        out_shape=tuple(jax.ShapeDtypeStruct(a.shape, a.dtype) for a in arrays),
        in_specs=[pl.BlockSpec(memory_space=pltpu.VMEM)] * 4,
        out_specs=(pl.BlockSpec(memory_space=pltpu.HBM),) * 4,
        scratch_shapes=[pltpu.SemaphoreType.DMA((4,))],
        compiler_params=pltpu.CompilerParams(vmem_limit_bytes=16 * 1024 * 1024),
    )(*arrays)


def local(
    tokens,
    norm_gain,
    in_weight,
    group_weight,
    step_weight,
    value_kernel,
    value_offset,
    group_kernel,
    group_offset,
    step_bias,
    decay_rate,
    skip_gain,
    out_gain,
    out_weight,
    scan_state,
    value_cache,
    group_cache,
    accepted,
    draft_lengths,
    live_flags,
):
    woven = in_weight.reshape(4096, 2, 4, 128).transpose(0, 2, 1, 3).reshape(32768, 128)
    rows, kept_state, value_kept, group_kept, total = layer(
        tokens.reshape(192, 4096),
        norm_gain.reshape(1, 4096),
        woven,
        group_weight,
        step_weight.T,
        value_kernel,
        value_offset,
        group_kernel,
        group_offset,
        step_bias.reshape(1, 8),
        decay_rate.reshape(1, 8),
        skip_gain.reshape(1, 8),
        out_gain.reshape(1, 512),
        out_weight,
        scan_state.reshape(24, 512, 128),
        value_cache.transpose(1, 0, 2),
        group_cache.transpose(1, 0, 2),
        accepted.reshape(1, 24),
        draft_lengths.reshape(1, 24),
        live_flags.reshape(1, 24),
    )
    rows, kept_state, value_kept, group_kept = place(rows, kept_state, value_kept, group_kept)
    return (
        rows.reshape(24, 8, 4096),
        kept_state.reshape(24, 8, 64, 128),
        value_kept.transpose(1, 0, 2),
        group_kept.transpose(1, 0, 2),
        total,
    )


def solution(mesh):
    in_specs = (
        P(DP, None, None),
        P(),
        P(None, None, "tensor"),
        P(None, "tensor"),
        P(None, "tensor"),
        P(None, "tensor"),
        P("tensor"),
        P(None, "tensor"),
        P("tensor"),
        P("tensor"),
        P("tensor"),
        P("tensor"),
        P("tensor"),
        P("tensor", None),
        P(DP, "tensor", None, None),
        P(DP, None, "tensor"),
        P(DP, None, "tensor"),
        P(DP),
        P(DP),
        P(DP),
    )
    out_specs = (
        P(DP, None, None),
        P(DP, "tensor", None, None),
        P(DP, None, "tensor"),
        P(DP, None, "tensor"),
        P(),
    )
    return jax.shard_map(local, mesh=mesh, in_specs=in_specs, out_specs=out_specs, check_vma=False)
```

```python
import jax
import jax.numpy as jnp
from jax import lax
from jax.experimental import pallas as pl
from jax.experimental.pallas import tpu as pltpu
from jax.sharding import PartitionSpec as P

DP = "dp"


EPSILON = 1e-05


def swapped(value, axis, distance):
    mask = 2**distance
    pairs = [(source, source ^ mask) for source in range(lax.axis_size(axis))]
    return lax.ppermute(value, axis, pairs)


MESH = pl.DeviceIdType.MESH
HALVES = (pl.ds(0, 512), pl.ds(512, 512))


def ring_places():
    tensor = lax.axis_index("tensor")
    z, y = tensor // 4, tensor % 4
    along_y = [{"tensor": z * 4 + (y + d) % 4} for d in range(4)]
    along_z = [{"tensor": ((z + d) % 4) * 4 + y} for d in range(4)]
    return (z, y, along_z, along_y)


def remote(src, dst, send, recv, place):
    return pltpu.make_async_remote_copy(
        src_ref=src,
        dst_ref=dst,
        send_sem=send,
        recv_sem=recv,
        device_id=place,
        device_id_type=MESH,
    )


def widened_sum(*refs):
    total = refs[0][...].astype(jnp.float32)
    for ref in refs[1:]:
        total = total + ref[...].astype(jnp.float32)
    return total.astype(jnp.bfloat16)


def layer_kernel(
    tokens_in,
    gain_in,
    in_weight_in,
    group_weight_in,
    step_weight_in,
    value_kernel_in,
    value_offset_in,
    group_kernel_in,
    group_offset_in,
    step_bias_in,
    decay_rate_in,
    skip_gain_in,
    out_gain_in,
    out_weight_in,
    state_in,
    value_cache_in,
    group_cache_in,
    accepted_in,
    lengths_in,
    live_in,
    out_ref,
    kept_ref,
    value_kept,
    group_kept,
    total_ref,
    tokens,
    gain,
    in_weight,
    group_weight,
    step_weight,
    value_kernel,
    value_offset,
    group_kernel,
    group_offset,
    step_bias,
    decay_rate,
    skip_gain,
    out_gain,
    out_weight,
    state,
    value_cache,
    group_cache,
    accepted,
    lengths,
    live,
    normed,
    spread_a,
    spread_b,
    inner,
    group_rows,
    step_rows,
    maps,
    map_rows,
    carried,
    small,
    mixing,
    decay_kept,
    weighted,
    turned,
    input_rows,
    gated_rows,
    rows_ref,
    squares,
    square_own,
    square_other,
    scale_rows,
    products,
    partial,
    first_recv,
    first_mix,
    gathered,
    count_buf,
    total_own,
    send_sems,
    recv_sems,
    count_sems,
    swap_sems,
    load_sems,
    token_sems,
    chunk_sems,
):
    z, y, along_z, along_y = ring_places()
    dp = lax.axis_index("dp")
    parity = y % 2
    mate = {"tensor": z * 4 + (y + 1 - 2 * parity)}
    barrier = pltpu.get_barrier_semaphore()
    dp_peers = [{"dp": (dp + d) % 8} for d in range(1, 8)]
    ring_peers = [along_z[1], along_z[3], along_y[1], along_y[3]]
    for place in ring_peers + dp_peers:
        pl.semaphore_signal(barrier, inc=1, device_id=place, device_id_type=MESH)
    loads = {}

    def load(name, src, dst, index):
        loads[name] = pltpu.make_async_copy(src, dst, load_sems.at[index])
        loads[name].start()

    token_copies = []
    for index in range(4):
        rows = pl.ds(index * 48, 48)
        copy = pltpu.make_async_copy(tokens_in.at[rows], tokens.at[rows], token_sems.at[index])
        copy.start()
        token_copies.append(copy)
    load("gain", gain_in, gain, 1)
    load("step_weight", step_weight_in, step_weight, 4)
    load("group_weight", group_weight_in, group_weight.at[:, 0:128], 3)
    load("accepted", accepted_in, accepted, 17)
    load("lengths", lengths_in, lengths, 18)
    load("live", live_in, live, 19)
    load("group_cache", group_cache_in, group_cache, 16)
    load("group_kernel", group_kernel_in, group_kernel, 7)
    load("group_offset", group_offset_in, group_offset, 8)
    load("step_bias", step_bias_in, step_bias, 9)
    load("decay_rate", decay_rate_in, decay_rate, 10)
    load("skip_gain", skip_gain_in, skip_gain, 11)
    def load_chunk(index):
        rows = pl.ds(index * 8192, 8192)
        pltpu.make_async_copy(in_weight_in.at[rows], in_weight.at[rows], chunk_sems.at[index]).start()

    load_chunk(0)
    load_chunk(1)

    def column(ref):
        square = lax.broadcasted_iota(jnp.int32, (24, 24), 0) == lax.broadcasted_iota(
            jnp.int32, (24, 24), 1
        )
        values = jnp.broadcast_to(ref[...].astype(jnp.float32), (24, 24))
        return jnp.sum(jnp.where(square, values, 0.0), axis=1, keepdims=True)

    loads["gain"].wait()

    def normalize(block):
        rows = slice(block * 16, block * 16 + 16)
        total = jnp.zeros((16, 256), jnp.float32)
        for part in range(16):
            piece = tokens[rows, part * 256 : (part + 1) * 256].astype(jnp.float32)
            total = total + piece * piece
        mean = jnp.sum(total, axis=1, keepdims=True) / 4096.0
        scale = jnp.broadcast_to(lax.rsqrt(mean + EPSILON), (16, 256))
        for part in range(16):
            columns = slice(part * 256, (part + 1) * 256)
            piece = tokens[rows, columns].astype(jnp.float32)
            normed[rows, columns] = (piece * scale * gain[:, columns]).astype(jnp.bfloat16)

    for index in range(4):
        token_copies[index].wait()
        if index in (0, 2):
            load_chunk(2 + index // 2)
        for block in range(3):
            normalize(index * 3 + block)
    loads["step_weight"].wait()
    for block in range(32):
        rows = slice(block * 128, (block + 1) * 128)
        group_weight[rows, 128:136] = jnp.transpose(
            step_weight[:, rows].astype(jnp.float32)
        ).astype(jnp.bfloat16)
    loads["group_weight"].wait()
    product = jnp.dot(normed[...], group_weight[...], preferred_element_type=jnp.float32)
    group_rows[...] = product[:, 0:128]
    step_rows[...] = product[:, 128:256]
    for name in ("accepted", "lengths", "live", "group_cache", "group_kernel", "group_offset"):
        loads[name].wait()
    kept = column(accepted) * column(live)
    alive = column(live) == 1.0
    length_column = column(lengths)

    def sequence_of(cache, rows):
        early = [cache[t].astype(jnp.float32) for t in range(3)]
        return early + [rounded(piece) for piece in rows]

    def rounded(piece):
        return piece.astype(jnp.bfloat16).astype(jnp.float32)

    def convolved(sequence, taps, offset):
        out = []
        for s in range(8):
            total = offset
            for k in range(4):
                total = total + taps[k] * sequence[s + k]
            out.append(total / (1.0 + jnp.exp(-total)))
        return out

    def kept_rows(sequence, counts, t):
        chosen = sequence[t]
        for k in range(1, 9):
            chosen = jnp.where(counts == float(k), sequence[k + t], chosen)
        return chosen.astype(jnp.bfloat16)

    group_taps = [group_kernel[k : k + 1, :].astype(jnp.float32) for k in range(4)]
    group_sequence = sequence_of(
        group_cache, [group_rows[pl.ds(s, 24, stride=8), :] for s in range(8)]
    )
    own_maps = convolved(
        group_sequence, group_taps, group_offset[...].astype(jnp.float32).reshape(1, 128)
    )
    for s in range(8):
        maps[parity, s] = own_maps[s]
    pl.semaphore_wait(barrier, 11)
    swap = pltpu.make_async_remote_copy(
        src_ref=maps.at[parity],
        dst_ref=maps.at[parity],
        send_sem=swap_sems.at[0],
        recv_sem=swap_sems.at[1],
        device_id=mate,
        device_id_type=MESH,
    )
    swap.start()
    count_buf[0] = jnp.broadcast_to(jnp.sum(kept, axis=0, keepdims=True), (8, 128))
    for d in range(1, 8):
        remote(
            count_buf.at[0], count_buf.at[d], count_sems.at[0], count_sems.at[1], dp_peers[d - 1]
        ).start()
    for t in range(3):
        group_kept[t] = kept_rows(group_sequence, kept, t)

    for name in ("step_bias", "decay_rate", "skip_gain"):
        loads[name].wait()

    inner[...] = jnp.zeros_like(inner)

    lower = lax.broadcasted_iota(jnp.int32, (256, 8, 128), 1) < 4

    def widen(start, spread):
        block = in_weight[pl.ds(pl.multiple_of(start * 4096, 4096), 4096), :].astype(jnp.float32)
        block = block.reshape(256, 16, 128)
        even, odd = block[:, 0:8], block[:, 8:16]
        spread[0] = jnp.where(lower, even, pltpu.roll(odd, 4, 1)).reshape(2048, 128)
        spread[1] = jnp.where(lower, pltpu.roll(even, 4, 1), odd).reshape(2048, 128)

    def multiply(start, spread):
        left = normed[:, pl.ds(pl.multiple_of(start * 512, 512), 512)]
        for part in range(2):
            for j in range(0, 4, 2):
                right = jnp.concatenate(
                    [
                        spread[j // 2, pl.ds(i * 2 + part, 512, stride=4), :].astype(jnp.bfloat16)
                        for i in range(2)
                    ],
                    axis=1,
                )
                product = jnp.dot(left, right, preferred_element_type=jnp.float32)
                for i in range(2):
                    inner[part * 4 + j + i] += product[:, i * 128 : (i + 1) * 128]

    def await_chunk(index):
        rows = pl.ds(pl.multiple_of(index * 8192, 8192), 8192)
        pltpu.make_async_copy(
            in_weight_in.at[rows], in_weight.at[rows], chunk_sems.at[index]
        ).wait()

    def pair(index, carry):
        await_chunk(index + 1)
        multiply(2 * index, spread_a)
        widen(2 * index + 1, spread_b)
        multiply(2 * index + 1, spread_b)
        widen(2 * index + 2, spread_a)
        return carry

    await_chunk(0)
    widen(0, spread_a)
    lax.fori_loop(0, 2, pair, 0)
    load("value_cache", value_cache_in, value_cache, 15)
    load("value_kernel", value_kernel_in, value_kernel, 5)
    load("value_offset", value_offset_in, value_offset, 6)
    load("out_gain", out_gain_in, out_gain, 12)
    load("state", state_in, state, 14)
    load("out_weight", out_weight_in, out_weight, 13)
    lax.fori_loop(2, 3, pair, 0)
    swap.wait_recv()
    multiply(6, spread_a)
    widen(7, spread_b)
    multiply(7, spread_b)

    steps, after = [], []
    running = None
    for s in range(8):
        raw = step_rows[pl.ds(s, 24, stride=8), 0:8] + step_bias[...]
        size = jnp.maximum(raw, 0.0) + jnp.log1p(jnp.exp(-jnp.abs(raw)))
        change = -size * decay_rate[...]
        running = change if running is None else running + change
        steps.append(size)
        after.append(running)
    prefix_kept = jnp.zeros_like(running)
    for s in range(8):
        prefix_kept = jnp.where(kept == float(s + 1), after[s], prefix_kept)
    for s in range(8):
        small[pl.ds((36 + s) * 24, 24), 0:8] = jnp.exp(after[s])
        small[pl.ds((44 + s) * 24, 24), 0:8] = (
            jnp.where(kept > float(s), jnp.exp(prefix_kept - after[s]), 0.0) * steps[s]
        )
    head_decay = jnp.exp(prefix_kept)
    for h in range(8):
        decay_kept[h] = jnp.broadcast_to(head_decay[:, h : h + 1], (24, 128))
    for s in range(8):
        map_rows[pl.ds(s, 24, stride=8), :] = maps[1, s]
        input_rows[pl.ds(s * 24, 24), :] = maps[0, s]
        for j in range(s + 1):
            match = jnp.sum(maps[1, s] * maps[0, j], axis=1, keepdims=True)
            small[pl.ds((s * (s + 1) // 2 + j) * 24, 24), 0:8] = (
                jnp.exp(after[s] - after[j]) * steps[j] * match
            )
    hot = (
        lax.broadcasted_iota(jnp.int32, (8, 512), 1) // 64
        == lax.broadcasted_iota(jnp.int32, (8, 512), 0)
    ).astype(jnp.bfloat16)

    def expand(index, carry):
        rows = pl.ds(index * 416, 416)
        mixing[rows, :] = jnp.dot(
            small[rows, 0:8].astype(jnp.bfloat16), hot, preferred_element_type=jnp.float32
        )
        return carry

    for index in range(3):
        expand(index, 0)
    loads["state"].wait()

    for name in ("value_cache", "value_kernel", "value_offset", "out_gain"):
        loads[name].wait()
    offset_row = value_offset[...].astype(jnp.float32).reshape(1, 512)
    lane = lax.broadcasted_iota(jnp.int32, (8, 128), 1)
    square_copies = []
    for tile in range(3):
        eight = pl.ds(tile * 8, 8)
        for request in range(tile * 8, tile * 8 + 8):
            rows = pl.ds(request * 8, 8)
            product = lax.dot_general(
                map_rows[rows, :].astype(jnp.bfloat16),
                state[request],
                (((1,), (1,)), ((), ())),
                preferred_element_type=jnp.float32,
            )
            for block in range(4):
                carried[block, rows, :] = product[:, block * 128 : (block + 1) * 128]
        for block in range(4):
            columns = slice(block * 128, (block + 1) * 128)
            skip = jnp.where(
                lane < 64,
                jnp.broadcast_to(skip_gain[:, 2 * block : 2 * block + 1], (8, 128)),
                jnp.broadcast_to(skip_gain[:, 2 * block + 1 : 2 * block + 2], (8, 128)),
            )
            taps = [value_kernel[k : k + 1, columns].astype(jnp.float32) for k in range(4)]
            offset = offset_row[:, columns]
            counts = kept[tile * 8 : tile * 8 + 8]
            sequence = [value_cache[t, eight, columns].astype(jnp.float32) for t in range(3)] + [
                rounded(inner[4 + block, pl.ds(tile * 64 + s, 8, stride=8), :])
                for s in range(8)
            ]
            for t in range(3):
                value_kept[t, eight, columns] = kept_rows(sequence, counts, t)
            values = convolved(sequence, taps, offset)
            for s in range(8):
                weighted[pl.ds(s * 24 + tile * 8, 8), columns] = (
                    mixing[pl.ds((44 + s) * 24 + tile * 8, 8), columns] * values[s]
                )
                total = (
                    mixing[pl.ds((36 + s) * 24 + tile * 8, 8), columns]
                    * carried[block, pl.ds(tile * 64 + s, 8, stride=8), :]
                    + skip * values[s]
                )
                for j in range(s + 1):
                    q = s * (s + 1) // 2 + j
                    total = total + mixing[pl.ds(q * 24 + tile * 8, 8), columns] * values[j]
                gate = rounded(inner[block, pl.ds(tile * 64 + s, 8, stride=8), :])
                gated = total * (gate / (1.0 + jnp.exp(-gate)))
                square = gated * gated
                if block:
                    square = square + squares[s, eight]
                squares[s, eight] = square
                valid = jnp.logical_and(
                    alive[tile * 8 : tile * 8 + 8],
                    length_column[tile * 8 : tile * 8 + 8] > float(s),
                )
                gated_rows[block, pl.ds(tile * 64 + s, 8, stride=8), :] = jnp.where(
                    valid, gated * out_gain[:, columns], 0.0
                )
            for route in range(2):
                rows_ref[route * 96 + tile * 32 : route * 96 + tile * 32 + 32, columns] = gated_rows[
                    block, tile * 64 + route * 32 : tile * 64 + route * 32 + 32, :
                ].astype(jnp.bfloat16)
        own = jnp.zeros((8, 128), jnp.float32)
        for s in range(8):
            own = jnp.where(lane == s, jnp.sum(squares[s, eight], axis=1, keepdims=True), own)
        square_own[tile] = own
        copy = remote(
            square_own.at[tile],
            square_other.at[tile],
            swap_sems.at[2 + tile],
            swap_sems.at[5 + tile],
            mate,
        )
        copy.start()
        square_copies.append(copy)
    loads["out_weight"].wait()
    firsts = [along_y, along_z]
    seconds = [along_z, along_y]
    first_at = [y, z]
    second_at = [z, y]

    def sem_at(stage, chunk):
        return chunk * 18 + (0, 8, 13)[stage]

    def launch(src, dst, stage, route, chunk, slot, place):
        if slot < 2:
            index = route * 2 + slot
        elif stage:
            index = 4
        else:
            index = 4 + route * 2 + (slot - 2) // 2
        landed = recv_sems.at[sem_at(stage, chunk) + index]
        copy = remote(src, dst, send_sems.at[0], landed, place)
        copy.start()
        return copy

    def await_bytes(ref, stage, chunk, index):
        pltpu.make_async_copy(ref, ref, recv_sems.at[sem_at(stage, chunk) + index]).wait()

    def multiply_out(route, step):
        base = ((first_at[route] + step) % 4) * 1024
        products[route, step] = jnp.dot(
            rows_ref[pl.ds(route * 96, 96), :],
            out_weight[:, pl.ds(pl.multiple_of(base, 1024), 1024)],
            preferred_element_type=jnp.float32,
        )

    def settle(route, step, chunk):
        scale = scale_rows[pl.ds(chunk * 64 + route * 32, 32), :]
        partial[route, step, chunk] = (
            products[route, step, pl.ds(chunk * 32, 32), :] * jnp.concatenate([scale] * 8, axis=1)
        ).astype(jnp.bfloat16)

    for step in (2, 1, 3, 0):
        for route in range(2):
            multiply_out(route, step)
    turned[...] = jnp.transpose(weighted[...]).astype(jnp.bfloat16)

    def keep_states(first, last):
        owner = lax.rem(lax.broadcasted_iota(jnp.int32, (192, 128), 0), 24)

        def keep(index, carry):
            inputs = input_rows[...]
            right = jnp.concatenate(
                [
                    jnp.where(owner == 2 * index + i, inputs, 0.0).astype(jnp.bfloat16)
                    for i in range(2)
                ],
                axis=1,
            )
            for h in range(8):
                update = jnp.dot(
                    turned[h * 64 : (h + 1) * 64, :], right, preferred_element_type=jnp.float32
                )
                for i in range(2):
                    request = 2 * index + i
                    decay = decay_kept[h, pl.ds(request, 1), :]
                    before = state[request, h * 64 : (h + 1) * 64, :].astype(jnp.float32)
                    kept_ref[request, h * 64 : (h + 1) * 64, :] = (
                        decay * before + update[:, i * 128 : (i + 1) * 128]
                    ).astype(jnp.bfloat16)
            return carry

        lax.fori_loop(first, last, keep, 0)

    held = {}
    for chunk in range(3):
        square_copies[chunk].wait_recv()
        scales = lax.rsqrt((square_own[chunk] + square_other[chunk]) / 1024.0 + EPSILON)
        for s in range(8):
            scale_rows[pl.ds(chunk * 64 + s, 8, stride=8), :] = jnp.broadcast_to(
                scales[:, s : s + 1], (8, 128)
            )
        for route in range(2):
            settle(route, 2, chunk)
            for half in range(2):
                held[route, chunk, half] = launch(
                    partial.at[route, 2, chunk, :, HALVES[half]],
                    first_recv.at[route, chunk, half],
                    0,
                    route,
                    chunk,
                    half,
                    firsts[route][(1, 3)[half]],
                )
    for chunk in range(3):
        for route in range(2):
            for step, half, slot in ((1, 1, 4), (3, 0, 3)):
                settle(route, step, chunk)
                launch(
                    partial.at[route, step, chunk, :, HALVES[half]],
                    first_recv.at[route, chunk, slot],
                    0,
                    route,
                    chunk,
                    slot,
                    firsts[route][step],
                )
    for chunk in range(3):
        for route in range(2):
            settle(route, 0, chunk)
    keep_states(0, 7)
    for chunk in range(3):
        for half in range(2):
            for route in range(2):
                landing = first_recv.at[route, chunk]
                held[route, chunk, half].wait_recv()
                mix = first_mix.at[route, chunk, half]
                mix[...] = widened_sum(
                    landing.at[half], partial.at[route, (1, 3)[half], chunk, :, HALVES[half]]
                )
                slot = (2, 5)[half]
                held[route, chunk, slot] = launch(
                    mix, landing.at[slot], 0, route, chunk, slot, firsts[route][(1, 3)[half]]
                )

    def spread_start(stage, places, piece, chunk, crossed):
        started = []
        for route in range(2):
            started.append([])
            for half in range(2):
                own = piece(route, chunk, half, 0)
                place = places[route][(1, 3)[half ^ crossed]]
                slot = 2 * crossed + half
                started[route].append(launch(own, own, stage, route, chunk, slot, place))
        return started

    def spread_forward(started, stage, places, piece, chunk):
        for half in range(2):
            for route in range(2):
                started[route][half].wait_recv()
                passed = piece(route, chunk, half, (3, 1)[half])
                launch(passed, passed, stage, route, chunk, 4 + half, places[route][(1, 3)[half]])

    def spread_finish(stage, chunk):
        await_bytes(in_weight.at[pl.ds(0, 1024)], stage, chunk, 4)

    def middle(route, chunk, half, k):
        return gathered.at[route, chunk, (second_at[route] + k) % 4, :, HALVES[half]]

    def spot(route, chunk, half, k):
        column = ((first_at[route] + k) % 4) * 1024 + half * 512
        return out_ref.at[
            pl.ds(chunk * 64 + route * 32, 32), pl.ds(pl.multiple_of(column, 512), 512)
        ]

    inner_spread = []
    for chunk in range(3):
        for half in range(2):
            for route in range(2):
                pair_ref = first_recv.at[route, chunk, pl.ds(2 + 2 * half, 2)]
                await_bytes(pair_ref, 0, chunk, 4 + route * 2 + half)
                own = middle(route, chunk, half, 0)
                own[...] = widened_sum(
                    partial.at[route, 0, chunk, :, HALVES[half]],
                    first_recv.at[route, chunk, 2 + 2 * half],
                    first_recv.at[route, chunk, 3 + 2 * half],
                )
        inner_spread.append(spread_start(1, seconds, middle, chunk, 0))
    for chunk in range(3):
        spread_start(1, seconds, middle, chunk, 1)
    pltpu.make_async_copy(
        count_buf.at[pl.ds(1, 7)], count_buf.at[pl.ds(1, 7)], count_sems.at[1]
    ).wait()
    everyone = count_buf[0]
    for d in range(1, 8):
        everyone = everyone + count_buf[d]
    total_own[0] = jnp.sum(everyone[0:1, 0:1]).astype(jnp.int32)
    total_copy = pltpu.make_async_copy(total_own, total_ref, swap_sems.at[8])
    total_copy.start()
    for chunk in range(3):
        spread_forward(inner_spread[chunk], 1, seconds, middle, chunk)
    outer_spread = []
    for chunk in range(3):
        spread_finish(1, chunk)
        for half in range(2):
            for route in range(2):
                own = spot(route, chunk, half, 0)
                own[...] = widened_sum(*(gathered.at[route, chunk, b, :, HALVES[half]] for b in range(4)))
        outer_spread.append(spread_start(2, firsts, spot, chunk, 0))
    for chunk in range(3):
        spread_start(2, firsts, spot, chunk, 1)
    for chunk in range(3):
        spread_forward(outer_spread[chunk], 2, firsts, spot, chunk)
    keep_states(7, 12)
    for chunk in range(3):
        spread_finish(2, chunk)
    total_copy.wait()
    pltpu.make_async_copy(
        count_buf.at[pl.ds(1, 7)], count_buf.at[pl.ds(1, 7)], count_sems.at[0]
    ).wait()
    for copy in square_copies + [swap]:
        copy.wait_send()
    sent = in_weight.at[pl.ds(0, 13824)]
    pltpu.make_async_copy(sent, sent, send_sems.at[0]).wait()


def layer(*operands):
    return pl.pallas_call(
        layer_kernel,
        out_shape=(
            jax.ShapeDtypeStruct((192, 4096), jnp.bfloat16),
            jax.ShapeDtypeStruct((24, 512, 128), jnp.bfloat16),
            jax.ShapeDtypeStruct((3, 24, 512), jnp.bfloat16),
            jax.ShapeDtypeStruct((3, 24, 128), jnp.bfloat16),
            jax.ShapeDtypeStruct((1,), jnp.int32),
        ),
        in_specs=[pl.BlockSpec(memory_space=pltpu.HBM)] * 20,
        out_specs=(pl.BlockSpec(memory_space=pltpu.VMEM),) * 4
        + (pl.BlockSpec(memory_space=pltpu.HBM),),
        scratch_shapes=[
            pltpu.VMEM((192, 4096), jnp.bfloat16),
            pltpu.VMEM((1, 4096), jnp.float32),
            pltpu.VMEM((32768, 128), jnp.bfloat16),
            pltpu.VMEM((4096, 256), jnp.bfloat16),
            pltpu.VMEM((8, 4096), jnp.bfloat16),
            pltpu.VMEM((4, 512), jnp.bfloat16),
            pltpu.VMEM((512,), jnp.bfloat16),
            pltpu.VMEM((4, 128), jnp.bfloat16),
            pltpu.VMEM((128,), jnp.bfloat16),
            pltpu.VMEM((1, 8), jnp.float32),
            pltpu.VMEM((1, 8), jnp.float32),
            pltpu.VMEM((1, 8), jnp.float32),
            pltpu.VMEM((1, 512), jnp.float32),
            pltpu.VMEM((512, 4096), jnp.bfloat16),
            pltpu.VMEM((24, 512, 128), jnp.bfloat16),
            pltpu.VMEM((3, 24, 512), jnp.bfloat16),
            pltpu.VMEM((3, 24, 128), jnp.bfloat16),
            pltpu.VMEM((1, 24), jnp.int32),
            pltpu.VMEM((1, 24), jnp.int32),
            pltpu.VMEM((1, 24), jnp.int32),
            pltpu.VMEM((192, 4096), jnp.bfloat16),
            pltpu.VMEM((2, 2048, 128), jnp.float32),
            pltpu.VMEM((2, 2048, 128), jnp.float32),
            pltpu.VMEM((8, 192, 128), jnp.float32),
            pltpu.VMEM((192, 128), jnp.float32),
            pltpu.VMEM((192, 128), jnp.float32),
            pltpu.VMEM((2, 8, 24, 128), jnp.float32),
            pltpu.VMEM((192, 128), jnp.float32),
            pltpu.VMEM((4, 192, 128), jnp.float32),
            pltpu.VMEM((1248, 128), jnp.float32),
            pltpu.VMEM((1248, 512), jnp.float32),
            pltpu.VMEM((8, 24, 128), jnp.float32),
            pltpu.VMEM((192, 512), jnp.float32),
            pltpu.VMEM((512, 192), jnp.bfloat16),
            pltpu.VMEM((192, 128), jnp.float32),
            pltpu.VMEM((4, 192, 128), jnp.float32),
            pltpu.VMEM((192, 512), jnp.bfloat16),
            pltpu.VMEM((8, 24, 128), jnp.float32),
            pltpu.VMEM((3, 8, 128), jnp.float32),
            pltpu.VMEM((3, 8, 128), jnp.float32),
            pltpu.VMEM((192, 128), jnp.float32),
            pltpu.VMEM((2, 4, 96, 1024), jnp.float32),
            pltpu.VMEM((2, 4, 3, 32, 1024), jnp.bfloat16),
            pltpu.VMEM((2, 3, 6, 32, 512), jnp.bfloat16),
            pltpu.VMEM((2, 3, 2, 32, 512), jnp.bfloat16),
            pltpu.VMEM((2, 3, 4, 32, 1024), jnp.bfloat16),
            pltpu.VMEM((8, 8, 128), jnp.float32),
            pltpu.SMEM((1,), jnp.int32),
            pltpu.SemaphoreType.DMA((1,)),
            pltpu.SemaphoreType.DMA((54,)),
            pltpu.SemaphoreType.DMA((2,)),
            pltpu.SemaphoreType.DMA((9,)),
            pltpu.SemaphoreType.DMA((20,)),
            pltpu.SemaphoreType.DMA((4,)),
            pltpu.SemaphoreType.DMA((4,)),
        ],
        compiler_params=pltpu.CompilerParams(
            collective_id=0, has_side_effects=True, vmem_limit_bytes=44 * 1024 * 1024
        ),
    )(*(pltpu.with_memory_space_constraint(operand, pltpu.HBM) for operand in operands))


def place_kernel(*refs):
    sources, total, targets, total_out = refs[:4], refs[4], refs[5:9], refs[9]
    held, sems = refs[10:]
    inward = pltpu.make_async_copy(total, held, sems.at[4])
    inward.start()
    copies = [
        pltpu.make_async_copy(source, target, sems.at[index])
        for index, (source, target) in enumerate(zip(sources, targets))
    ]
    for copy in copies:
        copy.start()
    inward.wait()
    outward = pltpu.make_async_copy(held, total_out, sems.at[5])
    outward.start()
    for copy in copies + [outward]:
        copy.wait()


def place(*arrays):
    return pl.pallas_call(
        place_kernel,
        out_shape=tuple(jax.ShapeDtypeStruct(a.shape, a.dtype) for a in arrays),
        in_specs=[pl.BlockSpec(memory_space=pltpu.VMEM)] * 4
        + [pl.BlockSpec(memory_space=pltpu.HBM)],
        out_specs=(pl.BlockSpec(memory_space=pltpu.HBM),) * 5,
        scratch_shapes=[pltpu.SMEM((1,), jnp.int32), pltpu.SemaphoreType.DMA((6,))],
        compiler_params=pltpu.CompilerParams(vmem_limit_bytes=16 * 1024 * 1024),
    )(*arrays)


def local(
    tokens,
    norm_gain,
    in_weight,
    group_weight,
    step_weight,
    value_kernel,
    value_offset,
    group_kernel,
    group_offset,
    step_bias,
    decay_rate,
    skip_gain,
    out_gain,
    out_weight,
    scan_state,
    value_cache,
    group_cache,
    accepted,
    draft_lengths,
    live_flags,
):
    woven = in_weight.reshape(4096, 2, 4, 128).transpose(0, 2, 1, 3).reshape(32768, 128)
    rows, kept_state, value_kept, group_kept, total = layer(
        tokens.reshape(192, 4096),
        norm_gain.reshape(1, 4096),
        woven,
        group_weight,
        step_weight.T,
        value_kernel,
        value_offset,
        group_kernel,
        group_offset,
        step_bias.reshape(1, 8),
        decay_rate.reshape(1, 8),
        skip_gain.reshape(1, 8),
        out_gain.reshape(1, 512),
        out_weight,
        scan_state.reshape(24, 512, 128),
        value_cache.transpose(1, 0, 2),
        group_cache.transpose(1, 0, 2),
        accepted.reshape(1, 24),
        draft_lengths.reshape(1, 24),
        live_flags.reshape(1, 24),
    )
    rows, kept_state, value_kept, group_kept, total = place(
        rows, kept_state, value_kept, group_kept, total
    )
    return (
        rows.reshape(24, 8, 4096),
        kept_state.reshape(24, 8, 64, 128),
        value_kept.transpose(1, 0, 2),
        group_kept.transpose(1, 0, 2),
        total,
    )


def solution(mesh):
    in_specs = (
        P(DP, None, None),
        P(),
        P(None, None, "tensor"),
        P(None, "tensor"),
        P(None, "tensor"),
        P(None, "tensor"),
        P("tensor"),
        P(None, "tensor"),
        P("tensor"),
        P("tensor"),
        P("tensor"),
        P("tensor"),
        P("tensor"),
        P("tensor", None),
        P(DP, "tensor", None, None),
        P(DP, None, "tensor"),
        P(DP, None, "tensor"),
        P(DP),
        P(DP),
        P(DP),
    )
    out_specs = (
        P(DP, None, None),
        P(DP, "tensor", None, None),
        P(DP, None, "tensor"),
        P(DP, None, "tensor"),
        P(),
    )
    return jax.shard_map(local, mesh=mesh, in_specs=in_specs, out_specs=out_specs, check_vma=False)
```

```python
import jax
import jax.numpy as jnp
from jax import lax
from jax.experimental import pallas as pl
from jax.experimental.pallas import tpu as pltpu
from jax.sharding import PartitionSpec as P

DP = "dp"


EPSILON = 1e-05


def swapped(value, axis, distance):
    mask = 2**distance
    pairs = [(source, source ^ mask) for source in range(lax.axis_size(axis))]
    return lax.ppermute(value, axis, pairs)


MESH = pl.DeviceIdType.MESH
HALVES = (pl.ds(0, 512), pl.ds(512, 512))


def ring_places():
    tensor = lax.axis_index("tensor")
    z, y = tensor // 4, tensor % 4
    along_y = [{"tensor": z * 4 + (y + d) % 4} for d in range(4)]
    along_z = [{"tensor": ((z + d) % 4) * 4 + y} for d in range(4)]
    return (z, y, along_z, along_y)


def remote(src, dst, send, recv, place):
    return pltpu.make_async_remote_copy(
        src_ref=src,
        dst_ref=dst,
        send_sem=send,
        recv_sem=recv,
        device_id=place,
        device_id_type=MESH,
    )


def widened_sum(*refs):
    total = refs[0][...].astype(jnp.float32)
    for ref in refs[1:]:
        total = total + ref[...].astype(jnp.float32)
    return total.astype(jnp.bfloat16)


def layer_kernel(
    tokens_in,
    gain_in,
    in_weight_in,
    group_weight_in,
    step_weight_in,
    value_kernel_in,
    value_offset_in,
    group_kernel_in,
    group_offset_in,
    step_bias_in,
    decay_rate_in,
    skip_gain_in,
    out_gain_in,
    out_weight_in,
    state_in,
    value_cache_in,
    group_cache_in,
    accepted_in,
    lengths_in,
    live_in,
    out_ref,
    kept_ref,
    value_kept,
    group_kept,
    total_ref,
    tokens,
    gain,
    in_weight,
    group_weight,
    step_weight,
    value_kernel,
    value_offset,
    group_kernel,
    group_offset,
    step_bias,
    decay_rate,
    skip_gain,
    out_gain,
    out_weight,
    state,
    value_cache,
    group_cache,
    accepted,
    lengths,
    live,
    normed,
    spread_a,
    spread_b,
    inner,
    group_rows,
    step_rows,
    maps,
    map_rows,
    carried,
    small,
    mixing,
    decay_kept,
    weighted,
    turned,
    input_rows,
    gated_rows,
    rows_ref,
    squares,
    square_own,
    square_other,
    scale_rows,
    products,
    partial,
    first_recv,
    first_mix,
    gathered,
    count_buf,
    send_sems,
    recv_sems,
    count_sems,
    swap_sems,
    load_sems,
    token_sems,
    chunk_sems,
):
    z, y, along_z, along_y = ring_places()
    dp = lax.axis_index("dp")
    parity = y % 2
    mate = {"tensor": z * 4 + (y + 1 - 2 * parity)}
    barrier = pltpu.get_barrier_semaphore()
    dp_peers = [{"dp": (dp + d) % 8} for d in range(1, 8)]
    ring_peers = [along_z[1], along_z[3], along_y[1], along_y[3]]
    loads = {}

    def load(name, src, dst, index):
        loads[name] = pltpu.make_async_copy(src, dst, load_sems.at[index])
        loads[name].start()

    token_copies = []
    for index in range(4):
        rows = pl.ds(index * 48, 48)
        copy = pltpu.make_async_copy(tokens_in.at[rows], tokens.at[rows], token_sems.at[index])
        copy.start()
        token_copies.append(copy)
    load("gain", gain_in, gain, 1)
    for place in ring_peers + dp_peers:
        pl.semaphore_signal(barrier, inc=1, device_id=place, device_id_type=MESH)
    load("step_weight", step_weight_in, step_weight, 4)
    load("group_weight", group_weight_in, group_weight.at[:, 0:128], 3)
    load("accepted", accepted_in, accepted, 17)
    load("lengths", lengths_in, lengths, 18)
    load("live", live_in, live, 19)
    load("group_cache", group_cache_in, group_cache, 16)
    load("group_kernel", group_kernel_in, group_kernel, 7)
    load("group_offset", group_offset_in, group_offset, 8)
    load("step_bias", step_bias_in, step_bias, 9)
    load("decay_rate", decay_rate_in, decay_rate, 10)
    load("skip_gain", skip_gain_in, skip_gain, 11)
    def load_chunk(index):
        rows = pl.ds(index * 8192, 8192)
        pltpu.make_async_copy(in_weight_in.at[rows], in_weight.at[rows], chunk_sems.at[index]).start()

    load_chunk(0)
    load_chunk(1)

    def column(ref):
        square = lax.broadcasted_iota(jnp.int32, (24, 24), 0) == lax.broadcasted_iota(
            jnp.int32, (24, 24), 1
        )
        values = jnp.broadcast_to(ref[...].astype(jnp.float32), (24, 24))
        return jnp.sum(jnp.where(square, values, 0.0), axis=1, keepdims=True)

    loads["gain"].wait()

    def normalize(block):
        rows = slice(block * 16, block * 16 + 16)
        total = jnp.zeros((16, 256), jnp.float32)
        for part in range(16):
            piece = tokens[rows, part * 256 : (part + 1) * 256].astype(jnp.float32)
            total = total + piece * piece
        mean = jnp.sum(total, axis=1, keepdims=True) / 4096.0
        scale = jnp.broadcast_to(lax.rsqrt(mean + EPSILON), (16, 256))
        for part in range(16):
            columns = slice(part * 256, (part + 1) * 256)
            piece = tokens[rows, columns].astype(jnp.float32)
            normed[rows, columns] = (piece * scale * gain[:, columns]).astype(jnp.bfloat16)

    for index in range(4):
        token_copies[index].wait()
        if index in (0, 2):
            load_chunk(2 + index // 2)
        for block in range(3):
            normalize(index * 3 + block)
    loads["step_weight"].wait()
    for block in range(32):
        rows = slice(block * 128, (block + 1) * 128)
        group_weight[rows, 128:136] = jnp.transpose(
            step_weight[:, rows].astype(jnp.float32)
        ).astype(jnp.bfloat16)
    loads["group_weight"].wait()
    product = jnp.dot(normed[...], group_weight[...], preferred_element_type=jnp.float32)
    group_rows[...] = product[:, 0:128]
    step_rows[...] = product[:, 128:256]
    for name in ("accepted", "lengths", "live", "group_cache", "group_kernel", "group_offset"):
        loads[name].wait()
    kept = column(accepted) * column(live)
    alive = column(live) == 1.0
    length_column = column(lengths)

    def sequence_of(cache, rows):
        early = [cache[t].astype(jnp.float32) for t in range(3)]
        return early + [rounded(piece) for piece in rows]

    def rounded(piece):
        return piece.astype(jnp.bfloat16).astype(jnp.float32)

    def convolved(sequence, taps, offset):
        out = []
        for s in range(8):
            total = offset
            for k in range(4):
                total = total + taps[k] * sequence[s + k]
            out.append(total / (1.0 + jnp.exp(-total)))
        return out

    def kept_rows(sequence, counts, t):
        chosen = sequence[t]
        for k in range(1, 9):
            chosen = jnp.where(counts == float(k), sequence[k + t], chosen)
        return chosen.astype(jnp.bfloat16)

    group_taps = [group_kernel[k : k + 1, :].astype(jnp.float32) for k in range(4)]
    group_sequence = sequence_of(
        group_cache, [group_rows[pl.ds(s, 24, stride=8), :] for s in range(8)]
    )
    own_maps = convolved(
        group_sequence, group_taps, group_offset[...].astype(jnp.float32).reshape(1, 128)
    )
    for s in range(8):
        maps[parity, s] = own_maps[s]
    pl.semaphore_wait(barrier, 11)
    swap = pltpu.make_async_remote_copy(
        src_ref=maps.at[parity],
        dst_ref=maps.at[parity],
        send_sem=swap_sems.at[0],
        recv_sem=swap_sems.at[1],
        device_id=mate,
        device_id_type=MESH,
    )
    swap.start()
    count_buf[0] = jnp.broadcast_to(jnp.sum(kept, axis=0, keepdims=True), (8, 128))
    for d in range(1, 8):
        remote(
            count_buf.at[0], count_buf.at[d], count_sems.at[0], count_sems.at[1], dp_peers[d - 1]
        ).start()
    for t in range(3):
        group_kept[t] = kept_rows(group_sequence, kept, t)

    for name in ("step_bias", "decay_rate", "skip_gain"):
        loads[name].wait()

    inner[...] = jnp.zeros_like(inner)

    lower = lax.broadcasted_iota(jnp.int32, (256, 8, 128), 1) < 4

    def widen(start, spread):
        block = in_weight[pl.ds(pl.multiple_of(start * 4096, 4096), 4096), :].astype(jnp.float32)
        block = block.reshape(256, 16, 128)
        even, odd = block[:, 0:8], block[:, 8:16]
        spread[0] = jnp.where(lower, even, pltpu.roll(odd, 4, 1)).reshape(2048, 128)
        spread[1] = jnp.where(lower, pltpu.roll(even, 4, 1), odd).reshape(2048, 128)

    def multiply(start, spread):
        left = normed[:, pl.ds(pl.multiple_of(start * 512, 512), 512)]
        for part in range(2):
            for j in range(0, 4, 2):
                right = jnp.concatenate(
                    [
                        spread[j // 2, pl.ds(i * 2 + part, 512, stride=4), :].astype(jnp.bfloat16)
                        for i in range(2)
                    ],
                    axis=1,
                )
                product = jnp.dot(left, right, preferred_element_type=jnp.float32)
                for i in range(2):
                    inner[part * 4 + j + i] += product[:, i * 128 : (i + 1) * 128]

    def await_chunk(index):
        rows = pl.ds(pl.multiple_of(index * 8192, 8192), 8192)
        pltpu.make_async_copy(
            in_weight_in.at[rows], in_weight.at[rows], chunk_sems.at[index]
        ).wait()

    def pair(index, carry):
        await_chunk(index + 1)
        multiply(2 * index, spread_a)
        widen(2 * index + 1, spread_b)
        multiply(2 * index + 1, spread_b)
        widen(2 * index + 2, spread_a)
        return carry

    await_chunk(0)
    widen(0, spread_a)
    lax.fori_loop(0, 2, pair, 0)
    load("value_cache", value_cache_in, value_cache, 15)
    load("value_kernel", value_kernel_in, value_kernel, 5)
    load("value_offset", value_offset_in, value_offset, 6)
    load("out_gain", out_gain_in, out_gain, 12)
    load("state", state_in, state, 14)
    load("out_weight", out_weight_in, out_weight, 13)
    lax.fori_loop(2, 3, pair, 0)
    multiply(6, spread_a)
    widen(7, spread_b)
    multiply(7, spread_b)

    steps, after = [], []
    running = None
    for s in range(8):
        raw = step_rows[pl.ds(s, 24, stride=8), 0:8] + step_bias[...]
        size = jnp.maximum(raw, 0.0) + jnp.log1p(jnp.exp(-jnp.abs(raw)))
        change = -size * decay_rate[...]
        running = change if running is None else running + change
        steps.append(size)
        after.append(running)
    prefix_kept = jnp.zeros_like(running)

    def keep_small(q, value):
        for tile in range(3):
            small[pl.ds(tile * 416 + q * 8, 8), 0:8] = value[tile * 8 : tile * 8 + 8]

    for s in range(8):
        prefix_kept = jnp.where(kept == float(s + 1), after[s], prefix_kept)
    for s in range(8):
        keep_small(36 + s, jnp.exp(after[s]))
        keep_small(
            44 + s, jnp.where(kept > float(s), jnp.exp(prefix_kept - after[s]), 0.0) * steps[s]
        )
    head_decay = jnp.exp(prefix_kept)
    for h in range(8):
        decay_kept[h] = jnp.broadcast_to(head_decay[:, h : h + 1], (24, 128))
    swap.wait_recv()
    for s in range(8):
        map_rows[pl.ds(s, 24, stride=8), :] = maps[1, s]
        input_rows[pl.ds(s * 24, 24), :] = maps[0, s]
        for j in range(s + 1):
            match = jnp.sum(maps[1, s] * maps[0, j], axis=1, keepdims=True)
            keep_small(
                s * (s + 1) // 2 + j, jnp.exp(after[s] - after[j]) * steps[j] * match
            )
    hot = (
        lax.broadcasted_iota(jnp.int32, (8, 512), 1) // 64
        == lax.broadcasted_iota(jnp.int32, (8, 512), 0)
    ).astype(jnp.bfloat16)

    def expand(index, carry):
        rows = pl.ds(index * 416, 416)
        mixing[rows, :] = jnp.dot(
            small[rows, 0:8].astype(jnp.bfloat16), hot, preferred_element_type=jnp.float32
        )
        return carry

    loads["state"].wait()

    for name in ("value_cache", "value_kernel", "value_offset", "out_gain"):
        loads[name].wait()
    offset_row = value_offset[...].astype(jnp.float32).reshape(1, 512)
    lane = lax.broadcasted_iota(jnp.int32, (8, 128), 1)
    square_copies = []
    for tile in range(3):
        expand(tile, 0)
        eight = pl.ds(tile * 8, 8)
        for request in range(tile * 8, tile * 8 + 8):
            rows = pl.ds(request * 8, 8)
            product = lax.dot_general(
                map_rows[rows, :].astype(jnp.bfloat16),
                state[request],
                (((1,), (1,)), ((), ())),
                preferred_element_type=jnp.float32,
            )
            for block in range(4):
                carried[block, rows, :] = product[:, block * 128 : (block + 1) * 128]
        for block in range(4):
            columns = slice(block * 128, (block + 1) * 128)
            skip = jnp.where(
                lane < 64,
                jnp.broadcast_to(skip_gain[:, 2 * block : 2 * block + 1], (8, 128)),
                jnp.broadcast_to(skip_gain[:, 2 * block + 1 : 2 * block + 2], (8, 128)),
            )
            taps = [value_kernel[k : k + 1, columns].astype(jnp.float32) for k in range(4)]
            offset = offset_row[:, columns]
            counts = kept[tile * 8 : tile * 8 + 8]
            sequence = [value_cache[t, eight, columns].astype(jnp.float32) for t in range(3)] + [
                rounded(inner[4 + block, pl.ds(tile * 64 + s, 8, stride=8), :])
                for s in range(8)
            ]
            for t in range(3):
                value_kept[t, eight, columns] = kept_rows(sequence, counts, t)
            values = convolved(sequence, taps, offset)
            for s in range(8):
                weighted[pl.ds(s * 24 + tile * 8, 8), columns] = (
                    mixing[pl.ds(tile * 416 + (44 + s) * 8, 8), columns] * values[s]
                )
                total = (
                    mixing[pl.ds(tile * 416 + (36 + s) * 8, 8), columns]
                    * carried[block, pl.ds(tile * 64 + s, 8, stride=8), :]
                    + skip * values[s]
                )
                for j in range(s + 1):
                    q = s * (s + 1) // 2 + j
                    total = total + mixing[pl.ds(tile * 416 + q * 8, 8), columns] * values[j]
                gate = rounded(inner[block, pl.ds(tile * 64 + s, 8, stride=8), :])
                gated = total * (gate / (1.0 + jnp.exp(-gate)))
                square = gated * gated
                if block:
                    square = square + squares[s, eight]
                squares[s, eight] = square
                valid = jnp.logical_and(
                    alive[tile * 8 : tile * 8 + 8],
                    length_column[tile * 8 : tile * 8 + 8] > float(s),
                )
                gated_rows[block, pl.ds(tile * 64 + s, 8, stride=8), :] = jnp.where(
                    valid, gated * out_gain[:, columns], 0.0
                )
            for route in range(2):
                rows_ref[route * 96 + tile * 32 : route * 96 + tile * 32 + 32, columns] = gated_rows[
                    block, tile * 64 + route * 32 : tile * 64 + route * 32 + 32, :
                ].astype(jnp.bfloat16)
        own = jnp.zeros((8, 128), jnp.float32)
        for s in range(8):
            own = jnp.where(lane == s, jnp.sum(squares[s, eight], axis=1, keepdims=True), own)
        square_own[tile] = own
        copy = remote(
            square_own.at[tile],
            square_other.at[tile],
            swap_sems.at[2 + tile],
            swap_sems.at[5 + tile],
            mate,
        )
        copy.start()
        square_copies.append(copy)
    loads["out_weight"].wait()
    firsts = [along_y, along_z]
    first_at = [y, z]
    halving = []
    for at, make in ((z, lambda i: i * 4 + y), (y, lambda i: z * 4 + i)):
        halving.append([{"tensor": make(at + 1 - 2 * (at % 2))}, {"tensor": make(3 - at)}])

    def sem_at(stage, chunk):
        return chunk * 21 + (0, 8, 16)[stage]

    def launch(src, dst, stage, route, chunk, slot, place):
        if stage == 1:
            index = route * 4 + slot
        elif slot < 2:
            index = route * 2 + slot
        elif stage:
            index = 4
        else:
            index = 4 + route * 2 + (slot - 2) // 2
        landed = recv_sems.at[sem_at(stage, chunk) + index]
        copy = remote(src, dst, send_sems.at[0], landed, place)
        copy.start()
        return copy

    def await_bytes(ref, stage, chunk, index):
        pltpu.make_async_copy(ref, ref, recv_sems.at[sem_at(stage, chunk) + index]).wait()

    def multiply_out(route, step):
        base = ((first_at[route] + step) % 4) * 1024
        products[route, step] = jnp.dot(
            rows_ref[pl.ds(route * 96, 96), :],
            out_weight[:, pl.ds(pl.multiple_of(base, 1024), 1024)],
            preferred_element_type=jnp.float32,
        )

    def settle(route, step, chunk):
        scale = scale_rows[pl.ds(chunk * 64 + route * 32, 32), :]
        partial[route, step, chunk] = (
            products[route, step, pl.ds(chunk * 32, 32), :] * jnp.concatenate([scale] * 8, axis=1)
        ).astype(jnp.bfloat16)

    for step in (2, 1, 3, 0):
        for route in range(2):
            multiply_out(route, step)
    def keep_states(first, last):
        owner = lax.rem(lax.broadcasted_iota(jnp.int32, (192, 128), 0), 24)

        def keep(index, carry):
            inputs = input_rows[...]
            right = jnp.concatenate(
                [
                    jnp.where(owner == 2 * index + i, inputs, 0.0).astype(jnp.bfloat16)
                    for i in range(2)
                ],
                axis=1,
            )
            for h in range(8):
                update = jnp.dot(
                    turned[h * 64 : (h + 1) * 64, :], right, preferred_element_type=jnp.float32
                )
                for i in range(2):
                    request = 2 * index + i
                    decay = decay_kept[h, pl.ds(request, 1), :]
                    before = state[request, h * 64 : (h + 1) * 64, :].astype(jnp.float32)
                    kept_ref[request, h * 64 : (h + 1) * 64, :] = (
                        decay * before + update[:, i * 128 : (i + 1) * 128]
                    ).astype(jnp.bfloat16)
            return carry

        lax.fori_loop(first, last, keep, 0)

    held = {}
    for chunk in range(3):
        square_copies[chunk].wait_recv()
        scales = lax.rsqrt((square_own[chunk] + square_other[chunk]) / 1024.0 + EPSILON)
        for s in range(8):
            scale_rows[pl.ds(chunk * 64 + s, 8, stride=8), :] = jnp.broadcast_to(
                scales[:, s : s + 1], (8, 128)
            )
        for route in range(2):
            settle(route, 2, chunk)
            for half in range(2):
                held[route, chunk, half] = launch(
                    partial.at[route, 2, chunk, :, HALVES[half]],
                    first_recv.at[route, chunk, half],
                    0,
                    route,
                    chunk,
                    half,
                    firsts[route][(1, 3)[half]],
                )
    for chunk in range(3):
        for route in range(2):
            for step, half, slot in ((1, 1, 4), (3, 0, 3)):
                settle(route, step, chunk)
                launch(
                    partial.at[route, step, chunk, :, HALVES[half]],
                    first_recv.at[route, chunk, slot],
                    0,
                    route,
                    chunk,
                    slot,
                    firsts[route][step],
                )
    for chunk in range(3):
        for route in range(2):
            settle(route, 0, chunk)
    turned[...] = jnp.transpose(weighted[...]).astype(jnp.bfloat16)
    keep_states(0, 7)
    for chunk in range(3):
        for half in range(2):
            for route in range(2):
                landing = first_recv.at[route, chunk]
                held[route, chunk, half].wait_recv()
                mix = first_mix.at[route, chunk, half]
                mix[...] = widened_sum(
                    landing.at[half], partial.at[route, (1, 3)[half], chunk, :, HALVES[half]]
                )
                slot = (2, 5)[half]
                held[route, chunk, slot] = launch(
                    mix, landing.at[slot], 0, route, chunk, slot, firsts[route][(1, 3)[half]]
                )

    def spread_start(stage, places, piece, chunk, crossed):
        started = []
        for route in range(2):
            started.append([])
            for half in range(2):
                own = piece(route, chunk, half, 0)
                place = places[route][(1, 3)[half ^ crossed]]
                slot = 2 * crossed + half
                started[route].append(launch(own, own, stage, route, chunk, slot, place))
        return started

    def spread_forward(started, stage, places, piece, chunk):
        for half in range(2):
            for route in range(2):
                started[route][half].wait_recv()
                passed = piece(route, chunk, half, (3, 1)[half])
                launch(passed, passed, stage, route, chunk, 4 + half, places[route][(1, 3)[half]])

    def spread_finish(stage, chunk):
        await_bytes(in_weight.at[pl.ds(0, 1024)], stage, chunk, 4)

    def spot(route, chunk, half, k):
        column = ((first_at[route] + k) % 4) * 1024 + half * 512
        return out_ref.at[
            pl.ds(chunk * 64 + route * 32, 32), pl.ds(pl.multiple_of(column, 512), 512)
        ]

    paired = {}
    for chunk in range(3):
        for half in range(2):
            for route in range(2):
                pair_ref = first_recv.at[route, chunk, pl.ds(2 + 2 * half, 2)]
                await_bytes(pair_ref, 0, chunk, 4 + route * 2 + half)
                own = gathered.at[route, chunk, half, 0]
                own[...] = widened_sum(
                    partial.at[route, 0, chunk, :, HALVES[half]],
                    first_recv.at[route, chunk, 2 + 2 * half],
                    first_recv.at[route, chunk, 3 + 2 * half],
                )
                paired[route, chunk, half] = launch(
                    own,
                    gathered.at[route, chunk, half, 1],
                    1,
                    route,
                    chunk,
                    half,
                    halving[route][half],
                )
    pltpu.make_async_copy(
        count_buf.at[pl.ds(1, 7)], count_buf.at[pl.ds(1, 7)], count_sems.at[1]
    ).wait()
    everyone = count_buf[0]
    for d in range(1, 8):
        everyone = everyone + count_buf[d]
    total_ref[...] = everyone
    crossed = {}
    for chunk in range(3):
        for half in range(2):
            for route in range(2):
                paired[route, chunk, half].wait_recv()
                both = gathered.at[route, chunk, half, 2]
                both[...] = widened_sum(
                    gathered.at[route, chunk, half, 0], gathered.at[route, chunk, half, 1]
                )
                crossed[route, chunk, half] = launch(
                    both,
                    gathered.at[route, chunk, half, 3],
                    1,
                    route,
                    chunk,
                    2 + half,
                    halving[route][1 - half],
                )
    outer_spread = []
    for chunk in range(3):
        for half in range(2):
            for route in range(2):
                crossed[route, chunk, half].wait_recv()
                own = spot(route, chunk, half, 0)
                own[...] = widened_sum(
                    gathered.at[route, chunk, half, 2], gathered.at[route, chunk, half, 3]
                )
        outer_spread.append(spread_start(2, firsts, spot, chunk, 0))
    for chunk in range(3):
        spread_start(2, firsts, spot, chunk, 1)
    for chunk in range(3):
        spread_forward(outer_spread[chunk], 2, firsts, spot, chunk)
    keep_states(7, 12)
    for chunk in range(3):
        spread_finish(2, chunk)
    pltpu.make_async_copy(
        count_buf.at[pl.ds(1, 7)], count_buf.at[pl.ds(1, 7)], count_sems.at[0]
    ).wait()
    for copy in square_copies + [swap]:
        copy.wait_send()
    sent = in_weight.at[pl.ds(0, 12288)]
    pltpu.make_async_copy(sent, sent, send_sems.at[0]).wait()


def layer(*operands):
    return pl.pallas_call(
        layer_kernel,
        out_shape=(
            jax.ShapeDtypeStruct((192, 4096), jnp.bfloat16),
            jax.ShapeDtypeStruct((24, 512, 128), jnp.bfloat16),
            jax.ShapeDtypeStruct((3, 24, 512), jnp.bfloat16),
            jax.ShapeDtypeStruct((3, 24, 128), jnp.bfloat16),
            jax.ShapeDtypeStruct((8, 128), jnp.float32),
        ),
        in_specs=[pl.BlockSpec(memory_space=pltpu.HBM)] * 20,
        out_specs=(pl.BlockSpec(memory_space=pltpu.VMEM),) * 5,
        scratch_shapes=[
            pltpu.VMEM((192, 4096), jnp.bfloat16),
            pltpu.VMEM((1, 4096), jnp.float32),
            pltpu.VMEM((32768, 128), jnp.bfloat16),
            pltpu.VMEM((4096, 256), jnp.bfloat16),
            pltpu.VMEM((8, 4096), jnp.bfloat16),
            pltpu.VMEM((4, 512), jnp.bfloat16),
            pltpu.VMEM((512,), jnp.bfloat16),
            pltpu.VMEM((4, 128), jnp.bfloat16),
            pltpu.VMEM((128,), jnp.bfloat16),
            pltpu.VMEM((1, 8), jnp.float32),
            pltpu.VMEM((1, 8), jnp.float32),
            pltpu.VMEM((1, 8), jnp.float32),
            pltpu.VMEM((1, 512), jnp.float32),
            pltpu.VMEM((512, 4096), jnp.bfloat16),
            pltpu.VMEM((24, 512, 128), jnp.bfloat16),
            pltpu.VMEM((3, 24, 512), jnp.bfloat16),
            pltpu.VMEM((3, 24, 128), jnp.bfloat16),
            pltpu.VMEM((1, 24), jnp.int32),
            pltpu.VMEM((1, 24), jnp.int32),
            pltpu.VMEM((1, 24), jnp.int32),
            pltpu.VMEM((192, 4096), jnp.bfloat16),
            pltpu.VMEM((2, 2048, 128), jnp.float32),
            pltpu.VMEM((2, 2048, 128), jnp.float32),
            pltpu.VMEM((8, 192, 128), jnp.float32),
            pltpu.VMEM((192, 128), jnp.float32),
            pltpu.VMEM((192, 128), jnp.float32),
            pltpu.VMEM((2, 8, 24, 128), jnp.float32),
            pltpu.VMEM((192, 128), jnp.float32),
            pltpu.VMEM((4, 192, 128), jnp.float32),
            pltpu.VMEM((1248, 128), jnp.float32),
            pltpu.VMEM((1248, 512), jnp.float32),
            pltpu.VMEM((8, 24, 128), jnp.float32),
            pltpu.VMEM((192, 512), jnp.float32),
            pltpu.VMEM((512, 192), jnp.bfloat16),
            pltpu.VMEM((192, 128), jnp.float32),
            pltpu.VMEM((4, 192, 128), jnp.float32),
            pltpu.VMEM((192, 512), jnp.bfloat16),
            pltpu.VMEM((8, 24, 128), jnp.float32),
            pltpu.VMEM((3, 8, 128), jnp.float32),
            pltpu.VMEM((3, 8, 128), jnp.float32),
            pltpu.VMEM((192, 128), jnp.float32),
            pltpu.VMEM((2, 4, 96, 1024), jnp.float32),
            pltpu.VMEM((2, 4, 3, 32, 1024), jnp.bfloat16),
            pltpu.VMEM((2, 3, 6, 32, 512), jnp.bfloat16),
            pltpu.VMEM((2, 3, 2, 32, 512), jnp.bfloat16),
            pltpu.VMEM((2, 3, 2, 4, 32, 512), jnp.bfloat16),
            pltpu.VMEM((8, 8, 128), jnp.float32),
            pltpu.SemaphoreType.DMA((1,)),
            pltpu.SemaphoreType.DMA((63,)),
            pltpu.SemaphoreType.DMA((2,)),
            pltpu.SemaphoreType.DMA((9,)),
            pltpu.SemaphoreType.DMA((20,)),
            pltpu.SemaphoreType.DMA((4,)),
            pltpu.SemaphoreType.DMA((4,)),
        ],
        compiler_params=pltpu.CompilerParams(
            collective_id=0, has_side_effects=True, vmem_limit_bytes=44 * 1024 * 1024
        ),
    )(*(pltpu.with_memory_space_constraint(operand, pltpu.HBM) for operand in operands))


def place_kernel(*refs):
    sources, total, targets, total_out = refs[:4], refs[4], refs[5:9], refs[9]
    held, sems = refs[10:]
    pieces = []
    for index, cuts in enumerate((2, 4, 1, 1)):
        length = sources[index].shape[0] // cuts
        for cut in range(cuts):
            span = pl.ds(cut * length, length)
            pieces.append((sources[index].at[span], targets[index].at[span]))
    copies = [
        pltpu.make_async_copy(source, target, sems.at[index])
        for index, (source, target) in enumerate(pieces)
    ]
    for copy in copies:
        copy.start()
    held[0] = jnp.sum(total[0:1, 0:1]).astype(jnp.int32)
    outward = pltpu.make_async_copy(held, total_out, sems.at[8])
    outward.start()
    for copy in copies + [outward]:
        copy.wait()


def place(*arrays):
    return pl.pallas_call(
        place_kernel,
        out_shape=tuple(jax.ShapeDtypeStruct(a.shape, a.dtype) for a in arrays[:4])
        + (jax.ShapeDtypeStruct((1,), jnp.int32),),
        in_specs=[pl.BlockSpec(memory_space=pltpu.VMEM)] * 5,
        out_specs=(pl.BlockSpec(memory_space=pltpu.HBM),) * 5,
        scratch_shapes=[pltpu.SMEM((1,), jnp.int32), pltpu.SemaphoreType.DMA((9,))],
        compiler_params=pltpu.CompilerParams(vmem_limit_bytes=16 * 1024 * 1024),
    )(*arrays)


def local(
    tokens,
    norm_gain,
    in_weight,
    group_weight,
    step_weight,
    value_kernel,
    value_offset,
    group_kernel,
    group_offset,
    step_bias,
    decay_rate,
    skip_gain,
    out_gain,
    out_weight,
    scan_state,
    value_cache,
    group_cache,
    accepted,
    draft_lengths,
    live_flags,
):
    woven = in_weight.reshape(4096, 2, 4, 128).transpose(0, 2, 1, 3).reshape(32768, 128)
    rows, kept_state, value_kept, group_kept, total = layer(
        tokens.reshape(192, 4096),
        norm_gain.reshape(1, 4096),
        woven,
        group_weight,
        step_weight.T,
        value_kernel,
        value_offset,
        group_kernel,
        group_offset,
        step_bias.reshape(1, 8),
        decay_rate.reshape(1, 8),
        skip_gain.reshape(1, 8),
        out_gain.reshape(1, 512),
        out_weight,
        scan_state.reshape(24, 512, 128),
        value_cache.transpose(1, 0, 2),
        group_cache.transpose(1, 0, 2),
        accepted.reshape(1, 24),
        draft_lengths.reshape(1, 24),
        live_flags.reshape(1, 24),
    )
    rows, kept_state, value_kept, group_kept, total = place(
        rows, kept_state, value_kept, group_kept, total
    )
    return (
        rows.reshape(24, 8, 4096),
        kept_state.reshape(24, 8, 64, 128),
        value_kept.transpose(1, 0, 2),
        group_kept.transpose(1, 0, 2),
        total,
    )


def solution(mesh):
    in_specs = (
        P(DP, None, None),
        P(),
        P(None, None, "tensor"),
        P(None, "tensor"),
        P(None, "tensor"),
        P(None, "tensor"),
        P("tensor"),
        P(None, "tensor"),
        P("tensor"),
        P("tensor"),
        P("tensor"),
        P("tensor"),
        P("tensor"),
        P("tensor", None),
        P(DP, "tensor", None, None),
        P(DP, None, "tensor"),
        P(DP, None, "tensor"),
        P(DP),
        P(DP),
        P(DP),
    )
    out_specs = (
        P(DP, None, None),
        P(DP, "tensor", None, None),
        P(DP, None, "tensor"),
        P(DP, None, "tensor"),
        P(),
    )
    return jax.shard_map(local, mesh=mesh, in_specs=in_specs, out_specs=out_specs, check_vma=False)
```

```python
import jax
import jax.numpy as jnp
from jax import lax
from jax.experimental import pallas as pl
from jax.experimental.pallas import tpu as pltpu
from jax.sharding import PartitionSpec as P

DP = "dp"


EPSILON = 1e-05


def swapped(value, axis, distance):
    mask = 2**distance
    pairs = [(source, source ^ mask) for source in range(lax.axis_size(axis))]
    return lax.ppermute(value, axis, pairs)


MESH = pl.DeviceIdType.MESH
HALVES = (pl.ds(0, 512), pl.ds(512, 512))


def ring_places():
    tensor = lax.axis_index("tensor")
    z, y = tensor // 4, tensor % 4
    along_y = [{"tensor": z * 4 + (y + d) % 4} for d in range(4)]
    along_z = [{"tensor": ((z + d) % 4) * 4 + y} for d in range(4)]
    return (z, y, along_z, along_y)


def remote(src, dst, send, recv, place):
    return pltpu.make_async_remote_copy(
        src_ref=src,
        dst_ref=dst,
        send_sem=send,
        recv_sem=recv,
        device_id=place,
        device_id_type=MESH,
    )


def widened_sum(*refs):
    total = refs[0][...].astype(jnp.float32)
    for ref in refs[1:]:
        total = total + ref[...].astype(jnp.float32)
    return total.astype(jnp.bfloat16)


def layer_kernel(
    tokens_in,
    gain_in,
    in_weight_in,
    group_weight_in,
    step_weight_in,
    value_kernel_in,
    value_offset_in,
    group_kernel_in,
    group_offset_in,
    step_bias_in,
    decay_rate_in,
    skip_gain_in,
    out_gain_in,
    out_weight_in,
    state_in,
    value_cache_in,
    group_cache_in,
    accepted_in,
    lengths_in,
    live_in,
    out_ref,
    kept_ref,
    value_kept,
    group_kept,
    total_ref,
    tokens,
    gain,
    in_weight,
    group_weight,
    step_weight,
    value_kernel,
    value_offset,
    group_kernel,
    group_offset,
    step_bias,
    decay_rate,
    skip_gain,
    out_gain,
    out_weight,
    state,
    value_cache,
    group_cache,
    accepted,
    lengths,
    live,
    normed,
    spread_a,
    spread_b,
    inner,
    group_rows,
    step_rows,
    maps,
    map_rows,
    carried,
    small,
    mixing,
    decay_kept,
    weighted,
    turned,
    input_rows,
    gated_rows,
    rows_ref,
    squares,
    square_own,
    square_other,
    scale_rows,
    products,
    partial,
    first_recv,
    first_mix,
    gathered,
    count_buf,
    send_sems,
    recv_sems,
    count_sems,
    swap_sems,
    load_sems,
    token_sems,
    chunk_sems,
):
    z, y, along_z, along_y = ring_places()
    dp = lax.axis_index("dp")
    parity = y % 2
    mate = {"tensor": z * 4 + (y + 1 - 2 * parity)}
    barrier = pltpu.get_barrier_semaphore()
    dp_peers = [{"dp": (dp + d) % 8} for d in range(1, 8)]
    ring_peers = [along_z[1], along_z[3], along_y[1], along_y[3]]
    loads = {}

    def load(name, src, dst, index):
        loads[name] = pltpu.make_async_copy(src, dst, load_sems.at[index])
        loads[name].start()

    token_copies = []
    for index in range(4):
        rows = pl.ds(index * 48, 48)
        copy = pltpu.make_async_copy(tokens_in.at[rows], tokens.at[rows], token_sems.at[index])
        copy.start()
        token_copies.append(copy)
    load("gain", gain_in, gain, 1)
    for place in ring_peers + dp_peers:
        pl.semaphore_signal(barrier, inc=1, device_id=place, device_id_type=MESH)
    load("step_weight", step_weight_in, step_weight, 4)
    load("group_weight", group_weight_in, group_weight.at[:, 0:128], 3)
    load("accepted", accepted_in, accepted, 17)
    load("lengths", lengths_in, lengths, 18)
    load("live", live_in, live, 19)
    load("group_cache", group_cache_in, group_cache, 16)
    load("group_kernel", group_kernel_in, group_kernel, 7)
    load("group_offset", group_offset_in, group_offset, 8)
    load("step_bias", step_bias_in, step_bias, 9)
    load("decay_rate", decay_rate_in, decay_rate, 10)
    load("skip_gain", skip_gain_in, skip_gain, 11)
    def load_chunk(index):
        rows = pl.ds(index * 8192, 8192)
        pltpu.make_async_copy(in_weight_in.at[rows], in_weight.at[rows], chunk_sems.at[index]).start()

    load_chunk(0)
    load_chunk(1)

    def column(ref):
        square = lax.broadcasted_iota(jnp.int32, (24, 24), 0) == lax.broadcasted_iota(
            jnp.int32, (24, 24), 1
        )
        values = jnp.broadcast_to(ref[...].astype(jnp.float32), (24, 24))
        return jnp.sum(jnp.where(square, values, 0.0), axis=1, keepdims=True)

    loads["gain"].wait()

    def normalize(block):
        rows = slice(block * 16, block * 16 + 16)
        total = jnp.zeros((16, 256), jnp.float32)
        for part in range(16):
            piece = tokens[rows, part * 256 : (part + 1) * 256].astype(jnp.float32)
            total = total + piece * piece
        mean = jnp.sum(total, axis=1, keepdims=True) / 4096.0
        scale = jnp.broadcast_to(lax.rsqrt(mean + EPSILON), (16, 256))
        for part in range(16):
            columns = slice(part * 256, (part + 1) * 256)
            piece = tokens[rows, columns].astype(jnp.float32)
            normed[rows, columns] = (piece * scale * gain[:, columns]).astype(jnp.bfloat16)

    for index in range(4):
        token_copies[index].wait()
        if index in (0, 2):
            load_chunk(2 + index // 2)
        for block in range(3):
            normalize(index * 3 + block)
    loads["step_weight"].wait()
    for block in range(32):
        rows = slice(block * 128, (block + 1) * 128)
        group_weight[rows, 128:136] = jnp.transpose(
            step_weight[:, rows].astype(jnp.float32)
        ).astype(jnp.bfloat16)
    loads["group_weight"].wait()
    product = jnp.dot(normed[...], group_weight[...], preferred_element_type=jnp.float32)
    group_rows[...] = product[:, 0:128]
    step_rows[...] = product[:, 128:256]
    for name in ("accepted", "lengths", "live", "group_cache", "group_kernel", "group_offset"):
        loads[name].wait()
    kept = column(accepted) * column(live)
    alive = column(live) == 1.0
    length_column = column(lengths)

    def sequence_of(cache, rows):
        early = [cache[t].astype(jnp.float32) for t in range(3)]
        return early + [rounded(piece) for piece in rows]

    def rounded(piece):
        return piece.astype(jnp.bfloat16).astype(jnp.float32)

    def convolved(sequence, taps, offset):
        out = []
        for s in range(8):
            total = offset
            for k in range(4):
                total = total + taps[k] * sequence[s + k]
            out.append(total / (1.0 + jnp.exp(-total)))
        return out

    def kept_rows(sequence, counts, t):
        chosen = sequence[t]
        for k in range(1, 9):
            chosen = jnp.where(counts == float(k), sequence[k + t], chosen)
        return chosen.astype(jnp.bfloat16)

    group_taps = [group_kernel[k : k + 1, :].astype(jnp.float32) for k in range(4)]
    group_sequence = sequence_of(
        group_cache, [group_rows[pl.ds(s, 24, stride=8), :] for s in range(8)]
    )
    own_maps = convolved(
        group_sequence, group_taps, group_offset[...].astype(jnp.float32).reshape(1, 128)
    )
    for s in range(8):
        maps[parity, s] = own_maps[s]
    pl.semaphore_wait(barrier, 11)
    swap = pltpu.make_async_remote_copy(
        src_ref=maps.at[parity],
        dst_ref=maps.at[parity],
        send_sem=swap_sems.at[0],
        recv_sem=swap_sems.at[1],
        device_id=mate,
        device_id_type=MESH,
    )
    swap.start()
    count_buf[0] = jnp.broadcast_to(jnp.sum(kept, axis=0, keepdims=True), (8, 128))
    for d in range(1, 8):
        remote(
            count_buf.at[0], count_buf.at[d], count_sems.at[0], count_sems.at[1], dp_peers[d - 1]
        ).start()
    for t in range(3):
        group_kept[t] = kept_rows(group_sequence, kept, t)

    for name in ("step_bias", "decay_rate", "skip_gain"):
        loads[name].wait()

    inner[...] = jnp.zeros_like(inner)

    lower = lax.broadcasted_iota(jnp.int32, (256, 8, 128), 1) < 4

    def widen(start, spread):
        block = in_weight[pl.ds(pl.multiple_of(start * 4096, 4096), 4096), :].astype(jnp.float32)
        block = block.reshape(256, 16, 128)
        even, odd = block[:, 0:8], block[:, 8:16]
        spread[0] = jnp.where(lower, even, pltpu.roll(odd, 4, 1)).reshape(2048, 128)
        spread[1] = jnp.where(lower, pltpu.roll(even, 4, 1), odd).reshape(2048, 128)

    def multiply(start, spread):
        left = normed[:, pl.ds(pl.multiple_of(start * 512, 512), 512)]
        for part in range(2):
            for j in range(0, 4, 2):
                right = jnp.concatenate(
                    [
                        spread[j // 2, pl.ds(i * 2 + part, 512, stride=4), :].astype(jnp.bfloat16)
                        for i in range(2)
                    ],
                    axis=1,
                )
                product = jnp.dot(left, right, preferred_element_type=jnp.float32)
                for i in range(2):
                    inner[part * 4 + j + i] += product[:, i * 128 : (i + 1) * 128]

    def await_chunk(index):
        rows = pl.ds(pl.multiple_of(index * 8192, 8192), 8192)
        pltpu.make_async_copy(
            in_weight_in.at[rows], in_weight.at[rows], chunk_sems.at[index]
        ).wait()

    def pair(index, carry):
        await_chunk(index + 1)
        multiply(2 * index, spread_a)
        widen(2 * index + 1, spread_b)
        multiply(2 * index + 1, spread_b)
        widen(2 * index + 2, spread_a)
        return carry

    await_chunk(0)
    widen(0, spread_a)
    lax.fori_loop(0, 2, pair, 0)
    load("value_cache", value_cache_in, value_cache, 15)
    load("value_kernel", value_kernel_in, value_kernel, 5)
    load("value_offset", value_offset_in, value_offset, 6)
    load("out_gain", out_gain_in, out_gain, 12)
    load("state", state_in, state, 14)
    load("out_weight", out_weight_in, out_weight, 13)
    lax.fori_loop(2, 3, pair, 0)
    multiply(6, spread_a)
    widen(7, spread_b)
    multiply(7, spread_b)

    steps, after = [], []
    running = None
    for s in range(8):
        raw = step_rows[pl.ds(s, 24, stride=8), 0:8] + step_bias[...]
        size = jnp.maximum(raw, 0.0) + jnp.log1p(jnp.exp(-jnp.abs(raw)))
        change = -size * decay_rate[...]
        running = change if running is None else running + change
        steps.append(size)
        after.append(running)
    prefix_kept = jnp.zeros_like(running)

    def keep_small(q, value):
        for tile in range(3):
            small[pl.ds(tile * 416 + q * 8, 8), 0:8] = value[tile * 8 : tile * 8 + 8]

    for s in range(8):
        prefix_kept = jnp.where(kept == float(s + 1), after[s], prefix_kept)
    for s in range(8):
        keep_small(36 + s, jnp.exp(after[s]))
        keep_small(
            44 + s, jnp.where(kept > float(s), jnp.exp(prefix_kept - after[s]), 0.0) * steps[s]
        )
    head_decay = jnp.exp(prefix_kept)
    for h in range(8):
        decay_kept[h] = jnp.broadcast_to(head_decay[:, h : h + 1], (24, 128))
    swap.wait_recv()
    for s in range(8):
        map_rows[pl.ds(s, 24, stride=8), :] = maps[1, s]
        input_rows[pl.ds(s * 24, 24), :] = maps[0, s]
        for j in range(s + 1):
            match = jnp.sum(maps[1, s] * maps[0, j], axis=1, keepdims=True)
            keep_small(
                s * (s + 1) // 2 + j, jnp.exp(after[s] - after[j]) * steps[j] * match
            )
    hot = (
        lax.broadcasted_iota(jnp.int32, (8, 512), 1) // 64
        == lax.broadcasted_iota(jnp.int32, (8, 512), 0)
    ).astype(jnp.bfloat16)

    def expand(index, carry):
        rows = pl.ds(index * 416, 416)
        mixing[rows, :] = jnp.dot(
            small[rows, 0:8].astype(jnp.bfloat16), hot, preferred_element_type=jnp.float32
        )
        return carry

    loads["state"].wait()

    for name in ("value_cache", "value_kernel", "value_offset", "out_gain"):
        loads[name].wait()
    offset_row = value_offset[...].astype(jnp.float32).reshape(1, 512)
    lane = lax.broadcasted_iota(jnp.int32, (8, 128), 1)
    square_copies = []
    for tile in range(3):
        expand(tile, 0)
        eight = pl.ds(tile * 8, 8)
        for request in range(tile * 8, tile * 8 + 8):
            rows = pl.ds(request * 8, 8)
            product = lax.dot_general(
                map_rows[rows, :].astype(jnp.bfloat16),
                state[request],
                (((1,), (1,)), ((), ())),
                preferred_element_type=jnp.float32,
            )
            for block in range(4):
                carried[block, rows, :] = product[:, block * 128 : (block + 1) * 128]
        for block in range(4):
            columns = slice(block * 128, (block + 1) * 128)
            skip = jnp.where(
                lane < 64,
                jnp.broadcast_to(skip_gain[:, 2 * block : 2 * block + 1], (8, 128)),
                jnp.broadcast_to(skip_gain[:, 2 * block + 1 : 2 * block + 2], (8, 128)),
            )
            taps = [value_kernel[k : k + 1, columns].astype(jnp.float32) for k in range(4)]
            offset = offset_row[:, columns]
            counts = kept[tile * 8 : tile * 8 + 8]
            sequence = [value_cache[t, eight, columns].astype(jnp.float32) for t in range(3)] + [
                rounded(inner[4 + block, pl.ds(tile * 64 + s, 8, stride=8), :])
                for s in range(8)
            ]
            for t in range(3):
                value_kept[t, eight, columns] = kept_rows(sequence, counts, t)
            values = convolved(sequence, taps, offset)
            for s in range(8):
                weighted[pl.ds(s * 24 + tile * 8, 8), columns] = (
                    mixing[pl.ds(tile * 416 + (44 + s) * 8, 8), columns] * values[s]
                )
                total = (
                    mixing[pl.ds(tile * 416 + (36 + s) * 8, 8), columns]
                    * carried[block, pl.ds(tile * 64 + s, 8, stride=8), :]
                    + skip * values[s]
                )
                for j in range(s + 1):
                    q = s * (s + 1) // 2 + j
                    total = total + mixing[pl.ds(tile * 416 + q * 8, 8), columns] * values[j]
                gate = rounded(inner[block, pl.ds(tile * 64 + s, 8, stride=8), :])
                gated = total * (gate / (1.0 + jnp.exp(-gate)))
                square = gated * gated
                if block:
                    square = square + squares[s, eight]
                squares[s, eight] = square
                valid = jnp.logical_and(
                    alive[tile * 8 : tile * 8 + 8],
                    length_column[tile * 8 : tile * 8 + 8] > float(s),
                )
                gated_rows[block, pl.ds(tile * 64 + s, 8, stride=8), :] = jnp.where(
                    valid, gated * out_gain[:, columns], 0.0
                )
            for route in range(2):
                rows_ref[route * 96 + tile * 32 : route * 96 + tile * 32 + 32, columns] = gated_rows[
                    block, tile * 64 + route * 32 : tile * 64 + route * 32 + 32, :
                ].astype(jnp.bfloat16)
        own = jnp.zeros((8, 128), jnp.float32)
        for s in range(8):
            own = jnp.where(lane == s, jnp.sum(squares[s, eight], axis=1, keepdims=True), own)
        square_own[tile] = own
        copy = remote(
            square_own.at[tile],
            square_other.at[tile],
            swap_sems.at[2 + tile],
            swap_sems.at[5 + tile],
            mate,
        )
        copy.start()
        square_copies.append(copy)
    loads["out_weight"].wait()
    firsts = [along_y, along_z]
    first_at = [y, z]
    halving = []
    for at, make in ((z, lambda i: i * 4 + y), (y, lambda i: z * 4 + i)):
        halving.append([{"tensor": make(at + 1 - 2 * (at % 2))}, {"tensor": make(3 - at)}])

    def sem_at(stage, chunk):
        return chunk * 21 + (0, 8, 16)[stage]

    def launch(src, dst, stage, route, chunk, slot, place):
        if stage == 1:
            index = route * 4 + slot
        elif slot < 2:
            index = route * 2 + slot
        elif stage:
            index = 4
        else:
            index = 4 + route * 2 + (slot - 2) // 2
        landed = recv_sems.at[sem_at(stage, chunk) + index]
        copy = remote(src, dst, send_sems.at[0], landed, place)
        copy.start()
        return copy

    def await_bytes(ref, stage, chunk, index):
        pltpu.make_async_copy(ref, ref, recv_sems.at[sem_at(stage, chunk) + index]).wait()

    def multiply_out(block):
        products[block] = jnp.dot(
            rows_ref[...],
            out_weight[:, block * 1024 : (block + 1) * 1024],
            preferred_element_type=jnp.float32,
        )

    def settle(route, step, chunk):
        scale = scale_rows[pl.ds(chunk * 64 + route * 32, 32), :]
        partial[route, step, chunk] = (
            products[
                (first_at[route] + step) % 4, pl.ds(route * 96 + chunk * 32, 32), :
            ] * jnp.concatenate([scale] * 8, axis=1)
        ).astype(jnp.bfloat16)

    for block in range(4):
        multiply_out(block)
    def keep_states(first, last):
        owner = lax.rem(lax.broadcasted_iota(jnp.int32, (192, 128), 0), 24)

        def keep(index, carry):
            inputs = input_rows[...]
            right = jnp.concatenate(
                [
                    jnp.where(owner == 2 * index + i, inputs, 0.0).astype(jnp.bfloat16)
                    for i in range(2)
                ],
                axis=1,
            )
            for h in range(8):
                update = jnp.dot(
                    turned[h * 64 : (h + 1) * 64, :], right, preferred_element_type=jnp.float32
                )
                for i in range(2):
                    request = 2 * index + i
                    decay = decay_kept[h, pl.ds(request, 1), :]
                    before = state[request, h * 64 : (h + 1) * 64, :].astype(jnp.float32)
                    kept_ref[request, h * 64 : (h + 1) * 64, :] = (
                        decay * before + update[:, i * 128 : (i + 1) * 128]
                    ).astype(jnp.bfloat16)
            return carry

        lax.fori_loop(first, last, keep, 0)

    held = {}
    for chunk in range(3):
        square_copies[chunk].wait_recv()
        scales = lax.rsqrt((square_own[chunk] + square_other[chunk]) / 1024.0 + EPSILON)
        for s in range(8):
            scale_rows[pl.ds(chunk * 64 + s, 8, stride=8), :] = jnp.broadcast_to(
                scales[:, s : s + 1], (8, 128)
            )
        for route in range(2):
            settle(route, 2, chunk)
            for half in range(2):
                held[route, chunk, half] = launch(
                    partial.at[route, 2, chunk, :, HALVES[half]],
                    first_recv.at[route, chunk, half],
                    0,
                    route,
                    chunk,
                    half,
                    firsts[route][(1, 3)[half]],
                )
    for chunk in range(3):
        for route in range(2):
            for step, half, slot in ((1, 1, 4), (3, 0, 3)):
                settle(route, step, chunk)
                launch(
                    partial.at[route, step, chunk, :, HALVES[half]],
                    first_recv.at[route, chunk, slot],
                    0,
                    route,
                    chunk,
                    slot,
                    firsts[route][step],
                )
    for chunk in range(3):
        for route in range(2):
            settle(route, 0, chunk)
    turned[...] = jnp.transpose(weighted[...]).astype(jnp.bfloat16)
    keep_states(0, 7)
    for chunk in range(3):
        for half in range(2):
            for route in range(2):
                landing = first_recv.at[route, chunk]
                held[route, chunk, half].wait_recv()
                mix = first_mix.at[route, chunk, half]
                mix[...] = widened_sum(
                    landing.at[half], partial.at[route, (1, 3)[half], chunk, :, HALVES[half]]
                )
                slot = (2, 5)[half]
                held[route, chunk, slot] = launch(
                    mix, landing.at[slot], 0, route, chunk, slot, firsts[route][(1, 3)[half]]
                )

    def spread_start(stage, places, piece, chunk, crossed):
        started = []
        for route in range(2):
            started.append([])
            for half in range(2):
                own = piece(route, chunk, half, 0)
                place = places[route][(1, 3)[half ^ crossed]]
                slot = 2 * crossed + half
                started[route].append(launch(own, own, stage, route, chunk, slot, place))
        return started

    def spread_forward(started, stage, places, piece, chunk):
        for half in range(2):
            for route in range(2):
                started[route][half].wait_recv()
                passed = piece(route, chunk, half, (3, 1)[half])
                launch(passed, passed, stage, route, chunk, 4 + half, places[route][(1, 3)[half]])

    def spread_finish(stage, chunk):
        await_bytes(in_weight.at[pl.ds(0, 1024)], stage, chunk, 4)

    def spot(route, chunk, half, k):
        column = ((first_at[route] + k) % 4) * 1024 + half * 512
        return out_ref.at[
            pl.ds(chunk * 64 + route * 32, 32), pl.ds(pl.multiple_of(column, 512), 512)
        ]

    paired = {}
    for chunk in range(3):
        for half in range(2):
            for route in range(2):
                pair_ref = first_recv.at[route, chunk, pl.ds(2 + 2 * half, 2)]
                await_bytes(pair_ref, 0, chunk, 4 + route * 2 + half)
                own = gathered.at[route, chunk, half, 0]
                own[...] = widened_sum(
                    partial.at[route, 0, chunk, :, HALVES[half]],
                    first_recv.at[route, chunk, 2 + 2 * half],
                    first_recv.at[route, chunk, 3 + 2 * half],
                )
                paired[route, chunk, half] = launch(
                    own,
                    gathered.at[route, chunk, half, 1],
                    1,
                    route,
                    chunk,
                    half,
                    halving[route][half],
                )
    pltpu.make_async_copy(
        count_buf.at[pl.ds(1, 7)], count_buf.at[pl.ds(1, 7)], count_sems.at[1]
    ).wait()
    everyone = count_buf[0]
    for d in range(1, 8):
        everyone = everyone + count_buf[d]
    total_ref[...] = everyone
    crossed = {}
    for chunk in range(3):
        for half in range(2):
            for route in range(2):
                paired[route, chunk, half].wait_recv()
                both = gathered.at[route, chunk, half, 2]
                both[...] = widened_sum(
                    gathered.at[route, chunk, half, 0], gathered.at[route, chunk, half, 1]
                )
                crossed[route, chunk, half] = launch(
                    both,
                    gathered.at[route, chunk, half, 3],
                    1,
                    route,
                    chunk,
                    2 + half,
                    halving[route][1 - half],
                )
    outer_spread = []
    for chunk in range(3):
        for half in range(2):
            for route in range(2):
                crossed[route, chunk, half].wait_recv()
                own = spot(route, chunk, half, 0)
                own[...] = widened_sum(
                    gathered.at[route, chunk, half, 2], gathered.at[route, chunk, half, 3]
                )
        outer_spread.append(spread_start(2, firsts, spot, chunk, 0))
    for chunk in range(3):
        spread_start(2, firsts, spot, chunk, 1)
    for chunk in range(3):
        spread_forward(outer_spread[chunk], 2, firsts, spot, chunk)
    keep_states(7, 12)
    for chunk in range(3):
        spread_finish(2, chunk)
    pltpu.make_async_copy(
        count_buf.at[pl.ds(1, 7)], count_buf.at[pl.ds(1, 7)], count_sems.at[0]
    ).wait()
    for copy in square_copies + [swap]:
        copy.wait_send()
    sent = in_weight.at[pl.ds(0, 12288)]
    pltpu.make_async_copy(sent, sent, send_sems.at[0]).wait()


def layer(*operands):
    return pl.pallas_call(
        layer_kernel,
        out_shape=(
            jax.ShapeDtypeStruct((192, 4096), jnp.bfloat16),
            jax.ShapeDtypeStruct((24, 512, 128), jnp.bfloat16),
            jax.ShapeDtypeStruct((3, 24, 512), jnp.bfloat16),
            jax.ShapeDtypeStruct((3, 24, 128), jnp.bfloat16),
            jax.ShapeDtypeStruct((8, 128), jnp.float32),
        ),
        in_specs=[pl.BlockSpec(memory_space=pltpu.HBM)] * 20,
        out_specs=(pl.BlockSpec(memory_space=pltpu.VMEM),) * 5,
        scratch_shapes=[
            pltpu.VMEM((192, 4096), jnp.bfloat16),
            pltpu.VMEM((1, 4096), jnp.float32),
            pltpu.VMEM((32768, 128), jnp.bfloat16),
            pltpu.VMEM((4096, 256), jnp.bfloat16),
            pltpu.VMEM((8, 4096), jnp.bfloat16),
            pltpu.VMEM((4, 512), jnp.bfloat16),
            pltpu.VMEM((512,), jnp.bfloat16),
            pltpu.VMEM((4, 128), jnp.bfloat16),
            pltpu.VMEM((128,), jnp.bfloat16),
            pltpu.VMEM((1, 8), jnp.float32),
            pltpu.VMEM((1, 8), jnp.float32),
            pltpu.VMEM((1, 8), jnp.float32),
            pltpu.VMEM((1, 512), jnp.float32),
            pltpu.VMEM((512, 4096), jnp.bfloat16),
            pltpu.VMEM((24, 512, 128), jnp.bfloat16),
            pltpu.VMEM((3, 24, 512), jnp.bfloat16),
            pltpu.VMEM((3, 24, 128), jnp.bfloat16),
            pltpu.VMEM((1, 24), jnp.int32),
            pltpu.VMEM((1, 24), jnp.int32),
            pltpu.VMEM((1, 24), jnp.int32),
            pltpu.VMEM((192, 4096), jnp.bfloat16),
            pltpu.VMEM((2, 2048, 128), jnp.float32),
            pltpu.VMEM((2, 2048, 128), jnp.float32),
            pltpu.VMEM((8, 192, 128), jnp.float32),
            pltpu.VMEM((192, 128), jnp.float32),
            pltpu.VMEM((192, 128), jnp.float32),
            pltpu.VMEM((2, 8, 24, 128), jnp.float32),
            pltpu.VMEM((192, 128), jnp.float32),
            pltpu.VMEM((4, 192, 128), jnp.float32),
            pltpu.VMEM((1248, 128), jnp.float32),
            pltpu.VMEM((1248, 512), jnp.float32),
            pltpu.VMEM((8, 24, 128), jnp.float32),
            pltpu.VMEM((192, 512), jnp.float32),
            pltpu.VMEM((512, 192), jnp.bfloat16),
            pltpu.VMEM((192, 128), jnp.float32),
            pltpu.VMEM((4, 192, 128), jnp.float32),
            pltpu.VMEM((192, 512), jnp.bfloat16),
            pltpu.VMEM((8, 24, 128), jnp.float32),
            pltpu.VMEM((3, 8, 128), jnp.float32),
            pltpu.VMEM((3, 8, 128), jnp.float32),
            pltpu.VMEM((192, 128), jnp.float32),
            pltpu.VMEM((4, 192, 1024), jnp.float32),
            pltpu.VMEM((2, 4, 3, 32, 1024), jnp.bfloat16),
            pltpu.VMEM((2, 3, 6, 32, 512), jnp.bfloat16),
            pltpu.VMEM((2, 3, 2, 32, 512), jnp.bfloat16),
            pltpu.VMEM((2, 3, 2, 4, 32, 512), jnp.bfloat16),
            pltpu.VMEM((8, 8, 128), jnp.float32),
            pltpu.SemaphoreType.DMA((1,)),
            pltpu.SemaphoreType.DMA((63,)),
            pltpu.SemaphoreType.DMA((2,)),
            pltpu.SemaphoreType.DMA((9,)),
            pltpu.SemaphoreType.DMA((20,)),
            pltpu.SemaphoreType.DMA((4,)),
            pltpu.SemaphoreType.DMA((4,)),
        ],
        compiler_params=pltpu.CompilerParams(
            collective_id=0, has_side_effects=True, vmem_limit_bytes=44 * 1024 * 1024
        ),
    )(*(pltpu.with_memory_space_constraint(operand, pltpu.HBM) for operand in operands))


def place_kernel(*refs):
    sources, total, targets, total_out = refs[:4], refs[4], refs[5:9], refs[9]
    held, sems = refs[10:]
    pieces = []
    for index, cuts in enumerate((2, 4, 1, 1)):
        length = sources[index].shape[0] // cuts
        for cut in range(cuts):
            span = pl.ds(cut * length, length)
            pieces.append((sources[index].at[span], targets[index].at[span]))
    copies = [
        pltpu.make_async_copy(source, target, sems.at[index])
        for index, (source, target) in enumerate(pieces)
    ]
    for copy in copies:
        copy.start()
    held[0] = jnp.sum(total[0:1, 0:1]).astype(jnp.int32)
    outward = pltpu.make_async_copy(held, total_out, sems.at[8])
    outward.start()
    for copy in copies + [outward]:
        copy.wait()


def place(*arrays):
    return pl.pallas_call(
        place_kernel,
        out_shape=tuple(jax.ShapeDtypeStruct(a.shape, a.dtype) for a in arrays[:4])
        + (jax.ShapeDtypeStruct((1,), jnp.int32),),
        in_specs=[pl.BlockSpec(memory_space=pltpu.VMEM)] * 5,
        out_specs=(pl.BlockSpec(memory_space=pltpu.HBM),) * 5,
        scratch_shapes=[pltpu.SMEM((1,), jnp.int32), pltpu.SemaphoreType.DMA((9,))],
        compiler_params=pltpu.CompilerParams(vmem_limit_bytes=16 * 1024 * 1024),
    )(*arrays)


def local(
    tokens,
    norm_gain,
    in_weight,
    group_weight,
    step_weight,
    value_kernel,
    value_offset,
    group_kernel,
    group_offset,
    step_bias,
    decay_rate,
    skip_gain,
    out_gain,
    out_weight,
    scan_state,
    value_cache,
    group_cache,
    accepted,
    draft_lengths,
    live_flags,
):
    woven = in_weight.reshape(4096, 2, 4, 128).transpose(0, 2, 1, 3).reshape(32768, 128)
    rows, kept_state, value_kept, group_kept, total = layer(
        tokens.reshape(192, 4096),
        norm_gain.reshape(1, 4096),
        woven,
        group_weight,
        step_weight.T,
        value_kernel,
        value_offset,
        group_kernel,
        group_offset,
        step_bias.reshape(1, 8),
        decay_rate.reshape(1, 8),
        skip_gain.reshape(1, 8),
        out_gain.reshape(1, 512),
        out_weight,
        scan_state.reshape(24, 512, 128),
        value_cache.transpose(1, 0, 2),
        group_cache.transpose(1, 0, 2),
        accepted.reshape(1, 24),
        draft_lengths.reshape(1, 24),
        live_flags.reshape(1, 24),
    )
    rows, kept_state, value_kept, group_kept, total = place(
        rows, kept_state, value_kept, group_kept, total
    )
    return (
        rows.reshape(24, 8, 4096),
        kept_state.reshape(24, 8, 64, 128),
        value_kept.transpose(1, 0, 2),
        group_kept.transpose(1, 0, 2),
        total,
    )


def solution(mesh):
    in_specs = (
        P(DP, None, None),
        P(),
        P(None, None, "tensor"),
        P(None, "tensor"),
        P(None, "tensor"),
        P(None, "tensor"),
        P("tensor"),
        P(None, "tensor"),
        P("tensor"),
        P("tensor"),
        P("tensor"),
        P("tensor"),
        P("tensor"),
        P("tensor", None),
        P(DP, "tensor", None, None),
        P(DP, None, "tensor"),
        P(DP, None, "tensor"),
        P(DP),
        P(DP),
        P(DP),
    )
    out_specs = (
        P(DP, None, None),
        P(DP, "tensor", None, None),
        P(DP, None, "tensor"),
        P(DP, None, "tensor"),
        P(),
    )
    return jax.shard_map(local, mesh=mesh, in_specs=in_specs, out_specs=out_specs, check_vma=False)
```
